32 devices in a mesh: dp: 2 (over x), tpa: 4 (over z), tpb: 4 (over y, core).
Axes of the slice: x: 2, y: 2, z: 4, core: 2. Of those that a mesh axis runs over, the one named last changes fastest.
Arguments:
- hidden: bfloat16 [512, 7, 2048], P('dp'), parts along dimension 0
- w_head: bfloat16 [2048, 49152], P(None, ('tpa', 'tpb'))
- q_draft: float32 [512, 6, 49152], P(('dp', 'tpa', 'tpb')), parts along dimension 0
- x_draft: int32 [512, 6], P('dp'), parts along dimension 0
Outputs:
- output 1: float32 [512, 6], P('dp'), parts along dimension 0
- output 2: float32 [512], P('dp'), parts along dimension 0
- output 3: float32 [512, 6, 49152], P('dp', None, ('tpa', 'tpb')), parts along dimension 0
- output 4: float32 [512, 49152], P('dp', ('tpa', 'tpb')), parts along dimension 0
There are 2 independent parts. The reference program is written for one: setup_inputs(seed, part) draws one part's arguments, and reference() takes and returns one part's arrays. A program takes and returns all parts, laid end to end along the dimension named above; an argument that names none is the same for every part.
All inputs are finite; a program needn't handle non-finite values.
Results may differ from the reference program's by a relative error of at most 0.001.
Values are sent between devices in bfloat16 or wider.
A program may use at most 1 GiB of HBM per device.

```python
import jax
import jax.numpy as jnp
from jax import lax

NUM_SEQS = 256
NUM_DRAFT = 6
D_MODEL = 2048
VOCAB_SIZE = 49152
ROW_BLOCK = 8
INV_TEMP = 1.25
DRAFT_LOGIT_SCALE = 0.5


def draw_tokens(tok_key):
    key_vals, key_low, key_high = jax.random.split(tok_key, 3)
    n_total = NUM_SEQS * NUM_DRAFT
    tokens = jax.random.randint(key_vals, (n_total,), 0, VOCAB_SIZE, jnp.int32)
    low_slot = jax.random.randint(key_low, (), 0, n_total, jnp.int32)
    high_slot = (low_slot + 1 + jax.random.randint(key_high, (), 0, n_total - 1, jnp.int32)) % n_total
    slots = jnp.arange(n_total, dtype=jnp.int32)
    tokens = jnp.where(slots == low_slot, 0, tokens)
    tokens = jnp.where(slots == high_slot, VOCAB_SIZE - 1, tokens)
    return tokens.reshape(NUM_SEQS, NUM_DRAFT)


def setup_inputs(seed: int = 0, part: int = 0) -> dict:
    base_key = jax.random.key(seed)
    part_key = jax.random.fold_in(base_key, part)
    key_hidden, key_draft, key_tok = jax.random.split(part_key, 3)
    hidden = jax.random.normal(key_hidden, (NUM_SEQS, NUM_DRAFT + 1, D_MODEL), jnp.float32)
    w_head = jax.random.normal(jax.random.key(seed + 1), (D_MODEL, VOCAB_SIZE), jnp.float32) * D_MODEL ** -0.5
    draft_logits = jax.random.normal(key_draft, (NUM_SEQS, NUM_DRAFT, VOCAB_SIZE), jnp.float32) * DRAFT_LOGIT_SCALE
    q_draft = jax.nn.softmax(draft_logits, axis=-1)
    x_draft = draw_tokens(key_tok)
    return {"hidden": hidden.astype(jnp.bfloat16), "w_head": w_head.astype(jnp.bfloat16), "q_draft": q_draft, "x_draft": x_draft}


def reference(hidden, w_head, q_draft, x_draft):
    num_blocks = NUM_SEQS // ROW_BLOCK

    def one_block(block):
        hid_blk, q_blk, tok_blk = block
        flat_hid = hid_blk.reshape(ROW_BLOCK * (NUM_DRAFT + 1), D_MODEL)
        logits = jnp.dot(flat_hid, w_head, preferred_element_type=jnp.float32) * INV_TEMP
        prob_all = jax.nn.softmax(logits, axis=-1).reshape(ROW_BLOCK, NUM_DRAFT + 1, VOCAB_SIZE)
        p_draft = prob_all[:, :NUM_DRAFT, :]
        tok_idx = tok_blk[:, :, None]
        p_pick = jnp.take_along_axis(p_draft, tok_idx, axis=2)[:, :, 0]
        q_pick = jnp.take_along_axis(q_blk, tok_idx, axis=2)[:, :, 0]
        accept = jnp.minimum(1.0, p_pick / q_pick)
        excess = jnp.maximum(p_draft - q_blk, 0.0)
        residual = excess / jnp.sum(excess, axis=-1, keepdims=True)
        return accept, residual, prob_all[:, NUM_DRAFT, :]

    block_outs = lax.map(one_block, (
        hidden.reshape(num_blocks, ROW_BLOCK, NUM_DRAFT + 1, D_MODEL),
        q_draft.reshape(num_blocks, ROW_BLOCK, NUM_DRAFT, VOCAB_SIZE),
        x_draft.reshape(num_blocks, ROW_BLOCK, NUM_DRAFT)))
    accept = block_outs[0].reshape(NUM_SEQS, NUM_DRAFT)
    residual = block_outs[1].reshape(NUM_SEQS, NUM_DRAFT, VOCAB_SIZE)
    bonus_prob = block_outs[2].reshape(NUM_SEQS, VOCAB_SIZE)
    expected = jnp.sum(jnp.cumprod(accept, axis=1), axis=1)
    return accept, expected, residual, bonus_prob
```

```python
import functools

import jax
import jax.numpy as jnp
from jax import lax
from jax.experimental import pallas as pl
from jax.experimental.pallas import tpu as pltpu
from jax.sharding import PartitionSpec as P

INV_TEMP = 1.25
VOCAB_AXES = ("tpa", "tpb")
MESH = pl.DeviceIdType.MESH
F32 = jnp.float32
FAR = ((3, 3, 0, 0), (2, 0, 3, 1), (1, 2, 1, 2))
CORE_OFFSETS = (0, 2, 1, 3)
NT = 512


def pick(index, values):
    out = jnp.int32(values[-1])
    for k in range(len(values) - 2, -1, -1):
        out = jnp.where(index == k, jnp.int32(values[k]), out)
    return out


def diag(n):
    return lax.broadcasted_iota(jnp.int32, (n, n), 0) == lax.broadcasted_iota(jnp.int32, (n, n), 1)


def to_col(row):
    return jnp.sum(jnp.where(diag(row.shape[1]), row, 0.0), axis=1, keepdims=True)


def to_row(col):
    return jnp.sum(jnp.where(diag(col.shape[0]), col, 0.0), axis=0, keepdims=True)


def put_row(acc, i, row):
    return jnp.where(lax.broadcasted_iota(jnp.int32, acc.shape, 0) == i, row, acc)


def get_row(rows, i):
    return jnp.sum(jnp.where(lax.broadcasted_iota(jnp.int32, rows.shape, 0) == i, rows, 0.0), axis=0, keepdims=True)


def exchange_kernel(dims, hid_ref, w_ref, q_ref, x_ref, ex_ref, bonus_ref, sums_ref,
                    hid_v, w_v, p_v, tok_v, stat_v, hid_sem, w_sem, own_sem,
                    q_send, q_recv, s_send, s_recv, z_send, z_recv):
    n_pos, seqs, depth, vocab, local_seqs, na, nb = dims
    n_draft = n_pos - 1
    n_peers = na * nb
    n_tiles = vocab // NT
    dp, za, tb = lax.axis_index("dp"), lax.axis_index("tpa"), lax.axis_index("tpb")
    me = za * nb + tb

    def peer(k):
        if isinstance(k, int):
            plane = pick(za, FAR[k // nb]) if k < 12 else za
            off = CORE_OFFSETS[k % nb] if k < 12 else k - 11
        else:
            group = k // nb
            plane = jnp.where(group == 0, pick(za, FAR[0]), jnp.where(group == 1, pick(za, FAR[1]),
                              jnp.where(group == 2, pick(za, FAR[2]), za)))
            off = jnp.where(k < 12, pick(lax.rem(k, nb), CORE_OFFSETS), k - 11)
        return plane, lax.rem(tb + off, nb)

    def q_copy(plane, core):
        other = plane * nb + core
        return pltpu.make_async_remote_copy(
            src_ref=q_ref.at[:, :, pl.ds(pl.multiple_of(other * vocab, 128), vocab)],
            dst_ref=ex_ref.at[:, pl.ds(pl.multiple_of(me * local_seqs, 8), local_seqs), :],
            send_sem=q_send.at[other], recv_sem=q_recv.at[me],
            device_id=(dp, plane, core), device_id_type=MESH)

    def q_arrival(other):
        return pltpu.make_async_remote_copy(
            src_ref=q_ref.at[:, :, pl.ds(0, vocab)],
            dst_ref=ex_ref.at[:, pl.ds(pl.multiple_of(other * local_seqs, 8), local_seqs), :],
            send_sem=q_send.at[other], recv_sem=q_recv.at[other],
            device_id=(dp, za, tb), device_id_type=MESH)

    def small_copy(ref, send, recv, slot, plane, core):
        other = plane * nb + core
        return pltpu.make_async_remote_copy(
            src_ref=ref.at[slot], dst_ref=ref.at[slot],
            send_sem=send.at[other], recv_sem=recv.at[slot],
            device_id=(dp, plane, core), device_id_type=MESH)

    def small_arrival(ref, send, recv, other):
        return pltpu.make_async_remote_copy(
            src_ref=ref.at[other], dst_ref=ref.at[other],
            send_sem=send.at[other], recv_sem=recv.at[other],
            device_id=(dp, za, tb), device_id_type=MESH)

    def w_copy(tile, slot):
        return pltpu.make_async_copy(w_ref.at[:, pl.ds(pl.multiple_of(tile * NT, NT), NT)], w_v.at[slot], w_sem.at[slot])

    hid_copy = pltpu.make_async_copy(hid_ref, hid_v, hid_sem)
    own_copy = pltpu.make_async_copy(
        q_ref.at[:, :, pl.ds(pl.multiple_of(me * vocab, 128), vocab)],
        ex_ref.at[:, pl.ds(pl.multiple_of(me * local_seqs, 8), local_seqs), :], own_sem)

    barrier = pltpu.get_barrier_semaphore()
    for k in range(1, n_peers):
        pl.semaphore_signal(barrier, inc=1, device_id=(dp, lax.rem(za + k // nb, na), lax.rem(tb + k % nb, nb)),
                            device_id_type=MESH)
    pl.semaphore_wait(barrier, n_peers - 1)

    for k in range(8):
        q_copy(*peer(k)).start()
    hid_copy.start()
    w_copy(0, 0).start()
    own_copy.start()

    first_id = me * vocab
    tok_rows = x_ref[...].astype(F32)
    for i in range(n_draft):
        tok_v[i] = jnp.broadcast_to(to_col(tok_rows[i:i + 1]), (seqs, 128)).astype(jnp.int32) - first_id
    hid_copy.wait()

    @pl.loop(0, n_tiles)
    def _(tile):
        slot = lax.rem(tile, 2)
        w_copy(tile, slot).wait()

        @pl.when(tile + 1 < n_tiles)
        def _():
            w_copy(tile + 1, 1 - slot).start()

        @pl.loop(0, n_pos)
        def _(i):
            p_v[i, :, pl.ds(pl.multiple_of(tile * NT, NT), NT)] = INV_TEMP * jnp.dot(
                hid_v[i], w_v[slot], preferred_element_type=F32)

    def stats(i, rows):
        def tile_max(t, m):
            return jnp.maximum(m, jnp.max(p_v[i, :, pl.ds(pl.multiple_of(t * NT, NT), NT)], axis=1, keepdims=True))

        m = lax.fori_loop(0, n_tiles, tile_max, jnp.full((seqs, 1), -jnp.inf, F32))

        def tile_sum(t, s):
            return s + jnp.sum(jnp.exp(p_v[i, :, pl.ds(pl.multiple_of(t * NT, NT), NT)] - m), axis=1, keepdims=True)

        s = lax.fori_loop(0, n_tiles, tile_sum, jnp.zeros((seqs, 1), F32))
        return put_row(rows[0], i, to_row(m)), put_row(rows[1], i, to_row(s))

    max_rows, sum_rows = lax.fori_loop(0, n_pos, stats, (jnp.zeros((8, seqs), F32), jnp.zeros((8, seqs), F32)))
    stat_v[me, 0:8, :] = max_rows
    stat_v[me, 8:16, :] = sum_rows
    for k in range(8, 15):
        if k == 11:
            for j in range(15):
                small_copy(stat_v, s_send, s_recv, me, *peer(j)).start()
        q_copy(*peer(k)).start()
    for j in range(15):
        plane, core = peer(j)
        small_arrival(stat_v, s_send, s_recv, plane * nb + core).wait_recv()

    all_max = stat_v[0, 0:8, :]
    for k in range(1, n_peers):
        all_max = jnp.maximum(all_max, stat_v[k, 0:8, :])
    all_sum = jnp.zeros((8, seqs), F32)
    for k in range(n_peers):
        all_sum += stat_v[k, 8:16, :] * jnp.exp(stat_v[k, 0:8, :] - all_max)
    inv_sum = 1.0 / jnp.where(lax.broadcasted_iota(jnp.int32, (8, seqs), 0) < n_pos, all_sum, 1.0)

    def normalise(i, picked):
        m, r = to_col(get_row(all_max, i)), to_col(get_row(inv_sum, i))
        tok = tok_v[i, :, 0:1]

        def tile(t, got):
            cols = pl.ds(pl.multiple_of(t * NT, NT), NT)
            prob = jnp.exp(p_v[i, :, cols] - m) * r
            p_v[i, :, cols] = prob
            lane = lax.broadcasted_iota(jnp.int32, (seqs, NT), 1) + t * NT
            return got + jnp.sum(jnp.where(lane == tok, prob, 0.0), axis=1, keepdims=True)

        return put_row(picked, i, to_row(lax.fori_loop(0, n_tiles, tile, jnp.zeros((seqs, 1), F32))))

    p_pick = lax.fori_loop(0, n_draft, normalise, jnp.zeros((8, seqs), F32))
    m, r = to_col(get_row(all_max, n_draft)), to_col(get_row(inv_sum, n_draft))

    @pl.loop(0, n_tiles)
    def _(t):
        cols = pl.ds(pl.multiple_of(t * NT, NT), NT)
        bonus_ref[:, cols] = jnp.exp(p_v[n_draft, :, cols] - m) * r

    def absorb(other, carry):
        first = pl.multiple_of(other * local_seqs, 8)
        rows = pl.ds(first, local_seqs)
        lane = lax.broadcasted_iota(jnp.int32, (local_seqs, vocab), 1)
        place = (lax.broadcasted_iota(jnp.int32, (local_seqs, seqs), 1)
                 == lax.broadcasted_iota(jnp.int32, (local_seqs, seqs), 0) + first)

        def one(i, carry):
            z_rows, q_rows = carry
            q = ex_ref[i, rows, :]
            got = jnp.sum(jnp.where(lane == tok_v[i, rows, 0:1], q, 0.0), axis=1, keepdims=True)
            excess = jnp.maximum(p_v[i, rows, :] - q, 0.0)
            ex_ref[i, rows, :] = excess
            z = jnp.sum(excess, axis=1, keepdims=True)
            here = lax.broadcasted_iota(jnp.int32, (8, seqs), 0) == i
            z_rows += jnp.where(here, jnp.sum(jnp.where(place, z, 0.0), axis=0, keepdims=True), 0.0)
            q_rows += jnp.where(here, jnp.sum(jnp.where(place, got, 0.0), axis=0, keepdims=True), 0.0)
            return z_rows, q_rows

        return lax.fori_loop(0, n_draft, one, carry)

    own_copy.wait()
    carry = absorb(me, (jnp.zeros((8, seqs), F32), jnp.zeros((8, seqs), F32)))

    def arrived(k, carry):
        plane, core = peer(lax.rem(k + 12, 15))
        other = plane * nb + core
        q_arrival(other).wait_recv()
        return absorb(other, carry)

    z_rows, q_pick = lax.fori_loop(0, 15, arrived, carry)

    local_tok = tok_rows - first_id.astype(F32)
    owned = (local_tok >= 0.0) & (local_tok < float(vocab))
    ratio = jnp.minimum(1.0, p_pick[:n_draft] / jnp.where(owned, q_pick[:n_draft], 1.0))
    sums_ref[me, 0:8, :] = z_rows
    sums_ref[me, 8:16, :] = jnp.zeros((8, seqs), F32)
    sums_ref[me, 8:8 + n_draft, :] = jnp.where(owned, ratio, 0.0)
    for j in range(15):
        small_copy(sums_ref, z_send, z_recv, me, *peer(j)).start()
    for j in range(15):
        plane, core = peer(j)
        small_arrival(sums_ref, z_send, z_recv, plane * nb + core).wait_recv()
    for j in range(15):
        q_copy(*peer(j)).wait_send()
        small_copy(stat_v, s_send, s_recv, me, *peer(j)).wait_send()
        small_copy(sums_ref, z_send, z_recv, me, *peer(j)).wait_send()


SLOTS = 4


def output_kernel(n_peers, ex_ref, bonus_ref, sums_ref, res_ref, bonus_out, accept_ref, expected_ref, stage, stage_sem, bonus_sem):
    n_draft, seqs, vocab = ex_ref.shape
    half = seqs // 2
    bonus_copy = pltpu.make_async_copy(bonus_ref, bonus_out, bonus_sem)
    bonus_copy.start()
    total = sums_ref[0]
    for k in range(1, n_peers):
        total += sums_ref[k]
    inv = 1.0 / jnp.where(lax.broadcasted_iota(jnp.int32, (8, seqs), 0) < n_draft, total[0:8], 1.0)

    def out_copy(k, slot):
        i, h = k // 2, lax.rem(k, 2)
        return pltpu.make_async_copy(
            stage.at[slot], res_ref.at[i, pl.ds(pl.multiple_of(h * half, half), half), :], stage_sem.at[slot])

    @pl.loop(0, 2 * n_draft)
    def _(k):
        i, h, slot = k // 2, lax.rem(k, 2), lax.rem(k, SLOTS)
        row = get_row(inv, i)
        col = to_col(jnp.where(h == 0, row[:, :half], row[:, half:]))

        @pl.when(k >= SLOTS)
        def _():
            out_copy(k - SLOTS, slot).wait()

        @pl.loop(0, vocab // NT)
        def _(t):
            cols = pl.ds(pl.multiple_of(t * NT, NT), NT)
            stage[slot, :, cols] = ex_ref[i, pl.ds(pl.multiple_of(h * half, half), half), cols] * col

        out_copy(k, slot).start()

    accept = total[8:8 + n_draft]
    accept_ref[...] = accept
    prod = accept[0:1]
    expected = prod
    for i in range(1, n_draft):
        prod = prod * accept[i:i + 1]
        expected += prod
    expected_ref[...] = expected
    for k in range(2 * n_draft - SLOTS, 2 * n_draft):
        out_copy(k, k % SLOTS).wait()
    bonus_copy.wait()


def solution(mesh):
    na, nb = mesh.shape["tpa"], mesh.shape["tpb"]
    n_peers = na * nb
    any_spec = pl.BlockSpec(memory_space=pl.ANY)
    vmem_spec = pl.BlockSpec(memory_space=pltpu.VMEM)

    def local_step(hidden, w_head, q_draft, x_draft):
        seqs, n_pos, depth = hidden.shape
        vocab = w_head.shape[1]
        local_seqs, n_draft, _ = q_draft.shape
        dims = (n_pos, seqs, depth, vocab, local_seqs, na, nb)
        dma = pltpu.SemaphoreType.DMA
        ex, bonus, sums = pl.pallas_call(
            functools.partial(exchange_kernel, dims),
            out_shape=(pltpu.VMEM((n_draft, seqs, vocab), F32), pltpu.VMEM((seqs, vocab), F32),
                       pltpu.VMEM((n_peers, 16, seqs), F32)),
            in_specs=[any_spec, any_spec, any_spec, vmem_spec],
            out_specs=(vmem_spec, vmem_spec, vmem_spec),
            scratch_shapes=[
                pltpu.VMEM((n_pos, seqs, depth), jnp.bfloat16),
                pltpu.VMEM((2, depth, NT), jnp.bfloat16),
                pltpu.VMEM((n_pos, seqs, vocab), F32),
                pltpu.VMEM((n_draft, seqs, 128), jnp.int32),
                pltpu.VMEM((n_peers, 16, seqs), F32),
                dma, dma((2,)), dma,
                dma((n_peers,)), dma((n_peers,)), dma((n_peers,)), dma((n_peers,)), dma((n_peers,)), dma((n_peers,)),
            ],
            compiler_params=pltpu.CompilerParams(collective_id=0, has_side_effects=True, vmem_limit_bytes=38 * 2**20),
            name="exchange",
        )(hidden.transpose(1, 0, 2), w_head, q_draft.transpose(1, 0, 2), x_draft.T)
        res, bonus_out, accept, expected = pl.pallas_call(
            functools.partial(output_kernel, n_peers),
            out_shape=(jax.ShapeDtypeStruct((n_draft, seqs, vocab), F32), jax.ShapeDtypeStruct((seqs, vocab), F32),
                       jax.ShapeDtypeStruct((n_draft, seqs), F32), jax.ShapeDtypeStruct((1, seqs), F32)),
            in_specs=[vmem_spec, vmem_spec, vmem_spec],
            out_specs=(any_spec, any_spec, vmem_spec, vmem_spec),
            scratch_shapes=[pltpu.VMEM((SLOTS, seqs // 2, vocab), F32), dma((SLOTS,)), dma],
            compiler_params=pltpu.CompilerParams(vmem_limit_bytes=12 * 2**20),
            name="output",
        )(ex, bonus, sums)
        return accept.T, expected.reshape(seqs), res.transpose(1, 0, 2), bonus_out

    return jax.shard_map(
        local_step, mesh=mesh,
        in_specs=(P("dp", None, None), P(None, VOCAB_AXES), P(("dp",) + VOCAB_AXES, None, None), P("dp", None)),
        out_specs=(P("dp", None), P("dp"), P("dp", None, VOCAB_AXES), P("dp", VOCAB_AXES)),
        check_vma=False)
```

```python
import functools

import jax
import jax.numpy as jnp
from jax import lax
from jax.experimental import pallas as pl
from jax.experimental.pallas import tpu as pltpu
from jax.sharding import PartitionSpec as P

INV_TEMP = 1.25
VOCAB_AXES = ("tpa", "tpb")
MESH = pl.DeviceIdType.MESH
F32 = jnp.float32
SEND = ((3, 3, 0, 0), (1, 0, 3, 2), (2, 2, 1, 1))
RECV = ((3, 0, 3, 0), (2, 3, 0, 1), (1, 2, 1, 2))
CORE_OFFSETS = (0, 2, 1, 3)
NT = 512


def pick(index, values):
    out = jnp.int32(values[-1])
    for k in range(len(values) - 2, -1, -1):
        out = jnp.where(index == k, jnp.int32(values[k]), out)
    return out


def diag(n):
    return lax.broadcasted_iota(jnp.int32, (n, n), 0) == lax.broadcasted_iota(jnp.int32, (n, n), 1)


def to_col(row):
    return jnp.sum(jnp.where(diag(row.shape[1]), row, 0.0), axis=1, keepdims=True)


def get_row(rows, i):
    return jnp.sum(jnp.where(lax.broadcasted_iota(jnp.int32, rows.shape, 0) == i, rows, 0.0), axis=0, keepdims=True)


def lanes(n, first, rows):
    return (lax.broadcasted_iota(jnp.int32, (rows, n), 1)
            == lax.broadcasted_iota(jnp.int32, (rows, n), 0) + first)


def spread(col, n, first):
    return jnp.sum(jnp.where(lanes(n, first, col.shape[0]), col, 0.0), axis=0, keepdims=True)


def gather(row, first, rows):
    return jnp.sum(jnp.where(lanes(row.shape[1], first, rows), row, 0.0), axis=1, keepdims=True)


def exchange_kernel(dims, hid_ref, w_ref, q_ref, x_ref, ex_ref, bonus_ref, early_ref, late_ref,
                    hid_v, w_v, z_v, tok_v, stat_out, stat_in, norm_v, sum_out, sum_in, hid_sem, w_sem, own_sem,
                    q_send, q_recv, r_send, r_recv, so_send, so_recv, n_send, n_recv, zo_send, zo_recv,
                    e_send, e_recv, l_send, l_recv):
    n_pos, seqs, depth, vocab, n_loc, na, nb = dims
    n_draft = n_pos - 1
    n_early = n_draft - 1
    n_peers = na * nb
    n_tiles = vocab // NT
    others = range(n_peers - 1)
    dp, za, tb = lax.axis_index("dp"), lax.axis_index("tpa"), lax.axis_index("tpb")
    me = za * nb + tb

    def send_peer(k):
        inner = (za == 1) | (za == 2)
        if k < 3:
            end, mid = (pick(za, SEND[0]), CORE_OFFSETS[k]), (za, k + 1)
        else:
            mid = (pick(za, SEND[(k - 3) // nb]), CORE_OFFSETS[(k - 3) % nb])
            end = (pick(za, SEND[k // nb]), CORE_OFFSETS[k % nb]) if k < 12 else (za, k - 11)
        plane = jnp.where(inner, mid[0], end[0])
        return plane, lax.rem(tb + jnp.where(inner, mid[1], end[1]), nb)

    def recv_peer(k):
        step, off = (k - 3) // nb, lax.rem(jnp.int32(k) + 1, nb)
        plane = jnp.where(k < 3, za, jnp.where(step == 0, pick(za, RECV[0]),
                          jnp.where(step == 1, pick(za, RECV[1]), pick(za, RECV[2]))))
        off = jnp.where(k < 3, k + 1, nb - pick(off, CORE_OFFSETS))
        return plane, lax.rem(tb + off, nb)

    def rows_of(group):
        return pl.ds(pl.multiple_of(group * n_loc, 8), n_loc)

    def q_copy(part, plane, core, own_group, column):
        i0, ni = (0, n_early) if part == 0 else (n_early, 1)
        send, recv = (q_send, q_recv) if part == 0 else (r_send, r_recv)
        return pltpu.make_async_remote_copy(
            src_ref=q_ref.at[pl.ds(i0, ni), :, pl.ds(pl.multiple_of(column * vocab, 128), vocab)],
            dst_ref=ex_ref.at[pl.ds(i0, ni), rows_of(own_group), :],
            send_sem=send.at[plane * nb + core], recv_sem=recv.at[own_group],
            device_id=(dp, plane, core), device_id_type=MESH)

    def q_to(part, k):
        plane, core = send_peer(k)
        return q_copy(part, plane, core, me, plane * nb + core)

    def q_from(part, group):
        return q_copy(part, za, tb, group, 0)

    def small(src, dst, send, recv, src_slot, dst_slot, plane, core):
        return pltpu.make_async_remote_copy(
            src_ref=src.at[src_slot], dst_ref=dst.at[dst_slot],
            send_sem=send.at[plane * nb + core], recv_sem=recv.at[dst_slot],
            device_id=(dp, plane, core), device_id_type=MESH)

    def scatter_to(src, dst, send, recv, plane, core):
        return small(src, dst, send, recv, plane * nb + core, me, plane, core)

    def share_to(ref, send, recv, plane, core):
        return small(ref, ref, send, recv, me, me, plane, core)

    def await_all(ref, send, recv):
        for k in others:
            plane, core = send_peer(k)
            small(ref, ref, send, recv, plane * nb + core, plane * nb + core, za, tb).wait_recv()

    def w_copy(tile, slot):
        return pltpu.make_async_copy(w_ref.at[:, pl.ds(pl.multiple_of(tile * NT, NT), NT)], w_v.at[slot], w_sem.at[slot])

    hid_copy = pltpu.make_async_copy(hid_ref, hid_v, hid_sem)
    own_copy = pltpu.make_async_copy(
        q_ref.at[:, :, pl.ds(pl.multiple_of(me * vocab, 128), vocab)], ex_ref.at[:, rows_of(me), :], own_sem)

    barrier = pltpu.get_barrier_semaphore()
    for k in range(1, n_peers):
        pl.semaphore_signal(barrier, inc=1, device_id=(dp, lax.rem(za + k // nb, na), lax.rem(tb + k % nb, nb)),
                            device_id_type=MESH)
    pl.semaphore_wait(barrier, n_peers - 1)

    for k in range(4):
        q_to(0, k).start()
    hid_copy.start()
    w_copy(0, 0).start()
    own_copy.start()

    tok_rows = x_ref[...].astype(F32)
    for i in range(n_draft):
        tok_v[i] = jnp.broadcast_to(to_col(tok_rows[i:i + 1]), (seqs, 128)).astype(jnp.int32) - me * vocab
    hid_copy.wait()

    @pl.loop(0, n_tiles)
    def _(tile):
        slot = lax.rem(tile, 2)
        w_copy(tile, slot).wait()

        @pl.when(tile + 1 < n_tiles)
        def _():
            w_copy(tile + 1, 1 - slot).start()

        @pl.loop(0, n_pos)
        def _(i):
            z_v[i, :, pl.ds(pl.multiple_of(tile * NT, NT), NT)] = INV_TEMP * jnp.dot(
                hid_v[i], w_v[slot], preferred_element_type=F32)

    @pl.loop(0, n_peers)
    def _(group):
        def one(i, rows):
            z = z_v[i, rows_of(group), :]
            m = jnp.max(z, axis=1, keepdims=True)
            s = jnp.sum(jnp.exp(z - m), axis=1, keepdims=True)
            return rows[0] + spread(m, 128, i * n_loc), rows[1] + spread(s, 128, i * n_loc)

        zero = jnp.zeros((1, 128), F32)
        m_row, s_row = lax.fori_loop(0, n_pos, one, (zero, zero))
        stat_out[group] = jnp.concatenate([m_row, s_row], axis=0)

    stat_in[me] = stat_out[me]
    for k in others:
        scatter_to(stat_out, stat_in, so_send, so_recv, *send_peer(k)).start()
    for k in (4, 5):
        q_to(0, k).start()
    await_all(stat_in, so_send, so_recv)
    top = stat_in[0, 0:1, :]
    for k in range(1, n_peers):
        top = jnp.maximum(top, stat_in[k, 0:1, :])
    total = jnp.zeros((1, 128), F32)
    for k in range(n_peers):
        total += stat_in[k, 1:2, :] * jnp.exp(stat_in[k, 0:1, :] - top)
    used = lax.broadcasted_iota(jnp.int32, (1, 128), 1) < n_pos * n_loc
    norm_v[me] = jnp.concatenate([top, 1.0 / jnp.where(used, total, 1.0)], axis=0)
    for k in others:
        share_to(norm_v, n_send, n_recv, *send_peer(k)).start()
    for k in range(6, 15):
        q_to(0, k).start()
    for k in range(11):
        q_to(1, k).start()
    await_all(norm_v, n_send, n_recv)

    def probs(i, group):
        norm = norm_v[group]
        m, r = gather(norm[0:1], i * n_loc, n_loc), gather(norm[1:2], i * n_loc, n_loc)
        return jnp.exp(z_v[i, rows_of(group), :] - m) * r

    @pl.loop(0, n_peers)
    def _(group):
        bonus_ref[rows_of(group), :] = probs(n_draft, group)

    def cell(i, group):
        rows = rows_of(group)
        p, q, tok = probs(i, group), ex_ref[i, rows, :], tok_v[i, rows, 0:1]
        hit = lax.broadcasted_iota(jnp.int32, (n_loc, vocab), 1) == tok
        p_pick = jnp.sum(jnp.where(hit, p, 0.0), axis=1, keepdims=True)
        q_pick = jnp.sum(jnp.where(hit, q, 0.0), axis=1, keepdims=True)
        excess = jnp.maximum(p - q, 0.0)
        ex_ref[i, rows, :] = excess
        owned = (tok >= 0) & (tok < vocab)
        accept = jnp.where(owned, jnp.minimum(1.0, p_pick / jnp.where(owned, q_pick, 1.0)), 0.0)
        return jnp.sum(excess, axis=1, keepdims=True), accept

    def absorb_early(group):
        def one(i, rows):
            z, a = cell(i, group)
            return rows[0] + spread(z, 128, i * n_loc), rows[1] + spread(a, 128, i * n_loc)

        zero = jnp.zeros((1, 128), F32)
        z_row, a_row = lax.fori_loop(0, n_early, one, (zero, zero))
        sum_out[group] = jnp.concatenate([z_row, a_row], axis=0)

    own_copy.wait()
    absorb_early(me)
    sum_in[me] = sum_out[me]

    @pl.loop(0, n_peers - 1)
    def _(k):
        plane, core = recv_peer(k)
        group = plane * nb + core
        q_from(0, group).wait_recv()
        absorb_early(group)
        scatter_to(sum_out, sum_in, zo_send, zo_recv, plane, core).start()

    for k in range(11, 15):
        q_to(1, k).start()

    def absorb_late(group, rows):
        z, a = cell(n_early, group)
        return rows[0] + spread(z, seqs, group * n_loc), rows[1] + spread(a, seqs, group * n_loc)

    def arrived(k, rows):
        plane, core = recv_peer(k)
        q_from(1, plane * nb + core).wait_recv()
        return absorb_late(plane * nb + core, rows)

    zero = jnp.zeros((1, seqs), F32)
    rows = lax.fori_loop(0, 11, arrived, absorb_late(me, (zero, zero)))
    await_all(sum_in, zo_send, zo_recv)
    total = sum_in[0]
    for k in range(1, n_peers):
        total += sum_in[k]
    early_ref[me] = total
    rows = arrived(11, rows)
    for k in others:
        share_to(early_ref, e_send, e_recv, *send_peer(k)).start()
    rows = lax.fori_loop(12, 15, arrived, rows)

    late_ref[me] = jnp.concatenate(rows, axis=0)
    for k in others:
        q_to(0, k).wait_send()
        q_to(1, k).wait_send()
    for k in others:
        share_to(late_ref, l_send, l_recv, *send_peer(k)).start()
    await_all(early_ref, e_send, e_recv)
    await_all(late_ref, l_send, l_recv)
    for k in others:
        plane, core = send_peer(k)
        scatter_to(stat_out, stat_in, so_send, so_recv, plane, core).wait_send()
        share_to(norm_v, n_send, n_recv, plane, core).wait_send()
        scatter_to(sum_out, sum_in, zo_send, zo_recv, plane, core).wait_send()
        share_to(early_ref, e_send, e_recv, plane, core).wait_send()
        share_to(late_ref, l_send, l_recv, plane, core).wait_send()


SLOTS = 4


def output_kernel(n_peers, ex_ref, bonus_ref, early_ref, late_ref, res_ref, bonus_out, accept_ref, expected_ref,
                  stage, stage_sem, bonus_sem):
    n_draft, seqs, vocab = ex_ref.shape
    n_loc, half = seqs // n_peers, seqs // 2
    bonus_copy = pltpu.make_async_copy(bonus_ref, bonus_out, bonus_sem)
    bonus_copy.start()

    late = late_ref[0]
    for k in range(1, n_peers):
        late += late_ref[k]
    lane = lax.broadcasted_iota(jnp.int32, (n_peers, 128), 1)
    mine = (lax.broadcasted_iota(jnp.int32, (n_peers, seqs), 1) // n_loc
            == lax.broadcasted_iota(jnp.int32, (n_peers, seqs), 0))

    def by_position(which):
        table = jnp.concatenate([early_ref[g, which:which + 1, :] for g in range(n_peers)], axis=0)
        out = jnp.broadcast_to(late[which:which + 1], (8, seqs))
        for i in range(n_draft - 1):
            x = pltpu.roll(table, (128 - n_loc * i) % 128, 1)
            x = jnp.where(lane < n_loc, x, 0.0)
            shift = n_loc
            while shift < 128:
                x = x + pltpu.roll(x, shift, 1)
                shift *= 2
            x = jnp.concatenate([x] * (seqs // 128), axis=1)
            row = jnp.sum(jnp.where(mine, x, 0.0), axis=0, keepdims=True)
            out = jnp.where(lax.broadcasted_iota(jnp.int32, (8, seqs), 0) == i, row, out)
        return out

    inv = 1.0 / by_position(0)

    def out_copy(k, slot):
        i, h = k // 2, lax.rem(k, 2)
        return pltpu.make_async_copy(
            stage.at[slot], res_ref.at[i, pl.ds(pl.multiple_of(h * half, half), half), :], stage_sem.at[slot])

    @pl.loop(0, 2 * n_draft)
    def _(k):
        i, h, slot = k // 2, lax.rem(k, 2), lax.rem(k, SLOTS)
        row = get_row(inv, i)
        col = to_col(jnp.where(h == 0, row[:, :half], row[:, half:]))

        @pl.when(k >= SLOTS)
        def _():
            out_copy(k - SLOTS, slot).wait()

        @pl.loop(0, vocab // NT)
        def _(t):
            cols = pl.ds(pl.multiple_of(t * NT, NT), NT)
            stage[slot, :, cols] = ex_ref[i, pl.ds(pl.multiple_of(h * half, half), half), cols] * col

        out_copy(k, slot).start()

    accept = by_position(1)[:n_draft]
    accept_ref[...] = accept
    prod = accept[0:1]
    expected = prod
    for i in range(1, n_draft):
        prod = prod * accept[i:i + 1]
        expected += prod
    expected_ref[...] = expected
    for k in range(2 * n_draft - SLOTS, 2 * n_draft):
        out_copy(k, k % SLOTS).wait()
    bonus_copy.wait()


def solution(mesh):
    na, nb = mesh.shape["tpa"], mesh.shape["tpb"]
    n_peers = na * nb
    any_spec = pl.BlockSpec(memory_space=pl.ANY)
    vmem_spec = pl.BlockSpec(memory_space=pltpu.VMEM)

    def local_step(hidden, w_head, q_draft, x_draft):
        seqs, n_pos, depth = hidden.shape
        vocab = w_head.shape[1]
        n_loc, n_draft, _ = q_draft.shape
        dims = (n_pos, seqs, depth, vocab, n_loc, na, nb)
        dma = pltpu.SemaphoreType.DMA
        small = pltpu.VMEM((n_peers, 2, 128), F32)
        ex, bonus, early, late = pl.pallas_call(
            functools.partial(exchange_kernel, dims),
            out_shape=(pltpu.VMEM((n_draft, seqs, vocab), F32), pltpu.VMEM((seqs, vocab), F32),
                       small, pltpu.VMEM((n_peers, 2, seqs), F32)),
            in_specs=[any_spec, any_spec, any_spec, vmem_spec],
            out_specs=(vmem_spec,) * 4,
            scratch_shapes=[
                pltpu.VMEM((n_pos, seqs, depth), jnp.bfloat16),
                pltpu.VMEM((2, depth, NT), jnp.bfloat16),
                pltpu.VMEM((n_pos, seqs, vocab), F32),
                pltpu.VMEM((n_draft, seqs, 128), jnp.int32),
                small, small, small, small, small,
                dma, dma((2,)), dma,
            ] + [dma((n_peers,))] * 14,
            compiler_params=pltpu.CompilerParams(collective_id=0, has_side_effects=True, vmem_limit_bytes=38 * 2**20),
            name="exchange",
        )(hidden.transpose(1, 0, 2), w_head, q_draft.transpose(1, 0, 2), x_draft.T)
        res, bonus_out, accept, expected = pl.pallas_call(
            functools.partial(output_kernel, n_peers),
            out_shape=(jax.ShapeDtypeStruct((n_draft, seqs, vocab), F32), jax.ShapeDtypeStruct((seqs, vocab), F32),
                       jax.ShapeDtypeStruct((n_draft, seqs), F32), jax.ShapeDtypeStruct((1, seqs), F32)),
            in_specs=[vmem_spec] * 4,
            out_specs=(any_spec, any_spec, vmem_spec, vmem_spec),
            scratch_shapes=[pltpu.VMEM((SLOTS, seqs // 2, vocab), F32), dma((SLOTS,)), dma],
            compiler_params=pltpu.CompilerParams(vmem_limit_bytes=12 * 2**20),
            name="output",
        )(ex, bonus, early, late)
        return accept.T, expected.reshape(seqs), res.transpose(1, 0, 2), bonus_out

    return jax.shard_map(
        local_step, mesh=mesh,
        in_specs=(P("dp", None, None), P(None, VOCAB_AXES), P(("dp",) + VOCAB_AXES, None, None), P("dp", None)),
        out_specs=(P("dp", None), P("dp"), P("dp", None, VOCAB_AXES), P("dp", VOCAB_AXES)),
        check_vma=False)
```

```python
import functools

import jax
import jax.numpy as jnp
from jax import lax
from jax.experimental import pallas as pl
from jax.experimental.pallas import tpu as pltpu
from jax.sharding import PartitionSpec as P

INV_TEMP = 1.25
VOCAB_AXES = ("tpa", "tpb")
MESH = pl.DeviceIdType.MESH
F32 = jnp.float32
SEND = ((3, 3, 0, 0), (1, 0, 3, 2), (2, 2, 1, 1))
RECV = ((3, 0, 3, 0), (2, 3, 0, 1), (1, 2, 1, 2))
CORE_OFFSETS = (0, 2, 1, 3)
NT = 512


def pick(index, values):
    out = jnp.int32(values[-1])
    for k in range(len(values) - 2, -1, -1):
        out = jnp.where(index == k, jnp.int32(values[k]), out)
    return out


def diag(n):
    return lax.broadcasted_iota(jnp.int32, (n, n), 0) == lax.broadcasted_iota(jnp.int32, (n, n), 1)


def to_col(row):
    return jnp.sum(jnp.where(diag(row.shape[1]), row, 0.0), axis=1, keepdims=True)


def get_row(rows, i):
    return jnp.sum(jnp.where(lax.broadcasted_iota(jnp.int32, rows.shape, 0) == i, rows, 0.0), axis=0, keepdims=True)


def lanes(n, first, rows):
    return (lax.broadcasted_iota(jnp.int32, (rows, n), 1)
            == lax.broadcasted_iota(jnp.int32, (rows, n), 0) + first)


def spread(col, n, first):
    return jnp.sum(jnp.where(lanes(n, first, col.shape[0]), col, 0.0), axis=0, keepdims=True)


def gather(row, first, rows):
    return jnp.sum(jnp.where(lanes(row.shape[1], first, rows), row, 0.0), axis=1, keepdims=True)


def exchange_kernel(dims, hid_ref, w_ref, q_ref, x_ref, ex_ref, bonus_ref, early_ref, late_ref,
                    hid_v, w_v, z_v, tok_v, stat_out, stat_1, stat_2, norm_v, sum_out, sum_1, sum_2, hid_sem, w_sem, own_sem,
                    q_send, q_recv, r_recv, l_send, l_recv,
                    a1_send, a1_recv, a2_send, a2_recv, a3_send, a3_recv, b1_send, b1_recv, b2_send, b2_recv, b3_send, b3_recv):
    n_pos, seqs, depth, vocab, n_loc, na, nb = dims
    n_draft = n_pos - 1
    n_early = n_draft - 1
    n_peers = na * nb
    n_tiles = vocab // NT
    others = range(n_peers - 1)
    dp, za, tb = lax.axis_index("dp"), lax.axis_index("tpa"), lax.axis_index("tpb")
    me = za * nb + tb

    def send_peer(k):
        inner = (za == 1) | (za == 2)
        if k < 3:
            end, mid = (pick(za, SEND[0]), CORE_OFFSETS[k]), (za, k + 1)
        else:
            mid = (pick(za, SEND[(k - 3) // nb]), CORE_OFFSETS[(k - 3) % nb])
            end = (pick(za, SEND[k // nb]), CORE_OFFSETS[k % nb]) if k < 12 else (za, k - 11)
        plane = jnp.where(inner, mid[0], end[0])
        return plane, lax.rem(tb + jnp.where(inner, mid[1], end[1]), nb)

    def recv_peer(k):
        step, off = (k - 3) // nb, lax.rem(jnp.int32(k) + 1, nb)
        plane = jnp.where(k < 3, za, jnp.where(step == 0, pick(za, RECV[0]),
                          jnp.where(step == 1, pick(za, RECV[1]), pick(za, RECV[2]))))
        off = jnp.where(k < 3, k + 1, nb - pick(off, CORE_OFFSETS))
        return plane, lax.rem(tb + off, nb)

    def rows_of(group):
        return pl.ds(pl.multiple_of(group * n_loc, 8), n_loc)

    def q_copy(part, plane, core, own_group, column):
        i0, ni = (0, n_early) if part == 0 else (n_early, 1)
        recv = q_recv.at[own_group // nb] if part == 0 else r_recv.at[own_group]
        return pltpu.make_async_remote_copy(
            src_ref=q_ref.at[pl.ds(i0, ni), :, pl.ds(pl.multiple_of(column * vocab, 128), vocab)],
            dst_ref=ex_ref.at[pl.ds(i0, ni), rows_of(own_group), :],
            send_sem=q_send, recv_sem=recv,
            device_id=(dp, plane, core), device_id_type=MESH)

    def q_to(part, k):
        plane, core = send_peer(k)
        return q_copy(part, plane, core, me, plane * nb + core)

    def q_from_plane(plane, count):
        rows = ex_ref.at[pl.ds(0, n_early), pl.ds(0, count * n_loc), :]
        pltpu.make_async_copy(rows, rows, q_recv.at[plane]).wait()

    def q_from(group):
        return q_copy(1, za, tb, group, 0)

    def small(src, dst, send, recv, src_slot, dst_slot, plane, core):
        return pltpu.make_async_remote_copy(
            src_ref=src.at[src_slot], dst_ref=dst.at[dst_slot], send_sem=send, recv_sem=recv,
            device_id=(dp, plane, core), device_id_type=MESH)

    def await_slots(ref, sem, count):
        part = ref.at[pl.ds(0, count)]
        pltpu.make_async_copy(part, part, sem).wait()

    def in_plane(src, dst, send, recv, scatter):
        cores = [lax.rem(tb + k, nb) for k in range(1, nb)]
        return [small(src, dst, send, recv, core if scatter else tb, tb, za, core) for core in cores]

    def across(ref, send, recv):
        planes = [lax.rem(za + k, na) for k in range(1, na)]
        return [small(ref, ref, send, recv, za, za, plane, tb) for plane in planes]

    def late_to(k):
        plane, core = send_peer(k)
        return small(late_ref, late_ref, l_send, l_recv, me, me, plane, core)

    def start(copies):
        for copy in copies:
            copy.start()

    def combine(ref):
        top = ref[0, 0:4]
        for k in range(1, 4):
            top = jnp.maximum(top, ref[k, 0:4])
        total = ref[0, 4:8] * jnp.exp(ref[0, 0:4] - top)
        for k in range(1, 4):
            total += ref[k, 4:8] * jnp.exp(ref[k, 0:4] - top)
        return top, total

    def add(ref):
        return (ref[0] + ref[1]) + (ref[2] + ref[3])

    def put(tile, plane, first, second):
        row = lax.broadcasted_iota(jnp.int32, tile.shape, 0)
        return jnp.where(row == plane, first, jnp.where(row == na + plane, second, tile))

    def w_copy(tile, slot):
        return pltpu.make_async_copy(w_ref.at[:, pl.ds(pl.multiple_of(tile * NT, NT), NT)], w_v.at[slot], w_sem.at[slot])

    hid_copy = pltpu.make_async_copy(hid_ref, hid_v, hid_sem)
    own_copy = pltpu.make_async_copy(
        q_ref.at[:, :, pl.ds(pl.multiple_of(me * vocab, 128), vocab)], ex_ref.at[:, rows_of(me), :], own_sem)

    barrier = pltpu.get_barrier_semaphore()
    for k in range(1, n_peers):
        pl.semaphore_signal(barrier, inc=1, device_id=(dp, lax.rem(za + k // nb, na), lax.rem(tb + k % nb, nb)),
                            device_id_type=MESH)
    pl.semaphore_wait(barrier, n_peers - 1)

    for k in range(4):
        q_to(0, k).start()
    hid_copy.start()
    w_copy(0, 0).start()
    own_copy.start()

    tok_rows = x_ref[...].astype(F32)
    for i in range(n_draft):
        tok_v[i] = jnp.broadcast_to(to_col(tok_rows[i:i + 1]), (seqs, 128)).astype(jnp.int32) - me * vocab
    hid_copy.wait()

    @pl.loop(0, n_tiles)
    def _(tile):
        slot = lax.rem(tile, 2)
        w_copy(tile, slot).wait()

        @pl.when(tile + 1 < n_tiles)
        def _():
            w_copy(tile + 1, 1 - slot).start()

        @pl.loop(0, n_pos)
        def _(i):
            z_v[i, :, pl.ds(pl.multiple_of(tile * NT, NT), NT)] = INV_TEMP * jnp.dot(
                hid_v[i], w_v[slot], preferred_element_type=F32)

    @pl.loop(0, nb)
    def _(core):
        def plane_rows(plane, tile):
            def one(i, rows):
                z = z_v[i, rows_of(plane * nb + core), :]
                m = jnp.max(z, axis=1, keepdims=True)
                s = jnp.sum(jnp.exp(z - m), axis=1, keepdims=True)
                return rows[0] + spread(m, 128, i * n_loc), rows[1] + spread(s, 128, i * n_loc)

            zero = jnp.zeros((1, 128), F32)
            return put(tile, plane, *lax.fori_loop(0, n_pos, one, (zero, zero)))

        stat_out[core] = lax.fori_loop(0, na, plane_rows, jnp.zeros((8, 128), F32))

    stat_1[tb] = stat_out[tb]
    start(in_plane(stat_out, stat_1, a1_send, a1_recv, True))
    await_slots(stat_1, a1_recv, 3)
    stat_2[za] = jnp.concatenate(combine(stat_1), axis=0)
    start(across(stat_2, a2_send, a2_recv))
    for k in (4, 5):
        q_to(0, k).start()
    await_slots(stat_2, a2_recv, 3)
    top, total = combine(stat_2)
    used = lax.broadcasted_iota(jnp.int32, (4, 128), 1) < n_pos * n_loc
    norm_v[tb] = jnp.concatenate([top, 1.0 / jnp.where(used, total, 1.0)], axis=0)
    start(in_plane(norm_v, norm_v, a3_send, a3_recv, False))
    for k in range(6, 15):
        q_to(0, k).start()
    for k in range(11):
        q_to(1, k).start()
    await_slots(norm_v, a3_recv, 3)

    def probs(i, group):
        norm, plane = norm_v[lax.rem(group, nb)], group // nb
        m = gather(get_row(norm, plane), i * n_loc, n_loc)
        r = gather(get_row(norm, na + plane), i * n_loc, n_loc)
        return jnp.exp(z_v[i, rows_of(group), :] - m) * r

    @pl.loop(0, n_peers)
    def _(group):
        bonus_ref[rows_of(group), :] = probs(n_draft, group)

    def cell(i, group):
        rows = rows_of(group)
        p, q, tok = probs(i, group), ex_ref[i, rows, :], tok_v[i, rows, 0:1]
        hit = lax.broadcasted_iota(jnp.int32, (n_loc, vocab), 1) == tok
        p_pick = jnp.sum(jnp.where(hit, p, 0.0), axis=1, keepdims=True)
        q_pick = jnp.sum(jnp.where(hit, q, 0.0), axis=1, keepdims=True)
        excess = jnp.maximum(p - q, 0.0)
        ex_ref[i, rows, :] = excess
        owned = (tok >= 0) & (tok < vocab)
        accept = jnp.where(owned, jnp.minimum(1.0, p_pick / jnp.where(owned, q_pick, 1.0)), 0.0)
        return jnp.sum(excess, axis=1, keepdims=True), accept

    def absorb_early(group):
        def one(i, rows):
            z, a = cell(i, group)
            return rows[0] + spread(z, 128, i * n_loc), rows[1] + spread(a, 128, i * n_loc)

        zero = jnp.zeros((1, 128), F32)
        z_row, a_row = lax.fori_loop(0, n_early, one, (zero, zero))
        core = lax.rem(group, nb)
        sum_out[core] = put(sum_out[core], group // nb, z_row, a_row)

    sum_out[...] = jnp.zeros_like(sum_out)
    own_copy.wait()
    absorb_early(me)

    q_from_plane(za, nb - 1)
    for k in range(1, nb):
        absorb_early(za * nb + lax.rem(tb + k, nb))

    @pl.loop(0, na - 1)
    def _(step):
        plane = jnp.where(step == 0, pick(za, RECV[0]), jnp.where(step == 1, pick(za, RECV[1]), pick(za, RECV[2])))
        q_from_plane(plane, nb)

        @pl.loop(0, nb)
        def _(core):
            absorb_early(plane * nb + core)

    sum_1[tb] = sum_out[tb]
    start(in_plane(sum_out, sum_1, b1_send, b1_recv, True))
    for k in (11, 12):
        q_to(1, k).start()
    await_slots(sum_1, b1_recv, 3)
    sum_2[za] = add(sum_1)
    start(across(sum_2, b2_send, b2_recv))
    for k in (13, 14):
        q_to(1, k).start()

    def absorb_late(group, rows):
        z, a = cell(n_early, group)
        return rows[0] + spread(z, seqs, group * n_loc), rows[1] + spread(a, seqs, group * n_loc)

    def arrived(k, rows):
        plane, core = recv_peer(k)
        q_from(plane * nb + core).wait_recv()
        return absorb_late(plane * nb + core, rows)

    zero = jnp.zeros((1, seqs), F32)
    rows = lax.fori_loop(0, 11, arrived, absorb_late(me, (zero, zero)))
    await_slots(sum_2, b2_recv, 3)
    early_ref[tb] = add(sum_2)
    start(in_plane(early_ref, early_ref, b3_send, b3_recv, False))
    rows = lax.fori_loop(11, 15, arrived, rows)

    late_ref[me] = jnp.concatenate(rows, axis=0)
    sent = q_ref.at[:, :, pl.ds(0, (n_peers - 1) * vocab)]
    pltpu.make_async_copy(sent, sent, q_send).wait()
    for k in others:
        late_to(k).start()
    await_slots(early_ref, b3_recv, 3)
    await_slots(late_ref, l_recv, n_peers - 1)
    await_slots(late_ref, l_send, n_peers - 1)
    for ref, sem in ((stat_1, a1_send), (stat_2, a2_send), (norm_v, a3_send), (sum_1, b1_send), (sum_2, b2_send),
                     (early_ref, b3_send)):
        await_slots(ref, sem, 3)


SLOTS = 4


def output_kernel(na, nb, ex_ref, bonus_ref, early_ref, late_ref, res_ref, bonus_out, accept_ref, expected_ref,
                  stage, stage_sem, bonus_sem):
    n_draft, seqs, vocab = ex_ref.shape
    n_peers = na * nb
    n_loc, half = seqs // n_peers, seqs // 2
    bonus_copy = pltpu.make_async_copy(bonus_ref, bonus_out, bonus_sem)
    bonus_copy.start()

    late = late_ref[0]
    for k in range(1, n_peers):
        late += late_ref[k]
    lane = lax.broadcasted_iota(jnp.int32, (n_peers, 128), 1)
    mine = (lax.broadcasted_iota(jnp.int32, (n_peers, seqs), 1) // n_loc
            == lax.broadcasted_iota(jnp.int32, (n_peers, seqs), 0))

    def by_position(which):
        table = jnp.concatenate(
            [early_ref[g % nb, na * which + g // nb:na * which + g // nb + 1, :] for g in range(n_peers)], axis=0)
        out = jnp.broadcast_to(late[which:which + 1], (8, seqs))
        for i in range(n_draft - 1):
            x = pltpu.roll(table, (128 - n_loc * i) % 128, 1)
            x = jnp.where(lane < n_loc, x, 0.0)
            shift = n_loc
            while shift < 128:
                x = x + pltpu.roll(x, shift, 1)
                shift *= 2
            x = jnp.concatenate([x] * (seqs // 128), axis=1)
            row = jnp.sum(jnp.where(mine, x, 0.0), axis=0, keepdims=True)
            out = jnp.where(lax.broadcasted_iota(jnp.int32, (8, seqs), 0) == i, row, out)
        return out

    inv = 1.0 / by_position(0)

    def out_copy(k, slot):
        i, h = k // 2, lax.rem(k, 2)
        return pltpu.make_async_copy(
            stage.at[slot], res_ref.at[i, pl.ds(pl.multiple_of(h * half, half), half), :], stage_sem.at[slot])

    @pl.loop(0, 2 * n_draft)
    def _(k):
        i, h, slot = k // 2, lax.rem(k, 2), lax.rem(k, SLOTS)
        row = get_row(inv, i)
        col = to_col(jnp.where(h == 0, row[:, :half], row[:, half:]))

        @pl.when(k >= SLOTS)
        def _():
            out_copy(k - SLOTS, slot).wait()

        @pl.loop(0, vocab // NT)
        def _(t):
            cols = pl.ds(pl.multiple_of(t * NT, NT), NT)
            stage[slot, :, cols] = ex_ref[i, pl.ds(pl.multiple_of(h * half, half), half), cols] * col

        out_copy(k, slot).start()

    accept = by_position(1)[:n_draft]
    accept_ref[...] = accept
    prod = accept[0:1]
    expected = prod
    for i in range(1, n_draft):
        prod = prod * accept[i:i + 1]
        expected += prod
    expected_ref[...] = expected
    for k in range(2 * n_draft - SLOTS, 2 * n_draft):
        out_copy(k, k % SLOTS).wait()
    bonus_copy.wait()


def solution(mesh):
    na, nb = mesh.shape["tpa"], mesh.shape["tpb"]
    n_peers = na * nb
    any_spec = pl.BlockSpec(memory_space=pl.ANY)
    vmem_spec = pl.BlockSpec(memory_space=pltpu.VMEM)

    def local_step(hidden, w_head, q_draft, x_draft):
        seqs, n_pos, depth = hidden.shape
        vocab = w_head.shape[1]
        n_loc, n_draft, _ = q_draft.shape
        dims = (n_pos, seqs, depth, vocab, n_loc, na, nb)
        dma = pltpu.SemaphoreType.DMA
        small = pltpu.VMEM((4, 8, 128), F32)
        ex, bonus, early, late = pl.pallas_call(
            functools.partial(exchange_kernel, dims),
            out_shape=(pltpu.VMEM((n_draft, seqs, vocab), F32), pltpu.VMEM((seqs, vocab), F32),
                       small, pltpu.VMEM((n_peers, 2, seqs), F32)),
            in_specs=[any_spec, any_spec, any_spec, vmem_spec],
            out_specs=(vmem_spec,) * 4,
            scratch_shapes=[
                pltpu.VMEM((n_pos, seqs, depth), jnp.bfloat16),
                pltpu.VMEM((2, depth, NT), jnp.bfloat16),
                pltpu.VMEM((n_pos, seqs, vocab), F32),
                pltpu.VMEM((n_draft, seqs, 128), jnp.int32),
                small, small, small, small, small, small, small,
                dma, dma((2,)), dma, dma, dma((na,)), dma((n_peers,)),
            ] + [dma] * 14,
            compiler_params=pltpu.CompilerParams(collective_id=0, has_side_effects=True, vmem_limit_bytes=38 * 2**20),
            name="exchange",
        )(hidden.transpose(1, 0, 2), w_head, q_draft.transpose(1, 0, 2), x_draft.T)
        res, bonus_out, accept, expected = pl.pallas_call(
            functools.partial(output_kernel, na, nb),
            out_shape=(jax.ShapeDtypeStruct((n_draft, seqs, vocab), F32), jax.ShapeDtypeStruct((seqs, vocab), F32),
                       jax.ShapeDtypeStruct((n_draft, seqs), F32), jax.ShapeDtypeStruct((1, seqs), F32)),
            in_specs=[vmem_spec] * 4,
            out_specs=(any_spec, any_spec, vmem_spec, vmem_spec),
            scratch_shapes=[pltpu.VMEM((SLOTS, seqs // 2, vocab), F32), dma((SLOTS,)), dma],
            compiler_params=pltpu.CompilerParams(vmem_limit_bytes=12 * 2**20),
            name="output",
        )(ex, bonus, early, late)
        return accept.T, expected.reshape(seqs), res.transpose(1, 0, 2), bonus_out

    return jax.shard_map(
        local_step, mesh=mesh,
        in_specs=(P("dp", None, None), P(None, VOCAB_AXES), P(("dp",) + VOCAB_AXES, None, None), P("dp", None)),
        out_specs=(P("dp", None), P("dp"), P("dp", None, VOCAB_AXES), P("dp", VOCAB_AXES)),
        check_vma=False)
```

```python
import functools

import jax
import jax.numpy as jnp
from jax import lax
from jax.experimental import pallas as pl
from jax.experimental.pallas import tpu as pltpu
from jax.sharding import PartitionSpec as P

INV_TEMP = 1.25
VOCAB_AXES = ("tpa", "tpb")
MESH = pl.DeviceIdType.MESH
F32 = jnp.float32
SEND = ((3, 3, 0, 0), (1, 0, 3, 2), (2, 2, 1, 1))
RECV = ((3, 0, 3, 0), (2, 3, 0, 1), (1, 2, 1, 2))
CORE_OFFSETS = (0, 2, 1, 3)
NT = 512


def pick(index, values):
    out = jnp.int32(values[-1])
    for k in range(len(values) - 2, -1, -1):
        out = jnp.where(index == k, jnp.int32(values[k]), out)
    return out


def diag(n):
    return lax.broadcasted_iota(jnp.int32, (n, n), 0) == lax.broadcasted_iota(jnp.int32, (n, n), 1)


def to_col(row):
    return jnp.sum(jnp.where(diag(row.shape[1]), row, 0.0), axis=1, keepdims=True)


def get_row(rows, i):
    return jnp.sum(jnp.where(lax.broadcasted_iota(jnp.int32, rows.shape, 0) == i, rows, 0.0), axis=0, keepdims=True)


def lanes(n, first, rows):
    return (lax.broadcasted_iota(jnp.int32, (rows, n), 1)
            == lax.broadcasted_iota(jnp.int32, (rows, n), 0) + first)


def spread(col, n, first):
    return jnp.sum(jnp.where(lanes(n, first, col.shape[0]), col, 0.0), axis=0, keepdims=True)


def gather(row, first, rows):
    return jnp.sum(jnp.where(lanes(row.shape[1], first, rows), row, 0.0), axis=1, keepdims=True)


def exchange_kernel(dims, hid_ref, w_ref, q_ref, x_ref, ex_ref, bonus_ref, early_ref, late_ref,
                    hid_v, w_v, z_v, x_v, tok_v, stat_out, stat_1, stat_2, norm_v, sum_out, sum_1, sum_2, hid_sem, w_sem, own_sem, x_sem,
                    q_send, q_recv, r_recv, l_send, l_recv,
                    a1_send, a1_recv, a2_send, a2_recv, a3_send, a3_recv, b1_send, b1_recv, b2_send, b2_recv, b3_send, b3_recv):
    n_pos, seqs, depth, vocab, n_loc, na, nb = dims
    n_draft = n_pos - 1
    n_early = n_draft - 1
    n_peers = na * nb
    n_tiles = vocab // NT
    others = range(n_peers - 1)
    dp, za, tb = lax.axis_index("dp"), lax.axis_index("tpa"), lax.axis_index("tpb")
    me = za * nb + tb

    def send_peer(k):
        inner = (za == 1) | (za == 2)
        if k < 3:
            end, mid = (pick(za, SEND[0]), CORE_OFFSETS[k]), (za, k + 1)
        else:
            mid = (pick(za, SEND[(k - 3) // nb]), CORE_OFFSETS[(k - 3) % nb])
            end = (pick(za, SEND[k // nb]), CORE_OFFSETS[k % nb]) if k < 12 else (za, k - 11)
        plane = jnp.where(inner, mid[0], end[0])
        return plane, lax.rem(tb + jnp.where(inner, mid[1], end[1]), nb)

    def recv_peer(k):
        step, off = (k - 3) // nb, lax.rem(jnp.int32(k) + 1, nb)
        plane = jnp.where(k < 3, za, jnp.where(step == 0, pick(za, RECV[0]),
                          jnp.where(step == 1, pick(za, RECV[1]), pick(za, RECV[2]))))
        off = jnp.where(k < 3, k + 1, nb - pick(off, CORE_OFFSETS))
        return plane, lax.rem(tb + off, nb)

    def rows_of(group):
        return pl.ds(pl.multiple_of(group * n_loc, 8), n_loc)

    def q_copy(part, plane, core, own_group, column):
        i0, ni = (0, n_early) if part == 0 else (n_early, 1)
        recv = q_recv.at[own_group // nb] if part == 0 else r_recv.at[own_group]
        return pltpu.make_async_remote_copy(
            src_ref=q_ref.at[pl.ds(i0, ni), :, pl.ds(pl.multiple_of(column * vocab, 128), vocab)],
            dst_ref=ex_ref.at[pl.ds(i0, ni), rows_of(own_group), :],
            send_sem=q_send, recv_sem=recv,
            device_id=(dp, plane, core), device_id_type=MESH)

    def q_to(part, k):
        plane, core = send_peer(k)
        return q_copy(part, plane, core, me, plane * nb + core)

    def q_from_plane(plane, count):
        rows = ex_ref.at[pl.ds(0, n_early), pl.ds(0, count * n_loc), :]
        pltpu.make_async_copy(rows, rows, q_recv.at[plane]).wait()

    def q_from(group):
        return q_copy(1, za, tb, group, 0)

    def small(src, dst, send, recv, src_slot, dst_slot, plane, core):
        return pltpu.make_async_remote_copy(
            src_ref=src.at[src_slot], dst_ref=dst.at[dst_slot], send_sem=send, recv_sem=recv,
            device_id=(dp, plane, core), device_id_type=MESH)

    def await_slots(ref, sem, count):
        part = ref.at[pl.ds(0, count)]
        pltpu.make_async_copy(part, part, sem).wait()

    def in_plane(src, dst, send, recv, scatter):
        cores = [lax.rem(tb + k, nb) for k in range(1, nb)]
        return [small(src, dst, send, recv, core if scatter else tb, tb, za, core) for core in cores]

    def across(ref, send, recv):
        planes = [lax.rem(za + k, na) for k in range(1, na)]
        return [small(ref, ref, send, recv, za, za, plane, tb) for plane in planes]

    def late_to(k):
        plane, core = send_peer(k)
        return small(late_ref, late_ref, l_send, l_recv, me, me, plane, core)

    def start(copies):
        for copy in copies:
            copy.start()

    def combine(ref):
        top = ref[0, 0:4]
        for k in range(1, 4):
            top = jnp.maximum(top, ref[k, 0:4])
        total = ref[0, 4:8] * jnp.exp(ref[0, 0:4] - top)
        for k in range(1, 4):
            total += ref[k, 4:8] * jnp.exp(ref[k, 0:4] - top)
        return top, total

    def add(ref):
        return (ref[0] + ref[1]) + (ref[2] + ref[3])

    def put(tile, plane, first, second):
        row = lax.broadcasted_iota(jnp.int32, tile.shape, 0)
        return jnp.where(row == plane, first, jnp.where(row == na + plane, second, tile))

    def w_copy(tile, slot):
        return pltpu.make_async_copy(w_ref.at[:, pl.ds(pl.multiple_of(tile * NT, NT), NT)], w_v.at[slot], w_sem.at[slot])

    hid_copy = pltpu.make_async_copy(hid_ref, hid_v, hid_sem)
    x_copy = pltpu.make_async_copy(x_ref, x_v, x_sem)
    own_copy = pltpu.make_async_copy(
        q_ref.at[:, :, pl.ds(pl.multiple_of(me * vocab, 128), vocab)], ex_ref.at[:, rows_of(me), :], own_sem)

    barrier = pltpu.get_barrier_semaphore()
    for k in range(1, n_peers):
        pl.semaphore_signal(barrier, inc=1, device_id=(dp, lax.rem(za + k // nb, na), lax.rem(tb + k % nb, nb)),
                            device_id_type=MESH)
    pl.semaphore_wait(barrier, n_peers - 1)

    for k in range(4):
        q_to(0, k).start()
    x_copy.start()
    hid_copy.start()
    w_copy(0, 0).start()
    own_copy.start()

    x_copy.wait()
    tok_rows = x_v[...].astype(F32)
    for i in range(n_draft):
        tok_v[i] = jnp.broadcast_to(to_col(tok_rows[i:i + 1]), (seqs, 128)).astype(jnp.int32) - me * vocab
    hid_copy.wait()

    @pl.loop(0, n_tiles)
    def _(tile):
        slot = lax.rem(tile, 2)
        w_copy(tile, slot).wait()

        @pl.when(tile + 1 < n_tiles)
        def _():
            w_copy(tile + 1, 1 - slot).start()

        @pl.loop(0, n_pos)
        def _(i):
            z_v[i, :, pl.ds(pl.multiple_of(tile * NT, NT), NT)] = INV_TEMP * jnp.dot(
                hid_v[i], w_v[slot], preferred_element_type=F32)

    @pl.loop(0, nb)
    def _(core):
        def plane_rows(plane, tile):
            def one(i, rows):
                z = z_v[i, rows_of(plane * nb + core), :]
                m = jnp.max(z, axis=1, keepdims=True)
                s = jnp.sum(jnp.exp(z - m), axis=1, keepdims=True)
                return rows[0] + spread(m, 128, i * n_loc), rows[1] + spread(s, 128, i * n_loc)

            zero = jnp.zeros((1, 128), F32)
            return put(tile, plane, *lax.fori_loop(0, n_pos, one, (zero, zero)))

        stat_out[core] = lax.fori_loop(0, na, plane_rows, jnp.zeros((8, 128), F32))

    stat_1[tb] = stat_out[tb]
    start(in_plane(stat_out, stat_1, a1_send, a1_recv, True))
    await_slots(stat_1, a1_recv, 3)
    stat_2[za] = jnp.concatenate(combine(stat_1), axis=0)
    start(across(stat_2, a2_send, a2_recv))
    for k in (4, 5):
        q_to(0, k).start()
    await_slots(stat_2, a2_recv, 3)
    top, total = combine(stat_2)
    used = lax.broadcasted_iota(jnp.int32, (4, 128), 1) < n_pos * n_loc
    norm_v[tb] = jnp.concatenate([top, 1.0 / jnp.where(used, total, 1.0)], axis=0)
    start(in_plane(norm_v, norm_v, a3_send, a3_recv, False))
    for k in range(6, 15):
        q_to(0, k).start()
    for k in range(11):
        q_to(1, k).start()
    await_slots(norm_v, a3_recv, 3)

    def probs(i, group):
        norm, plane = norm_v[lax.rem(group, nb)], group // nb
        m = gather(get_row(norm, plane), i * n_loc, n_loc)
        r = gather(get_row(norm, na + plane), i * n_loc, n_loc)
        return jnp.exp(z_v[i, rows_of(group), :] - m) * r

    @pl.loop(0, n_peers)
    def _(group):
        bonus_ref[rows_of(group), :] = probs(n_draft, group)

    def cell(i, group):
        rows = rows_of(group)
        p, q, tok = probs(i, group), ex_ref[i, rows, :], tok_v[i, rows, 0:1]
        hit = lax.broadcasted_iota(jnp.int32, (n_loc, vocab), 1) == tok
        p_pick = jnp.sum(jnp.where(hit, p, 0.0), axis=1, keepdims=True)
        q_pick = jnp.sum(jnp.where(hit, q, 0.0), axis=1, keepdims=True)
        excess = jnp.maximum(p - q, 0.0)
        ex_ref[i, rows, :] = excess
        owned = (tok >= 0) & (tok < vocab)
        accept = jnp.where(owned, jnp.minimum(1.0, p_pick / jnp.where(owned, q_pick, 1.0)), 0.0)
        return jnp.sum(excess, axis=1, keepdims=True), accept

    def absorb_early(group):
        def one(i, rows):
            z, a = cell(i, group)
            return rows[0] + spread(z, 128, i * n_loc), rows[1] + spread(a, 128, i * n_loc)

        zero = jnp.zeros((1, 128), F32)
        z_row, a_row = lax.fori_loop(0, n_early, one, (zero, zero))
        core = lax.rem(group, nb)
        sum_out[core] = put(sum_out[core], group // nb, z_row, a_row)

    sum_out[...] = jnp.zeros_like(sum_out)
    own_copy.wait()
    absorb_early(me)

    q_from_plane(za, nb - 1)
    for k in range(1, nb):
        absorb_early(za * nb + lax.rem(tb + k, nb))

    @pl.loop(0, na - 1)
    def _(step):
        plane = jnp.where(step == 0, pick(za, RECV[0]), jnp.where(step == 1, pick(za, RECV[1]), pick(za, RECV[2])))
        q_from_plane(plane, nb)

        @pl.loop(0, nb)
        def _(core):
            absorb_early(plane * nb + core)

    sum_1[tb] = sum_out[tb]
    start(in_plane(sum_out, sum_1, b1_send, b1_recv, True))
    for k in (11, 12):
        q_to(1, k).start()
    await_slots(sum_1, b1_recv, 3)
    sum_2[za] = add(sum_1)
    start(across(sum_2, b2_send, b2_recv))
    for k in (13, 14):
        q_to(1, k).start()

    def absorb_late(group, rows):
        z, a = cell(n_early, group)
        return rows[0] + spread(z, seqs, group * n_loc), rows[1] + spread(a, seqs, group * n_loc)

    def arrived(k, rows):
        plane, core = recv_peer(k)
        q_from(plane * nb + core).wait_recv()
        return absorb_late(plane * nb + core, rows)

    zero = jnp.zeros((1, seqs), F32)
    rows = lax.fori_loop(0, 11, arrived, absorb_late(me, (zero, zero)))
    await_slots(sum_2, b2_recv, 3)
    early_ref[tb] = add(sum_2)
    start(in_plane(early_ref, early_ref, b3_send, b3_recv, False))
    rows = lax.fori_loop(11, 15, arrived, rows)

    late_ref[me] = jnp.concatenate(rows, axis=0)
    sent = q_ref.at[:, :, pl.ds(0, (n_peers - 1) * vocab)]
    pltpu.make_async_copy(sent, sent, q_send).wait()
    for k in others:
        late_to(k).start()
    await_slots(early_ref, b3_recv, 3)
    await_slots(late_ref, l_recv, n_peers - 1)
    await_slots(late_ref, l_send, n_peers - 1)
    for ref, sem in ((stat_1, a1_send), (stat_2, a2_send), (norm_v, a3_send), (sum_1, b1_send), (sum_2, b2_send),
                     (early_ref, b3_send)):
        await_slots(ref, sem, 3)


SLOTS = 4


def output_kernel(na, nb, ex_ref, bonus_ref, early_ref, late_ref, res_ref, bonus_out, accept_ref, expected_ref,
                  stage, accept_v, expected_v, stage_sem, bonus_sem, small_sem):
    n_draft, seqs, vocab = ex_ref.shape
    n_peers = na * nb
    n_loc, half = seqs // n_peers, seqs // 2
    bonus_copy = pltpu.make_async_copy(bonus_ref, bonus_out, bonus_sem)
    bonus_copy.start()

    late = late_ref[0]
    for k in range(1, n_peers):
        late += late_ref[k]
    lane = lax.broadcasted_iota(jnp.int32, (n_peers, 128), 1)
    mine = (lax.broadcasted_iota(jnp.int32, (n_peers, seqs), 1) // n_loc
            == lax.broadcasted_iota(jnp.int32, (n_peers, seqs), 0))

    def by_position(which):
        table = jnp.concatenate(
            [early_ref[g % nb, na * which + g // nb:na * which + g // nb + 1, :] for g in range(n_peers)], axis=0)
        out = jnp.broadcast_to(late[which:which + 1], (8, seqs))
        for i in range(n_draft - 1):
            x = pltpu.roll(table, (128 - n_loc * i) % 128, 1)
            x = jnp.where(lane < n_loc, x, 0.0)
            shift = n_loc
            while shift < 128:
                x = x + pltpu.roll(x, shift, 1)
                shift *= 2
            x = jnp.concatenate([x] * (seqs // 128), axis=1)
            row = jnp.sum(jnp.where(mine, x, 0.0), axis=0, keepdims=True)
            out = jnp.where(lax.broadcasted_iota(jnp.int32, (8, seqs), 0) == i, row, out)
        return out

    inv = 1.0 / by_position(0)

    def out_copy(k, slot):
        i, h = k // 2, lax.rem(k, 2)
        return pltpu.make_async_copy(
            stage.at[slot], res_ref.at[i, pl.ds(pl.multiple_of(h * half, half), half), :], stage_sem.at[slot])

    @pl.loop(0, 2 * n_draft)
    def _(k):
        i, h, slot = k // 2, lax.rem(k, 2), lax.rem(k, SLOTS)
        row = get_row(inv, i)
        col = to_col(jnp.where(h == 0, row[:, :half], row[:, half:]))

        @pl.when(k >= SLOTS)
        def _():
            out_copy(k - SLOTS, slot).wait()

        @pl.loop(0, vocab // NT)
        def _(t):
            cols = pl.ds(pl.multiple_of(t * NT, NT), NT)
            stage[slot, :, cols] = ex_ref[i, pl.ds(pl.multiple_of(h * half, half), half), cols] * col

        out_copy(k, slot).start()

    accept = by_position(1)[:n_draft]
    accept_v[...] = accept
    prod = accept[0:1]
    expected = prod
    for i in range(1, n_draft):
        prod = prod * accept[i:i + 1]
        expected += prod
    expected_v[...] = expected
    small_copies = (pltpu.make_async_copy(accept_v, accept_ref, small_sem.at[0]),
                    pltpu.make_async_copy(expected_v, expected_ref, small_sem.at[1]))
    for copy in small_copies:
        copy.start()
    for k in range(2 * n_draft - SLOTS, 2 * n_draft):
        out_copy(k, k % SLOTS).wait()
    bonus_copy.wait()
    for copy in small_copies:
        copy.wait()


def solution(mesh):
    na, nb = mesh.shape["tpa"], mesh.shape["tpb"]
    n_peers = na * nb
    any_spec = pl.BlockSpec(memory_space=pl.ANY)
    vmem_spec = pl.BlockSpec(memory_space=pltpu.VMEM)

    def local_step(hidden, w_head, q_draft, x_draft):
        seqs, n_pos, depth = hidden.shape
        vocab = w_head.shape[1]
        n_loc, n_draft, _ = q_draft.shape
        dims = (n_pos, seqs, depth, vocab, n_loc, na, nb)
        dma = pltpu.SemaphoreType.DMA
        small = pltpu.VMEM((4, 8, 128), F32)
        ex, bonus, early, late = pl.pallas_call(
            functools.partial(exchange_kernel, dims),
            out_shape=(pltpu.VMEM((n_draft, seqs, vocab), F32), pltpu.VMEM((seqs, vocab), F32),
                       small, pltpu.VMEM((n_peers, 2, seqs), F32)),
            in_specs=[any_spec] * 4,
            out_specs=(vmem_spec,) * 4,
            scratch_shapes=[
                pltpu.VMEM((n_pos, seqs, depth), jnp.bfloat16),
                pltpu.VMEM((2, depth, NT), jnp.bfloat16),
                pltpu.VMEM((n_pos, seqs, vocab), F32),
                pltpu.VMEM((n_draft, seqs), jnp.int32),
                pltpu.VMEM((n_draft, seqs, 128), jnp.int32),
                small, small, small, small, small, small, small,
                dma, dma((2,)), dma, dma, dma, dma((na,)), dma((n_peers,)),
            ] + [dma] * 14,
            compiler_params=pltpu.CompilerParams(collective_id=0, has_side_effects=True, vmem_limit_bytes=38 * 2**20),
            name="exchange",
        )(hidden.transpose(1, 0, 2), w_head, q_draft.transpose(1, 0, 2), x_draft.T)
        res, bonus_out, accept, expected = pl.pallas_call(
            functools.partial(output_kernel, na, nb),
            out_shape=(jax.ShapeDtypeStruct((n_draft, seqs, vocab), F32), jax.ShapeDtypeStruct((seqs, vocab), F32),
                       jax.ShapeDtypeStruct((n_draft, seqs), F32), jax.ShapeDtypeStruct((1, seqs), F32)),
            in_specs=[vmem_spec] * 4,
            out_specs=(any_spec,) * 4,
            scratch_shapes=[pltpu.VMEM((SLOTS, seqs // 2, vocab), F32), pltpu.VMEM((n_draft, seqs), F32),
                            pltpu.VMEM((1, seqs), F32), dma((SLOTS,)), dma, dma((2,))],
            compiler_params=pltpu.CompilerParams(vmem_limit_bytes=12 * 2**20),
            name="output",
        )(ex, bonus, early, late)
        return accept.T, expected.reshape(seqs), res.transpose(1, 0, 2), bonus_out

    return jax.shard_map(
        local_step, mesh=mesh,
        in_specs=(P("dp", None, None), P(None, VOCAB_AXES), P(("dp",) + VOCAB_AXES, None, None), P("dp", None)),
        out_specs=(P("dp", None), P("dp"), P("dp", None, VOCAB_AXES), P("dp", VOCAB_AXES)),
        check_vma=False)
```

```python
import functools

import jax
import jax.numpy as jnp
from jax import lax
from jax.experimental import pallas as pl
from jax.experimental.pallas import tpu as pltpu
from jax.sharding import PartitionSpec as P

INV_TEMP = 1.25
VOCAB_AXES = ("tpa", "tpb")
MESH = pl.DeviceIdType.MESH
F32 = jnp.float32
SEND = ((3, 3, 0, 0), (1, 0, 3, 2), (2, 2, 1, 1))
RECV = ((3, 0, 3, 0), (2, 3, 0, 1), (1, 2, 1, 2))
LAST_RECV = ((1, 0, 3, 2), (2, 3, 0, 1))
CORE_OFFSETS = (0, 2, 1, 3)
NT = 512


def pick(index, values):
    out = jnp.int32(values[-1])
    for k in range(len(values) - 2, -1, -1):
        out = jnp.where(index == k, jnp.int32(values[k]), out)
    return out


def diag(n):
    return lax.broadcasted_iota(jnp.int32, (n, n), 0) == lax.broadcasted_iota(jnp.int32, (n, n), 1)


def to_col(row):
    return jnp.sum(jnp.where(diag(row.shape[1]), row, 0.0), axis=1, keepdims=True)


def get_row(rows, i):
    return jnp.sum(jnp.where(lax.broadcasted_iota(jnp.int32, rows.shape, 0) == i, rows, 0.0), axis=0, keepdims=True)


def lanes(n, first, rows):
    return (lax.broadcasted_iota(jnp.int32, (rows, n), 1)
            == lax.broadcasted_iota(jnp.int32, (rows, n), 0) + first)


def spread(col, n, first):
    return jnp.sum(jnp.where(lanes(n, first, col.shape[0]), col, 0.0), axis=0, keepdims=True)


def gather(row, first, rows):
    return jnp.sum(jnp.where(lanes(row.shape[1], first, rows), row, 0.0), axis=1, keepdims=True)


def exchange_kernel(dims, hid_ref, w_ref, q_ref, x_ref, ex_ref, bonus_ref, early_ref, late_ref, part_p_ref, part_q_ref, part_head_ref, part_tok_ref,
                    hid_v, w_v, z_v, x_v, tok_v, stat_out, stat_1, stat_2, norm_v, sum_out, sum_1, sum_2, hid_sem, w_sem, own_sem, x_sem, part_sem,
                    q_send, q_recv, r_send, r_recv, h_send, h_recv,
                    a1_send, a1_recv, a2_send, a2_recv, a3_send, a3_recv, b1_send, b1_recv, b2_send, b2_recv, b3_send, b3_recv):
    n_pos, seqs, depth, vocab, n_loc, na, nb = dims
    n_draft = n_pos - 1
    n_early = n_draft - 1
    n_peers = na * nb
    n_tiles = vocab // NT
    others = range(n_peers - 1)
    dp, za, tb = lax.axis_index("dp"), lax.axis_index("tpa"), lax.axis_index("tpb")
    me = za * nb + tb

    inner = (za == 1) | (za == 2)

    def choose(end, mid):
        return [(jnp.where(inner, m[0], e[0]), lax.rem(tb + jnp.where(inner, m[1], e[1]), nb)) for e, m in zip(end, mid)]

    own = [(za, k) for k in range(1, nb)]
    steps = [[(pick(za, SEND[step]), CORE_OFFSETS[k]) for k in range(nb)] for step in range(3)]
    first_order = choose(steps[0] + steps[1] + steps[2] + own, own + steps[0] + steps[1] + steps[2])
    last_order = choose(steps[1] + own + steps[2] + steps[0], own + steps[1] + steps[0] + steps[2])

    def recv_peer(k):
        step, off = (k - 3) // nb, lax.rem(jnp.int32(k) + 1, nb)
        plane = jnp.where(k < 3, za, jnp.where(step == 0, pick(za, LAST_RECV[0]),
                          jnp.where(step == 1, pick(za, LAST_RECV[1]), na - 1 - za)))
        off = jnp.where(k < 3, k + 1, nb - pick(off, CORE_OFFSETS))
        return plane, lax.rem(tb + off, nb)

    def rows_of(group):
        return pl.ds(pl.multiple_of(group * n_loc, 8), n_loc)

    def q_copy(part, plane, core, own_group, column, send=q_send):
        i0, ni = (0, n_early) if part == 0 else (n_early, 1)
        recv = q_recv.at[own_group // nb] if part == 0 else r_recv.at[own_group]
        return pltpu.make_async_remote_copy(
            src_ref=q_ref.at[pl.ds(i0, ni), :, pl.ds(pl.multiple_of(column * vocab, 128), vocab)],
            dst_ref=ex_ref.at[pl.ds(i0, ni), rows_of(own_group), :],
            send_sem=send, recv_sem=recv,
            device_id=(dp, plane, core), device_id_type=MESH)

    def q_to(part, k):
        plane, core = (first_order, last_order)[part][k]
        return q_copy(part, plane, core, me, plane * nb + core, r_send if (part, k) >= (1, 11) else q_send)

    def q_from_plane(plane, count):
        rows = ex_ref.at[pl.ds(0, n_early), pl.ds(0, count * n_loc), :]
        pltpu.make_async_copy(rows, rows, q_recv.at[plane]).wait()

    def q_from(group):
        return q_copy(1, za, tb, group, 0)

    def small(src, dst, send, recv, src_slot, dst_slot, plane, core):
        return pltpu.make_async_remote_copy(
            src_ref=src.at[src_slot], dst_ref=dst.at[dst_slot], send_sem=send, recv_sem=recv,
            device_id=(dp, plane, core), device_id_type=MESH)

    def await_slots(ref, sem, count):
        part = ref.at[pl.ds(0, count)]
        pltpu.make_async_copy(part, part, sem).wait()

    def in_plane(src, dst, send, recv, scatter):
        cores = [lax.rem(tb + k, nb) for k in range(1, nb)]
        return [small(src, dst, send, recv, core if scatter else tb, tb, za, core) for core in cores]

    def across(ref, send, recv):
        planes = [lax.rem(za + k, na) for k in range(1, na)]
        return [small(ref, ref, send, recv, za, za, plane, tb) for plane in planes]

    def start(copies):
        for copy in copies:
            copy.start()

    def combine(ref):
        top = ref[0, 0:4]
        for k in range(1, 4):
            top = jnp.maximum(top, ref[k, 0:4])
        total = ref[0, 4:8] * jnp.exp(ref[0, 0:4] - top)
        for k in range(1, 4):
            total += ref[k, 4:8] * jnp.exp(ref[k, 0:4] - top)
        return top, total

    def add(ref):
        return (ref[0] + ref[1]) + (ref[2] + ref[3])

    def put(tile, plane, first, second):
        row = lax.broadcasted_iota(jnp.int32, tile.shape, 0)
        return jnp.where(row == plane, first, jnp.where(row == na + plane, second, tile))

    def w_copy(tile, slot):
        return pltpu.make_async_copy(w_ref.at[:, pl.ds(pl.multiple_of(tile * NT, NT), NT)], w_v.at[slot], w_sem.at[slot])

    hid_copy = pltpu.make_async_copy(hid_ref, hid_v, hid_sem)
    part_copies = [pltpu.make_async_copy(
        q_ref.at[n_early, :, pl.ds(pl.multiple_of(((na - 1 - za) * nb + core) * vocab, 128), vocab)],
        part_q_ref.at[pl.ds(core * n_loc, n_loc), :], part_sem.at[core]) for core in range(nb)]
    x_copy = pltpu.make_async_copy(x_ref, x_v, x_sem)
    own_copy = pltpu.make_async_copy(
        q_ref.at[:, :, pl.ds(pl.multiple_of(me * vocab, 128), vocab)], ex_ref.at[:, rows_of(me), :], own_sem)

    barrier = pltpu.get_barrier_semaphore()
    for k in range(1, n_peers):
        pl.semaphore_signal(barrier, inc=1, device_id=(dp, lax.rem(za + k // nb, na), lax.rem(tb + k % nb, nb)),
                            device_id_type=MESH)
    pl.semaphore_wait(barrier, n_peers - 1)

    for k in range(4):
        q_to(0, k).start()
    x_copy.start()
    for copy in part_copies:
        copy.start()
    hid_copy.start()
    w_copy(0, 0).start()
    own_copy.start()

    x_copy.wait()
    tok_rows = x_v[...].astype(F32)
    for i in range(n_draft):
        tok_v[i] = jnp.broadcast_to(to_col(tok_rows[i:i + 1]), (seqs, 128)).astype(jnp.int32) - me * vocab
    hid_copy.wait()
    for copy in part_copies:
        copy.wait()

    @pl.loop(0, n_tiles)
    def _(tile):
        slot = lax.rem(tile, 2)
        w_copy(tile, slot).wait()

        @pl.when(tile + 1 < n_tiles)
        def _():
            w_copy(tile + 1, 1 - slot).start()

        @pl.loop(0, n_pos)
        def _(i):
            z_v[i, :, pl.ds(pl.multiple_of(tile * NT, NT), NT)] = INV_TEMP * jnp.dot(
                hid_v[i], w_v[slot], preferred_element_type=F32)

    @pl.loop(0, nb)
    def _(core):
        def plane_rows(plane, tile):
            def one(i, rows):
                z = z_v[i, rows_of(plane * nb + core), :]
                m = jnp.max(z, axis=1, keepdims=True)
                s = jnp.sum(jnp.exp(z - m), axis=1, keepdims=True)
                return rows[0] + spread(m, 128, i * n_loc), rows[1] + spread(s, 128, i * n_loc)

            zero = jnp.zeros((1, 128), F32)
            return put(tile, plane, *lax.fori_loop(0, n_pos, one, (zero, zero)))

        stat_out[core] = lax.fori_loop(0, na, plane_rows, jnp.zeros((8, 128), F32))

    stat_1[tb] = stat_out[tb]
    start(in_plane(stat_out, stat_1, a1_send, a1_recv, True))
    await_slots(stat_1, a1_recv, 3)
    stat_2[za] = jnp.concatenate(combine(stat_1), axis=0)
    start(across(stat_2, a2_send, a2_recv))
    for k in (4, 5):
        q_to(0, k).start()
    await_slots(stat_2, a2_recv, 3)
    top, total = combine(stat_2)
    used = lax.broadcasted_iota(jnp.int32, (4, 128), 1) < n_pos * n_loc
    norm_v[tb] = jnp.concatenate([top, 1.0 / jnp.where(used, total, 1.0)], axis=0)
    start(in_plane(norm_v, norm_v, a3_send, a3_recv, False))
    for k in range(6, 15):
        q_to(0, k).start()
    for k in range(10):
        q_to(1, k).start()

    @pl.when(jnp.logical_not(inner))
    def _():
        q_to(1, 10).start()

    await_slots(norm_v, a3_recv, 3)

    def probs(i, group):
        norm, plane = norm_v[lax.rem(group, nb)], group // nb
        m = gather(get_row(norm, plane), i * n_loc, n_loc)
        r = gather(get_row(norm, na + plane), i * n_loc, n_loc)
        return jnp.exp(z_v[i, rows_of(group), :] - m) * r

    @pl.loop(0, n_peers)
    def _(group):
        bonus_ref[rows_of(group), :] = probs(n_draft, group)

    def cell(i, group):
        rows = rows_of(group)
        p, q, tok = probs(i, group), ex_ref[i, rows, :], tok_v[i, rows, 0:1]
        hit = lax.broadcasted_iota(jnp.int32, (n_loc, vocab), 1) == tok
        p_pick = jnp.sum(jnp.where(hit, p, 0.0), axis=1, keepdims=True)
        q_pick = jnp.sum(jnp.where(hit, q, 0.0), axis=1, keepdims=True)
        excess = jnp.maximum(p - q, 0.0)
        ex_ref[i, rows, :] = excess
        owned = (tok >= 0) & (tok < vocab)
        accept = jnp.where(owned, jnp.minimum(1.0, p_pick / jnp.where(owned, q_pick, 1.0)), 0.0)
        return jnp.sum(excess, axis=1, keepdims=True), accept

    def absorb_early(group):
        def one(i, rows):
            z, a = cell(i, group)
            return rows[0] + spread(z, 128, i * n_loc), rows[1] + spread(a, 128, i * n_loc)

        zero = jnp.zeros((1, 128), F32)
        z_row, a_row = lax.fori_loop(0, n_early, one, (zero, zero))
        core = lax.rem(group, nb)
        sum_out[core] = put(sum_out[core], group // nb, z_row, a_row)

    sum_out[...] = jnp.zeros_like(sum_out)
    own_copy.wait()
    absorb_early(me)

    q_from_plane(za, nb - 1)
    for k in range(1, nb):
        absorb_early(za * nb + lax.rem(tb + k, nb))

    @pl.loop(0, na - 1)
    def _(step):
        plane = jnp.where(step == 0, pick(za, RECV[0]), jnp.where(step == 1, pick(za, RECV[1]), pick(za, RECV[2])))
        q_from_plane(plane, nb)

        @pl.loop(0, nb)
        def _(core):
            absorb_early(plane * nb + core)

    sum_1[tb] = sum_out[tb]
    start(in_plane(sum_out, sum_1, b1_send, b1_recv, True))
    await_slots(sum_1, b1_recv, 3)
    sum_2[za] = add(sum_1)
    start(across(sum_2, b2_send, b2_recv))

    partner = na - 1 - za
    head = pltpu.make_async_remote_copy(
        src_ref=q_ref.at[n_early, pl.ds(0, n_loc // 2), pl.ds(pl.multiple_of((partner * nb + tb) * vocab, 128), vocab)],
        dst_ref=part_head_ref, send_sem=h_send, recv_sem=h_recv, device_id=(dp, partner, tb), device_id_type=MESH)

    @pl.when(inner)
    def _():
        q_to(1, 10).start()
        head.start()

    @pl.loop(0, nb)
    def _(core):
        group = partner * nb + core
        part_p_ref[pl.ds(pl.multiple_of(core * n_loc, 8), n_loc), :] = probs(n_early, group)
        part_tok_ref[pl.ds(pl.multiple_of(core * n_loc, 8), n_loc), :] = tok_v[n_early, rows_of(group), :]

    def absorb_late(group):
        z, a = cell(n_early, group)
        late_ref[...] += jnp.concatenate([spread(z, seqs, group * n_loc), spread(a, seqs, group * n_loc)], axis=0)

    def arrived(k):
        plane, core = recv_peer(k)
        q_from(plane * nb + core).wait_recv()
        absorb_late(plane * nb + core)

    late_ref[...] = jnp.zeros_like(late_ref)
    absorb_late(me)
    pl.loop(0, 10)(arrived)

    plane, core = recv_peer(10)
    q_from(plane * nb + core).wait_recv()

    @pl.when(jnp.logical_not(inner))
    def _():
        for k in range(11, 15):
            q_to(1, k).start()

    absorb_late(plane * nb + core)
    await_slots(sum_2, b2_recv, 3)
    early_ref[tb] = add(sum_2)
    start(in_plane(early_ref, early_ref, b3_send, b3_recv, False))

    @pl.when(inner)
    def _():
        head.wait()

    @pl.when(jnp.logical_not(inner))
    def _():
        pl.loop(11, 15)(arrived)
        sent = q_ref.at[0:4, :, pl.ds(0, vocab)]
        pltpu.make_async_copy(sent, sent, r_send).wait()

    await_slots(early_ref, b3_recv, 3)
    slices = (n_peers - 1) * n_early + 11
    sent = q_ref.at[:, :, pl.ds(0, slices * vocab // n_draft)]
    pltpu.make_async_copy(sent, sent, q_send).wait()
    for ref, sem in ((stat_1, a1_send), (stat_2, a2_send), (norm_v, a3_send), (sum_1, b1_send), (sum_2, b2_send),
                     (early_ref, b3_send)):
        await_slots(ref, sem, 3)


def last_kernel(dims, q_ref, head_ref, p_ref, tok_ref, part_ref, order_ref, ex_ref, late_ref, own_v, ready, q_send, q_recv, l_send, l_recv):
    n_draft, seqs, vocab, n_loc, na, nb = dims
    n_peers = na * nb
    dp, za, tb = lax.axis_index("dp"), lax.axis_index("tpa"), lax.axis_index("tpb")
    me, partner = za * nb + tb, na - 1 - za
    inner = (za == 1) | (za == 2)
    same = [(za, lax.rem(tb + k, nb)) for k in range(1, nb)] + [(partner, lax.rem(tb + k, nb)) for k in range(nb)]
    other_planes = (jnp.where(inner, 0, 1), jnp.where(inner, 3, 2))
    other = [(plane, lax.rem(tb + k, nb)) for plane in other_planes for k in range(nb)]

    def signal(sem, peers):
        for plane, core in peers:
            pl.semaphore_signal(sem, inc=1, device_id=(dp, plane, core), device_id_type=MESH)

    barrier = pltpu.get_barrier_semaphore()
    signal(barrier, same)

    @pl.when(inner)
    def _():
        signal(barrier, other)

    pl.semaphore_wait(barrier, jnp.where(inner, 2 * nb - 1, n_peers - 1))

    @pl.when(jnp.logical_not(inner))
    def _():
        signal(ready, other)

    def q_copy(core, own_core, first):
        return pltpu.make_async_remote_copy(
            src_ref=q_ref.at[pl.ds(pl.multiple_of(core * n_loc + first, 8), n_loc - first), :],
            dst_ref=ex_ref.at[pl.ds(pl.multiple_of(own_core * n_loc + first, 8), n_loc - first), :],
            send_sem=q_send, recv_sem=q_recv.at[own_core], device_id=(dp, partner, core), device_id_type=MESH)

    def late_to(peer):
        plane, core = peer
        return pltpu.make_async_remote_copy(
            src_ref=late_ref.at[me], dst_ref=late_ref.at[me], send_sem=l_send, recv_sem=l_recv,
            device_id=(dp, plane, core), device_id_type=MESH)

    own_v[...] = part_ref[...]

    @pl.when(inner)
    def _():
        for k in CORE_OFFSETS:
            q_copy(lax.rem(tb + k, nb), tb, 0 if k else n_loc // 2).start()

        ex_ref[pl.ds(pl.multiple_of(tb * n_loc, 8), n_loc // 2), :] = head_ref[...]
        q_copy(tb, tb, n_loc // 2).wait_recv()

        @pl.loop(0, nb)
        def _(k):
            core = lax.rem(tb + nb - pick(k, CORE_OFFSETS), nb)
            rows = pl.ds(pl.multiple_of(core * n_loc, 8), n_loc)

            @pl.when(k > 0)
            def _():
                q_copy(core, core, 0).wait_recv()

            p, q, tok = p_ref[rows, :], ex_ref[rows, :], tok_ref[rows, 0:1]
            hit = lax.broadcasted_iota(jnp.int32, (n_loc, vocab), 1) == tok
            excess = jnp.maximum(p - q, 0.0)
            ex_ref[rows, :] = excess
            z = jnp.sum(excess, axis=1, keepdims=True)
            p_pick = jnp.sum(jnp.where(hit, p, 0.0), axis=1, keepdims=True)
            q_pick = jnp.sum(jnp.where(hit, q, 0.0), axis=1, keepdims=True)
            owned = (tok >= 0) & (tok < vocab)
            a = jnp.where(owned, jnp.minimum(1.0, p_pick / jnp.where(owned, q_pick, 1.0)), 0.0)
            first = (partner * nb + core) * n_loc
            own_v[...] += jnp.concatenate([spread(z, seqs, first), spread(a, seqs, first)], axis=0)

    late_ref[me] = own_v[...]

    @pl.when(inner)
    def _():
        sent = q_ref.at[pl.ds(0, nb * n_loc - n_loc // 2), :]
        pltpu.make_async_copy(sent, sent, q_send).wait()
        pl.semaphore_wait(ready, 2 * nb)

    for peer in other + same:
        late_to(peer).start()
    slots = late_ref.at[pl.ds(0, n_peers - 1)]
    pltpu.make_async_copy(slots, slots, l_recv).wait()
    pltpu.make_async_copy(slots, slots, l_send).wait()


SLOTS = 4


def by_position(na, nb, early_ref, which, n_early, seqs):
    n_peers = na * nb
    n_loc = seqs // n_peers
    lane = lax.broadcasted_iota(jnp.int32, (n_peers, 128), 1)
    mine = (lax.broadcasted_iota(jnp.int32, (n_peers, seqs), 1) // n_loc
            == lax.broadcasted_iota(jnp.int32, (n_peers, seqs), 0))
    table = jnp.concatenate(
        [early_ref[g % nb, na * which + g // nb:na * which + g // nb + 1, :] for g in range(n_peers)], axis=0)
    out = jnp.ones((8, seqs), F32)
    for i in range(n_early):
        x = pltpu.roll(table, (128 - n_loc * i) % 128, 1)
        x = jnp.where(lane < n_loc, x, 0.0)
        shift = n_loc
        while shift < 128:
            x = x + pltpu.roll(x, shift, 1)
            shift *= 2
        x = jnp.concatenate([x] * (seqs // 128), axis=1)
        row = jnp.sum(jnp.where(mine, x, 0.0), axis=0, keepdims=True)
        out = jnp.where(lax.broadcasted_iota(jnp.int32, (8, seqs), 0) == i, row, out)
    return out


def early_output_kernel(na, nb, ex_ref, bonus_ref, early_ref, res_ref, bonus_out, order_ref, stage, stage_sem, bonus_sem):
    n_draft, seqs, vocab = ex_ref.shape
    n_early, half = n_draft - 1, seqs // 2
    bonus_copy = pltpu.make_async_copy(bonus_ref, bonus_out, bonus_sem)
    bonus_copy.start()
    order_ref[...] = jnp.zeros_like(order_ref)
    inv = 1.0 / by_position(na, nb, early_ref, 0, n_early, seqs)

    def out_copy(k, slot):
        i, h = k // 2, lax.rem(k, 2)
        return pltpu.make_async_copy(
            stage.at[slot], res_ref.at[i, pl.ds(pl.multiple_of(h * half, half), half), :], stage_sem.at[slot])

    @pl.loop(0, 2 * n_early)
    def _(k):
        i, h, slot = k // 2, lax.rem(k, 2), lax.rem(k, SLOTS)
        row = get_row(inv, i)
        col = to_col(jnp.where(h == 0, row[:, :half], row[:, half:]))

        @pl.when(k >= SLOTS)
        def _():
            out_copy(k - SLOTS, slot).wait()

        @pl.loop(0, vocab // NT)
        def _(t):
            cols = pl.ds(pl.multiple_of(t * NT, NT), NT)
            stage[slot, :, cols] = ex_ref[i, pl.ds(pl.multiple_of(h * half, half), half), cols] * col

        out_copy(k, slot).start()

    for k in range(2 * n_early - SLOTS, 2 * n_early):
        out_copy(k, k % SLOTS).wait()
    bonus_copy.wait()


def late_output_kernel(na, nb, ex_ref, part_ref, early_ref, late_ref, res_in, res_ref, accept_ref, expected_ref,
                       stage, accept_v, expected_v, stage_sem, small_sem):
    n_draft, seqs, vocab = ex_ref.shape
    n_early, block = n_draft - 1, seqs // na
    za = lax.axis_index("tpa")
    inner, partner = (za == 1) | (za == 2), na - 1 - za
    late = late_ref[0]
    for k in range(1, na * nb):
        late += late_ref[k]
    col = to_col(1.0 / late[0:1])

    def out_copy(plane):
        rows = pl.ds(plane * block, block)
        return pltpu.make_async_copy(stage.at[rows], res_ref.at[n_early, rows, :], stage_sem.at[plane])

    for plane in range(na):
        rows, scale = pl.ds(plane * block, block), col[plane * block:(plane + 1) * block]
        from_part = inner & (partner == plane)

        @pl.when(from_part)
        def _():
            @pl.loop(0, vocab // NT)
            def _(t):
                cols = pl.ds(pl.multiple_of(t * NT, NT), NT)
                stage[rows, cols] = part_ref[:, cols] * scale

        @pl.when(jnp.logical_not(from_part))
        def _():
            @pl.loop(0, vocab // NT)
            def _(t):
                cols = pl.ds(pl.multiple_of(t * NT, NT), NT)
                stage[rows, cols] = ex_ref[n_early, rows, cols] * scale

        out_copy(plane).start()

    accept = by_position(na, nb, early_ref, 1, n_early, seqs)
    accept = jnp.where(lax.broadcasted_iota(jnp.int32, accept.shape, 0) == n_early, late[1:2], accept)[:n_draft]
    accept_v[...] = accept
    prod = accept[0:1]
    expected = prod
    for i in range(1, n_draft):
        prod = prod * accept[i:i + 1]
        expected += prod
    expected_v[...] = expected
    small_copies = (pltpu.make_async_copy(accept_v, accept_ref, small_sem.at[0]),
                    pltpu.make_async_copy(expected_v, expected_ref, small_sem.at[1]))
    for copy in small_copies:
        copy.start()
    for plane in range(na):
        out_copy(plane).wait()
    for copy in small_copies:
        copy.wait()


def solution(mesh):
    na, nb = mesh.shape["tpa"], mesh.shape["tpb"]
    n_peers = na * nb
    any_spec = pl.BlockSpec(memory_space=pl.ANY)
    vmem_spec = pl.BlockSpec(memory_space=pltpu.VMEM)

    def local_step(hidden, w_head, q_draft, x_draft):
        seqs, n_pos, depth = hidden.shape
        vocab = w_head.shape[1]
        n_loc, n_draft, _ = q_draft.shape
        dims = (n_pos, seqs, depth, vocab, n_loc, na, nb)
        dma = pltpu.SemaphoreType.DMA
        small = pltpu.VMEM((4, 8, 128), F32)
        q_rows = q_draft.transpose(1, 0, 2)
        block = seqs // na
        ex, bonus, early, late_part, part_p, part_q, part_head, part_tok = pl.pallas_call(
            functools.partial(exchange_kernel, dims),
            out_shape=(pltpu.VMEM((n_draft, seqs, vocab), F32), pltpu.VMEM((seqs, vocab), F32), small,
                       pltpu.VMEM((2, seqs), F32), pltpu.VMEM((block, vocab), F32), pltpu.VMEM((block, vocab), F32),
                       pltpu.VMEM((n_loc // 2, vocab), F32), pltpu.VMEM((block, 128), jnp.int32)),
            in_specs=[any_spec] * 4,
            out_specs=(vmem_spec,) * 8,
            scratch_shapes=[
                pltpu.VMEM((n_pos, seqs, depth), jnp.bfloat16),
                pltpu.VMEM((2, depth, NT), jnp.bfloat16),
                pltpu.VMEM((n_pos, seqs, vocab), F32),
                pltpu.VMEM((n_draft, seqs), jnp.int32),
                pltpu.VMEM((n_draft, seqs, 128), jnp.int32),
                small, small, small, small, small, small, small,
                dma, dma((2,)), dma, dma, dma((nb,)), dma, dma((na,)), dma, dma((n_peers,)),
            ] + [dma] * 14,
            compiler_params=pltpu.CompilerParams(collective_id=0, has_side_effects=True, vmem_limit_bytes=38 * 2**20),
            name="exchange",
        )(hidden.transpose(1, 0, 2), w_head, q_rows, x_draft.T)
        res, bonus_out, order = pl.pallas_call(
            functools.partial(early_output_kernel, na, nb),
            out_shape=(jax.ShapeDtypeStruct((n_draft, seqs, vocab), F32), jax.ShapeDtypeStruct((seqs, vocab), F32),
                       pltpu.VMEM((8, 128), F32)),
            in_specs=[vmem_spec] * 3,
            out_specs=(any_spec, any_spec, vmem_spec),
            scratch_shapes=[pltpu.VMEM((SLOTS, seqs // 2, vocab), F32), dma((SLOTS,)), dma],
            compiler_params=pltpu.CompilerParams(vmem_limit_bytes=12 * 2**20),
            name="early_output",
        )(ex, bonus, early)
        part, late = pl.pallas_call(
            functools.partial(last_kernel, (n_draft, seqs, vocab, n_loc, na, nb)),
            out_shape=(pltpu.VMEM((block, vocab), F32), pltpu.VMEM((n_peers, 2, seqs), F32)),
            in_specs=[vmem_spec] * 6,
            out_specs=(vmem_spec, vmem_spec),
            scratch_shapes=[pltpu.VMEM((2, seqs), F32), pltpu.SemaphoreType.REGULAR, dma, dma((nb,)), dma, dma],
            compiler_params=pltpu.CompilerParams(collective_id=1, has_side_effects=True, vmem_limit_bytes=28 * 2**20),
            name="last",
        )(part_q, part_head, part_p, part_tok, late_part, order)
        res, accept, expected = pl.pallas_call(
            functools.partial(late_output_kernel, na, nb),
            out_shape=(jax.ShapeDtypeStruct((n_draft, seqs, vocab), F32), jax.ShapeDtypeStruct((n_draft, seqs), F32),
                       jax.ShapeDtypeStruct((1, seqs), F32)),
            in_specs=[vmem_spec] * 4 + [any_spec],
            out_specs=(any_spec,) * 3,
            scratch_shapes=[pltpu.VMEM((seqs, vocab), F32), pltpu.VMEM((n_draft, seqs), F32), pltpu.VMEM((1, seqs), F32),
                            dma((na,)), dma((2,))],
            input_output_aliases={4: 0},
            compiler_params=pltpu.CompilerParams(vmem_limit_bytes=12 * 2**20),
            name="late_output",
        )(ex, part, early, late, res)
        return accept.T, expected.reshape(seqs), res.transpose(1, 0, 2), bonus_out

    return jax.shard_map(
        local_step, mesh=mesh,
        in_specs=(P("dp", None, None), P(None, VOCAB_AXES), P(("dp",) + VOCAB_AXES, None, None), P("dp", None)),
        out_specs=(P("dp", None), P("dp"), P("dp", None, VOCAB_AXES), P("dp", VOCAB_AXES)),
        check_vma=False)
```

```python
import functools

import jax
import jax.numpy as jnp
from jax import lax
from jax.experimental import pallas as pl
from jax.experimental.pallas import tpu as pltpu
from jax.sharding import PartitionSpec as P

INV_TEMP = 1.25
VOCAB_AXES = ("tpa", "tpb")
MESH = pl.DeviceIdType.MESH
F32 = jnp.float32
SEND = ((3, 3, 0, 0), (1, 0, 3, 2), (2, 2, 1, 1))
RECV = ((3, 0, 3, 0), (2, 3, 0, 1), (1, 2, 1, 2))
LAST_RECV = ((1, 0, 3, 2), (2, 3, 0, 1))
CORE_OFFSETS = (0, 2, 1, 3)
NT = 512


def pick(index, values):
    out = jnp.int32(values[-1])
    for k in range(len(values) - 2, -1, -1):
        out = jnp.where(index == k, jnp.int32(values[k]), out)
    return out


def diag(n):
    return lax.broadcasted_iota(jnp.int32, (n, n), 0) == lax.broadcasted_iota(jnp.int32, (n, n), 1)


def to_col(row):
    return jnp.sum(jnp.where(diag(row.shape[1]), row, 0.0), axis=1, keepdims=True)


def get_row(rows, i):
    return jnp.sum(jnp.where(lax.broadcasted_iota(jnp.int32, rows.shape, 0) == i, rows, 0.0), axis=0, keepdims=True)


def lanes(n, first, rows):
    return (lax.broadcasted_iota(jnp.int32, (rows, n), 1)
            == lax.broadcasted_iota(jnp.int32, (rows, n), 0) + first)


def spread(col, n, first):
    return jnp.sum(jnp.where(lanes(n, first, col.shape[0]), col, 0.0), axis=0, keepdims=True)


def gather(row, first, rows):
    return jnp.sum(jnp.where(lanes(row.shape[1], first, rows), row, 0.0), axis=1, keepdims=True)


def exchange_kernel(dims, hid_ref, w_ref, q_ref, x_ref, ex_ref, bonus_ref, early_ref, late_ref, part_p_ref, part_q_ref, part_head_ref, part_tok_ref,
                    hid_v, w_v, z_v, x_v, tok_v, stat_out, stat_1, stat_2, norm_v, sum_out, sum_1, sum_2, hid_sem, w_sem, own_sem, x_sem, part_sem,
                    ready, q_send, q_recv, r_send, r_recv, h_send, h_recv,
                    a1_send, a1_recv, a2_send, a2_recv, a3_send, a3_recv, b1_send, b1_recv, b2_send, b2_recv, b3_send, b3_recv):
    n_pos, seqs, depth, vocab, n_loc, na, nb = dims
    n_draft = n_pos - 1
    n_early = n_draft - 1
    n_peers = na * nb
    n_tiles = vocab // NT
    others = range(n_peers - 1)
    dp, za, tb = lax.axis_index("dp"), lax.axis_index("tpa"), lax.axis_index("tpb")
    me = za * nb + tb

    inner = (za == 1) | (za == 2)

    def choose(end, mid):
        return [(jnp.where(inner, m[0], e[0]), lax.rem(tb + jnp.where(inner, m[1], e[1]), nb)) for e, m in zip(end, mid)]

    own = [(za, k) for k in range(1, nb)]
    steps = [[(pick(za, SEND[step]), CORE_OFFSETS[k]) for k in range(nb)] for step in range(3)]
    first_order = choose(steps[0] + steps[1] + steps[2] + own, steps[2][:1] + own + steps[0] + steps[1] + steps[2][1:])
    last_order = choose(steps[1] + own + steps[2] + steps[0], own + steps[1] + steps[0] + steps[2])

    def recv_peer(k):
        step, off = (k - 3) // nb, lax.rem(jnp.int32(k) + 1, nb)
        plane = jnp.where(k < 3, za, jnp.where(step == 0, pick(za, LAST_RECV[0]),
                          jnp.where(step == 1, pick(za, LAST_RECV[1]), na - 1 - za)))
        off = jnp.where(k < 3, k + 1, nb - pick(off, CORE_OFFSETS))
        return plane, lax.rem(tb + off, nb)

    def rows_of(group):
        return pl.ds(pl.multiple_of(group * n_loc, 8), n_loc)

    def q_copy(part, plane, core, own_group, column, send=q_send):
        i0, ni = (0, n_early) if part == 0 else (n_early, 1)
        recv = q_recv.at[own_group // nb] if part == 0 else r_recv.at[own_group]
        return pltpu.make_async_remote_copy(
            src_ref=q_ref.at[pl.ds(i0, ni), :, pl.ds(pl.multiple_of(column * vocab, 128), vocab)],
            dst_ref=ex_ref.at[pl.ds(i0, ni), rows_of(own_group), :],
            send_sem=send, recv_sem=recv,
            device_id=(dp, plane, core), device_id_type=MESH)

    def q_to(part, k):
        plane, core = (first_order, last_order)[part][k]
        return q_copy(part, plane, core, me, plane * nb + core, r_send if (part, k) >= (1, 11) else q_send)

    def q_from_plane(plane, count):
        rows = ex_ref.at[pl.ds(0, n_early), pl.ds(0, count * n_loc), :]
        pltpu.make_async_copy(rows, rows, q_recv.at[plane]).wait()

    def q_from(group):
        return q_copy(1, za, tb, group, 0)

    def small(src, dst, send, recv, src_slot, dst_slot, plane, core):
        return pltpu.make_async_remote_copy(
            src_ref=src.at[src_slot], dst_ref=dst.at[dst_slot], send_sem=send, recv_sem=recv,
            device_id=(dp, plane, core), device_id_type=MESH)

    def await_slots(ref, sem, count):
        part = ref.at[pl.ds(0, count)]
        pltpu.make_async_copy(part, part, sem).wait()

    def in_plane(src, dst, send, recv, scatter):
        cores = [lax.rem(tb + k, nb) for k in range(1, nb)]
        return [small(src, dst, send, recv, core if scatter else tb, tb, za, core) for core in cores]

    def across(ref, send, recv):
        planes = [lax.rem(za + k, na) for k in range(1, na)]
        return [small(ref, ref, send, recv, za, za, plane, tb) for plane in planes]

    def start(copies):
        for copy in copies:
            copy.start()

    def combine(ref):
        top = ref[0, 0:4]
        for k in range(1, 4):
            top = jnp.maximum(top, ref[k, 0:4])
        total = ref[0, 4:8] * jnp.exp(ref[0, 0:4] - top)
        for k in range(1, 4):
            total += ref[k, 4:8] * jnp.exp(ref[k, 0:4] - top)
        return top, total

    def add(ref):
        return (ref[0] + ref[1]) + (ref[2] + ref[3])

    def put(tile, plane, first, second):
        row = lax.broadcasted_iota(jnp.int32, tile.shape, 0)
        return jnp.where(row == plane, first, jnp.where(row == na + plane, second, tile))

    def w_copy(tile, slot):
        return pltpu.make_async_copy(w_ref.at[:, pl.ds(pl.multiple_of(tile * NT, NT), NT)], w_v.at[slot], w_sem.at[slot])

    hid_copy = pltpu.make_async_copy(hid_ref, hid_v, hid_sem)
    part_copies = [pltpu.make_async_copy(
        q_ref.at[n_early, :, pl.ds(pl.multiple_of(((na - 1 - za) * nb + core) * vocab, 128), vocab)],
        part_q_ref.at[pl.ds(core * n_loc, n_loc), :], part_sem.at[core]) for core in range(nb)]
    x_copy = pltpu.make_async_copy(x_ref, x_v, x_sem)
    own_copy = pltpu.make_async_copy(
        q_ref.at[:, :, pl.ds(pl.multiple_of(me * vocab, 128), vocab)], ex_ref.at[:, rows_of(me), :], own_sem)

    def signal(sem, peers):
        for plane, core in peers:
            pl.semaphore_signal(sem, inc=1, device_id=(dp, plane, core), device_id_type=MESH)

    partner = na - 1 - za
    own_plane = [(za, lax.rem(tb + k, nb)) for k in range(1, nb)]
    partner_plane = [(partner, lax.rem(tb + k, nb)) for k in range(nb)]
    other_planes = [(plane, lax.rem(tb + k, nb)) for plane in (jnp.where(inner, 0, 1), jnp.where(inner, 3, 2)) for k in range(nb)]

    barrier = pltpu.get_barrier_semaphore()
    signal(barrier, partner_plane)

    @pl.when(inner)
    def _():
        signal(barrier, other_planes)

    @pl.when(jnp.logical_not(inner))
    def _():
        signal(barrier, own_plane)

    pl.semaphore_wait(barrier, jnp.where(inner, nb, n_peers - 1))
    q_to(0, 0).start()

    @pl.when(jnp.logical_not(inner))
    def _():
        for k in range(1, 4):
            q_to(0, k).start()
        signal(ready, other_planes)

    x_copy.start()
    for copy in part_copies:
        copy.start()
    hid_copy.start()
    w_copy(0, 0).start()
    own_copy.start()

    @pl.when(inner)
    def _():
        pl.semaphore_wait(ready, 2 * nb)
        for k in range(1, 4):
            q_to(0, k).start()

    x_copy.wait()
    tok_rows = x_v[...].astype(F32)
    for i in range(n_draft):
        tok_v[i] = jnp.broadcast_to(to_col(tok_rows[i:i + 1]), (seqs, 128)).astype(jnp.int32) - me * vocab
    hid_copy.wait()
    for copy in part_copies:
        copy.wait()

    @pl.loop(0, n_tiles)
    def _(tile):
        slot = lax.rem(tile, 2)
        w_copy(tile, slot).wait()

        @pl.when(tile + 1 < n_tiles)
        def _():
            w_copy(tile + 1, 1 - slot).start()

        @pl.loop(0, n_pos)
        def _(i):
            z_v[i, :, pl.ds(pl.multiple_of(tile * NT, NT), NT)] = INV_TEMP * jnp.dot(
                hid_v[i], w_v[slot], preferred_element_type=F32)

    @pl.loop(0, nb)
    def _(core):
        def plane_rows(plane, tile):
            def one(i, rows):
                z = z_v[i, rows_of(plane * nb + core), :]
                m = jnp.max(z, axis=1, keepdims=True)
                s = jnp.sum(jnp.exp(z - m), axis=1, keepdims=True)
                return rows[0] + spread(m, 128, i * n_loc), rows[1] + spread(s, 128, i * n_loc)

            zero = jnp.zeros((1, 128), F32)
            return put(tile, plane, *lax.fori_loop(0, n_pos, one, (zero, zero)))

        stat_out[core] = lax.fori_loop(0, na, plane_rows, jnp.zeros((8, 128), F32))

    stat_1[tb] = stat_out[tb]
    start(in_plane(stat_out, stat_1, a1_send, a1_recv, True))
    await_slots(stat_1, a1_recv, 3)
    stat_2[za] = jnp.concatenate(combine(stat_1), axis=0)
    start(across(stat_2, a2_send, a2_recv))
    for k in (4, 5):
        q_to(0, k).start()
    await_slots(stat_2, a2_recv, 3)
    top, total = combine(stat_2)
    used = lax.broadcasted_iota(jnp.int32, (4, 128), 1) < n_pos * n_loc
    norm_v[tb] = jnp.concatenate([top, 1.0 / jnp.where(used, total, 1.0)], axis=0)
    start(in_plane(norm_v, norm_v, a3_send, a3_recv, False))
    for k in range(6, 15):
        q_to(0, k).start()
    for k in range(10):
        q_to(1, k).start()

    @pl.when(jnp.logical_not(inner))
    def _():
        q_to(1, 10).start()

    await_slots(norm_v, a3_recv, 3)

    def probs(i, group):
        norm, plane = norm_v[lax.rem(group, nb)], group // nb
        m = gather(get_row(norm, plane), i * n_loc, n_loc)
        r = gather(get_row(norm, na + plane), i * n_loc, n_loc)
        return jnp.exp(z_v[i, rows_of(group), :] - m) * r

    @pl.loop(0, n_peers)
    def _(group):
        bonus_ref[rows_of(group), :] = probs(n_draft, group)

    def cell(i, group):
        rows = rows_of(group)
        p, q, tok = probs(i, group), ex_ref[i, rows, :], tok_v[i, rows, 0:1]
        hit = lax.broadcasted_iota(jnp.int32, (n_loc, vocab), 1) == tok
        p_pick = jnp.sum(jnp.where(hit, p, 0.0), axis=1, keepdims=True)
        q_pick = jnp.sum(jnp.where(hit, q, 0.0), axis=1, keepdims=True)
        excess = jnp.maximum(p - q, 0.0)
        ex_ref[i, rows, :] = excess
        owned = (tok >= 0) & (tok < vocab)
        accept = jnp.where(owned, jnp.minimum(1.0, p_pick / jnp.where(owned, q_pick, 1.0)), 0.0)
        return jnp.sum(excess, axis=1, keepdims=True), accept

    def absorb_early(group):
        def one(i, rows):
            z, a = cell(i, group)
            return rows[0] + spread(z, 128, i * n_loc), rows[1] + spread(a, 128, i * n_loc)

        zero = jnp.zeros((1, 128), F32)
        z_row, a_row = lax.fori_loop(0, n_early, one, (zero, zero))
        core = lax.rem(group, nb)
        sum_out[core] = put(sum_out[core], group // nb, z_row, a_row)

    sum_out[...] = jnp.zeros_like(sum_out)
    own_copy.wait()
    absorb_early(me)

    q_from_plane(za, nb - 1)
    for k in range(1, nb):
        absorb_early(za * nb + lax.rem(tb + k, nb))

    @pl.loop(0, na - 1)
    def _(step):
        plane = jnp.where(step == 0, pick(za, RECV[0]), jnp.where(step == 1, pick(za, RECV[1]), pick(za, RECV[2])))
        q_from_plane(plane, nb)

        @pl.loop(0, nb)
        def _(core):
            absorb_early(plane * nb + core)

    sum_1[tb] = sum_out[tb]
    start(in_plane(sum_out, sum_1, b1_send, b1_recv, True))
    await_slots(sum_1, b1_recv, 3)
    sum_2[za] = add(sum_1)
    start(across(sum_2, b2_send, b2_recv))

    head = pltpu.make_async_remote_copy(
        src_ref=q_ref.at[n_early, pl.ds(0, n_loc // 2), pl.ds(pl.multiple_of((partner * nb + tb) * vocab, 128), vocab)],
        dst_ref=part_head_ref, send_sem=h_send, recv_sem=h_recv, device_id=(dp, partner, tb), device_id_type=MESH)

    @pl.when(inner)
    def _():
        q_to(1, 10).start()
        head.start()

    @pl.loop(0, nb)
    def _(core):
        group = partner * nb + core
        part_p_ref[pl.ds(pl.multiple_of(core * n_loc, 8), n_loc), :] = probs(n_early, group)
        part_tok_ref[pl.ds(pl.multiple_of(core * n_loc, 8), n_loc), :] = tok_v[n_early, rows_of(group), :]

    def absorb_late(group):
        z, a = cell(n_early, group)
        late_ref[...] += jnp.concatenate([spread(z, seqs, group * n_loc), spread(a, seqs, group * n_loc)], axis=0)

    def arrived(k):
        plane, core = recv_peer(k)
        q_from(plane * nb + core).wait_recv()
        absorb_late(plane * nb + core)

    late_ref[...] = jnp.zeros_like(late_ref)
    absorb_late(me)
    pl.loop(0, 10)(arrived)

    plane, core = recv_peer(10)
    q_from(plane * nb + core).wait_recv()

    @pl.when(jnp.logical_not(inner))
    def _():
        for k in range(11, 15):
            q_to(1, k).start()

    absorb_late(plane * nb + core)
    await_slots(sum_2, b2_recv, 3)
    early_ref[tb] = add(sum_2)
    start(in_plane(early_ref, early_ref, b3_send, b3_recv, False))

    @pl.when(inner)
    def _():
        head.wait()

    @pl.when(jnp.logical_not(inner))
    def _():
        pl.loop(11, 15)(arrived)
        sent = q_ref.at[0:4, :, pl.ds(0, vocab)]
        pltpu.make_async_copy(sent, sent, r_send).wait()

    await_slots(early_ref, b3_recv, 3)
    slices = (n_peers - 1) * n_early + 11
    sent = q_ref.at[:, :, pl.ds(0, slices * vocab // n_draft)]
    pltpu.make_async_copy(sent, sent, q_send).wait()
    for ref, sem in ((stat_1, a1_send), (stat_2, a2_send), (norm_v, a3_send), (sum_1, b1_send), (sum_2, b2_send),
                     (early_ref, b3_send)):
        await_slots(ref, sem, 3)


def last_kernel(dims, q_ref, head_ref, p_ref, tok_ref, part_ref, order_ref, ex_ref, late_ref, own_v, ready, q_send, q_recv, l_send, l_recv):
    n_draft, seqs, vocab, n_loc, na, nb = dims
    n_peers = na * nb
    dp, za, tb = lax.axis_index("dp"), lax.axis_index("tpa"), lax.axis_index("tpb")
    me, partner = za * nb + tb, na - 1 - za
    inner = (za == 1) | (za == 2)
    same = [(za, lax.rem(tb + k, nb)) for k in range(1, nb)] + [(partner, lax.rem(tb + k, nb)) for k in range(nb)]
    other_planes = (jnp.where(inner, 0, 1), jnp.where(inner, 3, 2))
    other = [(plane, lax.rem(tb + k, nb)) for plane in other_planes for k in range(nb)]

    def signal(sem, peers):
        for plane, core in peers:
            pl.semaphore_signal(sem, inc=1, device_id=(dp, plane, core), device_id_type=MESH)

    barrier = pltpu.get_barrier_semaphore()
    signal(barrier, same)

    @pl.when(inner)
    def _():
        signal(barrier, other)

    pl.semaphore_wait(barrier, jnp.where(inner, 2 * nb - 1, n_peers - 1))

    @pl.when(jnp.logical_not(inner))
    def _():
        signal(ready, other)

    def q_copy(core, own_core, first):
        return pltpu.make_async_remote_copy(
            src_ref=q_ref.at[pl.ds(pl.multiple_of(core * n_loc + first, 8), n_loc - first), :],
            dst_ref=ex_ref.at[pl.ds(pl.multiple_of(own_core * n_loc + first, 8), n_loc - first), :],
            send_sem=q_send, recv_sem=q_recv.at[own_core], device_id=(dp, partner, core), device_id_type=MESH)

    def late_to(peer):
        plane, core = peer
        return pltpu.make_async_remote_copy(
            src_ref=late_ref.at[me], dst_ref=late_ref.at[me], send_sem=l_send, recv_sem=l_recv,
            device_id=(dp, plane, core), device_id_type=MESH)

    own_v[...] = part_ref[...]

    @pl.when(inner)
    def _():
        for k in CORE_OFFSETS:
            q_copy(lax.rem(tb + k, nb), tb, 0 if k else n_loc // 2).start()

        ex_ref[pl.ds(pl.multiple_of(tb * n_loc, 8), n_loc // 2), :] = head_ref[...]
        q_copy(tb, tb, n_loc // 2).wait_recv()

        @pl.loop(0, nb)
        def _(k):
            core = lax.rem(tb + nb - pick(k, CORE_OFFSETS), nb)
            rows = pl.ds(pl.multiple_of(core * n_loc, 8), n_loc)

            @pl.when(k > 0)
            def _():
                q_copy(core, core, 0).wait_recv()

            p, q, tok = p_ref[rows, :], ex_ref[rows, :], tok_ref[rows, 0:1]
            hit = lax.broadcasted_iota(jnp.int32, (n_loc, vocab), 1) == tok
            excess = jnp.maximum(p - q, 0.0)
            ex_ref[rows, :] = excess
            z = jnp.sum(excess, axis=1, keepdims=True)
            p_pick = jnp.sum(jnp.where(hit, p, 0.0), axis=1, keepdims=True)
            q_pick = jnp.sum(jnp.where(hit, q, 0.0), axis=1, keepdims=True)
            owned = (tok >= 0) & (tok < vocab)
            a = jnp.where(owned, jnp.minimum(1.0, p_pick / jnp.where(owned, q_pick, 1.0)), 0.0)
            first = (partner * nb + core) * n_loc
            own_v[...] += jnp.concatenate([spread(z, seqs, first), spread(a, seqs, first)], axis=0)

    late_ref[me] = own_v[...]

    @pl.when(inner)
    def _():
        sent = q_ref.at[pl.ds(0, nb * n_loc - n_loc // 2), :]
        pltpu.make_async_copy(sent, sent, q_send).wait()
        pl.semaphore_wait(ready, 2 * nb)

    for peer in other + same:
        late_to(peer).start()
    slots = late_ref.at[pl.ds(0, n_peers - 1)]
    pltpu.make_async_copy(slots, slots, l_recv).wait()
    pltpu.make_async_copy(slots, slots, l_send).wait()


SLOTS = 4


def by_position(na, nb, early_ref, which, n_early, seqs):
    n_peers = na * nb
    n_loc = seqs // n_peers
    lane = lax.broadcasted_iota(jnp.int32, (n_peers, 128), 1)
    mine = (lax.broadcasted_iota(jnp.int32, (n_peers, seqs), 1) // n_loc
            == lax.broadcasted_iota(jnp.int32, (n_peers, seqs), 0))
    table = jnp.concatenate(
        [early_ref[g % nb, na * which + g // nb:na * which + g // nb + 1, :] for g in range(n_peers)], axis=0)
    out = jnp.ones((8, seqs), F32)
    for i in range(n_early):
        x = pltpu.roll(table, (128 - n_loc * i) % 128, 1)
        x = jnp.where(lane < n_loc, x, 0.0)
        shift = n_loc
        while shift < 128:
            x = x + pltpu.roll(x, shift, 1)
            shift *= 2
        x = jnp.concatenate([x] * (seqs // 128), axis=1)
        row = jnp.sum(jnp.where(mine, x, 0.0), axis=0, keepdims=True)
        out = jnp.where(lax.broadcasted_iota(jnp.int32, (8, seqs), 0) == i, row, out)
    return out


def early_output_kernel(na, nb, ex_ref, bonus_ref, early_ref, res_ref, bonus_out, order_ref, stage, stage_sem, bonus_sem):
    n_draft, seqs, vocab = ex_ref.shape
    n_early, half = n_draft - 1, seqs // 2
    bonus_copy = pltpu.make_async_copy(bonus_ref, bonus_out, bonus_sem)
    bonus_copy.start()
    order_ref[...] = jnp.zeros_like(order_ref)
    inv = 1.0 / by_position(na, nb, early_ref, 0, n_early, seqs)

    def out_copy(k, slot):
        i, h = k // 2, lax.rem(k, 2)
        return pltpu.make_async_copy(
            stage.at[slot], res_ref.at[i, pl.ds(pl.multiple_of(h * half, half), half), :], stage_sem.at[slot])

    @pl.loop(0, 2 * n_early)
    def _(k):
        i, h, slot = k // 2, lax.rem(k, 2), lax.rem(k, SLOTS)
        row = get_row(inv, i)
        col = to_col(jnp.where(h == 0, row[:, :half], row[:, half:]))

        @pl.when(k >= SLOTS)
        def _():
            out_copy(k - SLOTS, slot).wait()

        @pl.loop(0, vocab // NT)
        def _(t):
            cols = pl.ds(pl.multiple_of(t * NT, NT), NT)
            stage[slot, :, cols] = ex_ref[i, pl.ds(pl.multiple_of(h * half, half), half), cols] * col

        out_copy(k, slot).start()

    for k in range(2 * n_early - SLOTS, 2 * n_early):
        out_copy(k, k % SLOTS).wait()
    bonus_copy.wait()


def late_output_kernel(na, nb, ex_ref, part_ref, early_ref, late_ref, res_in, res_ref, accept_ref, expected_ref,
                       stage, accept_v, expected_v, stage_sem, small_sem):
    n_draft, seqs, vocab = ex_ref.shape
    n_early, block = n_draft - 1, seqs // na
    za = lax.axis_index("tpa")
    inner, partner = (za == 1) | (za == 2), na - 1 - za
    late = late_ref[0]
    for k in range(1, na * nb):
        late += late_ref[k]
    col = to_col(1.0 / late[0:1])

    def out_copy(plane):
        rows = pl.ds(plane * block, block)
        return pltpu.make_async_copy(stage.at[rows], res_ref.at[n_early, rows, :], stage_sem.at[plane])

    for plane in range(na):
        rows, scale = pl.ds(plane * block, block), col[plane * block:(plane + 1) * block]
        from_part = inner & (partner == plane)

        @pl.when(from_part)
        def _():
            @pl.loop(0, vocab // NT)
            def _(t):
                cols = pl.ds(pl.multiple_of(t * NT, NT), NT)
                stage[rows, cols] = part_ref[:, cols] * scale

        @pl.when(jnp.logical_not(from_part))
        def _():
            @pl.loop(0, vocab // NT)
            def _(t):
                cols = pl.ds(pl.multiple_of(t * NT, NT), NT)
                stage[rows, cols] = ex_ref[n_early, rows, cols] * scale

        out_copy(plane).start()

    accept = by_position(na, nb, early_ref, 1, n_early, seqs)
    accept = jnp.where(lax.broadcasted_iota(jnp.int32, accept.shape, 0) == n_early, late[1:2], accept)[:n_draft]
    accept_v[...] = accept
    prod = accept[0:1]
    expected = prod
    for i in range(1, n_draft):
        prod = prod * accept[i:i + 1]
        expected += prod
    expected_v[...] = expected
    small_copies = (pltpu.make_async_copy(accept_v, accept_ref, small_sem.at[0]),
                    pltpu.make_async_copy(expected_v, expected_ref, small_sem.at[1]))
    for copy in small_copies:
        copy.start()
    for plane in range(na):
        out_copy(plane).wait()
    for copy in small_copies:
        copy.wait()


def solution(mesh):
    na, nb = mesh.shape["tpa"], mesh.shape["tpb"]
    n_peers = na * nb
    any_spec = pl.BlockSpec(memory_space=pl.ANY)
    vmem_spec = pl.BlockSpec(memory_space=pltpu.VMEM)

    def local_step(hidden, w_head, q_draft, x_draft):
        seqs, n_pos, depth = hidden.shape
        vocab = w_head.shape[1]
        n_loc, n_draft, _ = q_draft.shape
        dims = (n_pos, seqs, depth, vocab, n_loc, na, nb)
        dma = pltpu.SemaphoreType.DMA
        small = pltpu.VMEM((4, 8, 128), F32)
        q_rows = q_draft.transpose(1, 0, 2)
        block = seqs // na
        ex, bonus, early, late_part, part_p, part_q, part_head, part_tok = pl.pallas_call(
            functools.partial(exchange_kernel, dims),
            out_shape=(pltpu.VMEM((n_draft, seqs, vocab), F32), pltpu.VMEM((seqs, vocab), F32), small,
                       pltpu.VMEM((2, seqs), F32), pltpu.VMEM((block, vocab), F32), pltpu.VMEM((block, vocab), F32),
                       pltpu.VMEM((n_loc // 2, vocab), F32), pltpu.VMEM((block, 128), jnp.int32)),
            in_specs=[any_spec] * 4,
            out_specs=(vmem_spec,) * 8,
            scratch_shapes=[
                pltpu.VMEM((n_pos, seqs, depth), jnp.bfloat16),
                pltpu.VMEM((2, depth, NT), jnp.bfloat16),
                pltpu.VMEM((n_pos, seqs, vocab), F32),
                pltpu.VMEM((n_draft, seqs), jnp.int32),
                pltpu.VMEM((n_draft, seqs, 128), jnp.int32),
                small, small, small, small, small, small, small,
                dma, dma((2,)), dma, dma, dma((nb,)), pltpu.SemaphoreType.REGULAR, dma, dma((na,)), dma, dma((n_peers,)),
            ] + [dma] * 14,
            compiler_params=pltpu.CompilerParams(collective_id=0, has_side_effects=True, vmem_limit_bytes=38 * 2**20),
            name="exchange",
        )(hidden.transpose(1, 0, 2), w_head, q_rows, x_draft.T)
        res, bonus_out, order = pl.pallas_call(
            functools.partial(early_output_kernel, na, nb),
            out_shape=(jax.ShapeDtypeStruct((n_draft, seqs, vocab), F32), jax.ShapeDtypeStruct((seqs, vocab), F32),
                       pltpu.VMEM((8, 128), F32)),
            in_specs=[vmem_spec] * 3,
            out_specs=(any_spec, any_spec, vmem_spec),
            scratch_shapes=[pltpu.VMEM((SLOTS, seqs // 2, vocab), F32), dma((SLOTS,)), dma],
            compiler_params=pltpu.CompilerParams(vmem_limit_bytes=12 * 2**20),
            name="early_output",
        )(ex, bonus, early)
        part, late = pl.pallas_call(
            functools.partial(last_kernel, (n_draft, seqs, vocab, n_loc, na, nb)),
            out_shape=(pltpu.VMEM((block, vocab), F32), pltpu.VMEM((n_peers, 2, seqs), F32)),
            in_specs=[vmem_spec] * 6,
            out_specs=(vmem_spec, vmem_spec),
            scratch_shapes=[pltpu.VMEM((2, seqs), F32), pltpu.SemaphoreType.REGULAR, dma, dma((nb,)), dma, dma],
            compiler_params=pltpu.CompilerParams(collective_id=1, has_side_effects=True, vmem_limit_bytes=28 * 2**20),
            name="last",
        )(part_q, part_head, part_p, part_tok, late_part, order)
        res, accept, expected = pl.pallas_call(
            functools.partial(late_output_kernel, na, nb),
            out_shape=(jax.ShapeDtypeStruct((n_draft, seqs, vocab), F32), jax.ShapeDtypeStruct((n_draft, seqs), F32),
                       jax.ShapeDtypeStruct((1, seqs), F32)),
            in_specs=[vmem_spec] * 4 + [any_spec],
            out_specs=(any_spec,) * 3,
            scratch_shapes=[pltpu.VMEM((seqs, vocab), F32), pltpu.VMEM((n_draft, seqs), F32), pltpu.VMEM((1, seqs), F32),
                            dma((na,)), dma((2,))],
            input_output_aliases={4: 0},
            compiler_params=pltpu.CompilerParams(vmem_limit_bytes=12 * 2**20),
            name="late_output",
        )(ex, part, early, late, res)
        return accept.T, expected.reshape(seqs), res.transpose(1, 0, 2), bonus_out

    return jax.shard_map(
        local_step, mesh=mesh,
        in_specs=(P("dp", None, None), P(None, VOCAB_AXES), P(("dp",) + VOCAB_AXES, None, None), P("dp", None)),
        out_specs=(P("dp", None), P("dp"), P("dp", None, VOCAB_AXES), P("dp", VOCAB_AXES)),
        check_vma=False)
```

```python
import functools

import jax
import jax.numpy as jnp
from jax import lax
from jax.experimental import pallas as pl
from jax.experimental.pallas import tpu as pltpu
from jax.sharding import PartitionSpec as P

INV_TEMP = 1.25
VOCAB_AXES = ("tpa", "tpb")
MESH = pl.DeviceIdType.MESH
F32 = jnp.float32
SEND = ((3, 3, 0, 0), (1, 0, 3, 2), (2, 2, 1, 1))
RECV = ((3, 0, 3, 0), (2, 3, 0, 1), (1, 2, 1, 2))
LAST_RECV = ((1, 0, 3, 2), (2, 3, 0, 1))
CORE_OFFSETS = (0, 2, 1, 3)
NT = 512


def pick(index, values):
    out = jnp.int32(values[-1])
    for k in range(len(values) - 2, -1, -1):
        out = jnp.where(index == k, jnp.int32(values[k]), out)
    return out


def diag(n):
    return lax.broadcasted_iota(jnp.int32, (n, n), 0) == lax.broadcasted_iota(jnp.int32, (n, n), 1)


def to_col(row):
    return jnp.sum(jnp.where(diag(row.shape[1]), row, 0.0), axis=1, keepdims=True)


def get_row(rows, i):
    return jnp.sum(jnp.where(lax.broadcasted_iota(jnp.int32, rows.shape, 0) == i, rows, 0.0), axis=0, keepdims=True)


def lanes(n, first, rows):
    return (lax.broadcasted_iota(jnp.int32, (rows, n), 1)
            == lax.broadcasted_iota(jnp.int32, (rows, n), 0) + first)


def spread(col, n, first):
    return jnp.sum(jnp.where(lanes(n, first, col.shape[0]), col, 0.0), axis=0, keepdims=True)


def gather(row, first, rows):
    return jnp.sum(jnp.where(lanes(row.shape[1], first, rows), row, 0.0), axis=1, keepdims=True)


def exchange_kernel(dims, hid_ref, w_ref, q_ref, x_ref, ex_ref, bonus_ref, early_ref, late_ref, part_p_ref, part_q_ref, part_head_ref, part_tok_ref,
                    hid_v, w_v, z_v, x_v, tok_v, stat_out, stat_1, stat_2, norm_v, sum_out, sum_1, sum_2, hid_sem, w_sem, own_sem, x_sem, part_sem,
                    ready, q_send, q_recv, r_send, r_recv, h_send, h_recv,
                    a1_send, a1_recv, a2_send, a2_recv, a3_send, a3_recv, b1_send, b1_recv, b2_send, b2_recv, b3_send, b3_recv):
    n_pos, seqs, depth, vocab, n_loc, na, nb = dims
    n_draft = n_pos - 1
    n_early = n_draft - 1
    n_peers = na * nb
    n_tiles = vocab // NT
    others = range(n_peers - 1)
    dp, za, tb = lax.axis_index("dp"), lax.axis_index("tpa"), lax.axis_index("tpb")
    me = za * nb + tb

    inner = (za == 1) | (za == 2)

    def choose(end, mid):
        return [(jnp.where(inner, m[0], e[0]), lax.rem(tb + jnp.where(inner, m[1], e[1]), nb)) for e, m in zip(end, mid)]

    own = [(za, k) for k in range(1, nb)]
    steps = [[(pick(za, SEND[step]), CORE_OFFSETS[k]) for k in range(nb)] for step in range(3)]
    first_order = choose(steps[0] + steps[1] + steps[2] + own, steps[2][:1] + own + steps[0] + steps[1] + steps[2][1:])
    last_order = choose(steps[1] + own + steps[2] + steps[0], own + steps[1] + steps[0] + steps[2])

    def recv_peer(k):
        step, off = (k - 3) // nb, lax.rem(jnp.int32(k) + 1, nb)
        plane = jnp.where(k < 3, za, jnp.where(step == 0, pick(za, LAST_RECV[0]),
                          jnp.where(step == 1, pick(za, LAST_RECV[1]), na - 1 - za)))
        off = jnp.where(k < 3, k + 1, nb - pick(off, CORE_OFFSETS))
        return plane, lax.rem(tb + off, nb)

    def rows_of(group):
        return pl.ds(pl.multiple_of(group * n_loc, 8), n_loc)

    def q_copy(part, plane, core, own_group, column, send=q_send):
        i0, ni = (0, n_early) if part == 0 else (n_early, 1)
        recv = q_recv.at[own_group // nb] if part == 0 else r_recv.at[own_group]
        return pltpu.make_async_remote_copy(
            src_ref=q_ref.at[pl.ds(i0, ni), :, pl.ds(pl.multiple_of(column * vocab, 128), vocab)],
            dst_ref=ex_ref.at[pl.ds(i0, ni), rows_of(own_group), :],
            send_sem=send, recv_sem=recv,
            device_id=(dp, plane, core), device_id_type=MESH)

    def q_to(part, k):
        plane, core = (first_order, last_order)[part][k]
        return q_copy(part, plane, core, me, plane * nb + core, r_send if (part, k) >= (1, 11) else q_send)

    def q_from_plane(plane, count):
        rows = ex_ref.at[pl.ds(0, n_early), pl.ds(0, count * n_loc), :]
        pltpu.make_async_copy(rows, rows, q_recv.at[plane]).wait()

    def q_from(group):
        return q_copy(1, za, tb, group, 0)

    def small(src, dst, send, recv, src_slot, dst_slot, plane, core):
        return pltpu.make_async_remote_copy(
            src_ref=src.at[src_slot], dst_ref=dst.at[dst_slot], send_sem=send, recv_sem=recv,
            device_id=(dp, plane, core), device_id_type=MESH)

    def await_slots(ref, sem, count):
        part = ref.at[pl.ds(0, count)]
        pltpu.make_async_copy(part, part, sem).wait()

    def in_plane(src, dst, send, recv, scatter):
        cores = [lax.rem(tb + k, nb) for k in range(1, nb)]
        return [small(src, dst, send, recv, core if scatter else tb, tb, za, core) for core in cores]

    def across(ref, send, recv):
        planes = [lax.rem(za + k, na) for k in range(1, na)]
        return [small(ref, ref, send, recv, za, za, plane, tb) for plane in planes]

    def start(copies):
        for copy in copies:
            copy.start()

    def combine(ref):
        top = ref[0, 0:4]
        for k in range(1, 4):
            top = jnp.maximum(top, ref[k, 0:4])
        total = ref[0, 4:8] * jnp.exp(ref[0, 0:4] - top)
        for k in range(1, 4):
            total += ref[k, 4:8] * jnp.exp(ref[k, 0:4] - top)
        return top, total

    def add(ref):
        return (ref[0] + ref[1]) + (ref[2] + ref[3])

    def put(tile, plane, first, second):
        row = lax.broadcasted_iota(jnp.int32, tile.shape, 0)
        return jnp.where(row == plane, first, jnp.where(row == na + plane, second, tile))

    def w_copy(tile, slot):
        return pltpu.make_async_copy(w_ref.at[:, pl.ds(pl.multiple_of(tile * NT, NT), NT)], w_v.at[slot], w_sem.at[slot])

    hid_copy = pltpu.make_async_copy(hid_ref, hid_v, hid_sem)
    part_copies = [pltpu.make_async_copy(
        q_ref.at[n_early, :, pl.ds(pl.multiple_of(((na - 1 - za) * nb + core) * vocab, 128), vocab)],
        part_q_ref.at[pl.ds(core * n_loc, n_loc), :], part_sem.at[core]) for core in range(nb)]
    x_copy = pltpu.make_async_copy(x_ref, x_v, x_sem)
    own_copy = pltpu.make_async_copy(
        q_ref.at[:, :, pl.ds(pl.multiple_of(me * vocab, 128), vocab)], ex_ref.at[:, rows_of(me), :], own_sem)

    def signal(sem, peers):
        for plane, core in peers:
            pl.semaphore_signal(sem, inc=1, device_id=(dp, plane, core), device_id_type=MESH)

    partner = na - 1 - za
    own_plane = [(za, lax.rem(tb + k, nb)) for k in range(1, nb)]
    partner_plane = [(partner, lax.rem(tb + k, nb)) for k in range(nb)]
    other_planes = [(plane, lax.rem(tb + k, nb)) for plane in (jnp.where(inner, 0, 1), jnp.where(inner, 3, 2)) for k in range(nb)]

    barrier = pltpu.get_barrier_semaphore()

    @pl.when(inner)
    def _():
        signal(barrier, [(partner, tb)] + other_planes)

    @pl.when(jnp.logical_not(inner))
    def _():
        signal(barrier, partner_plane + own_plane)

    pl.semaphore_wait(barrier, jnp.where(inner, 1, n_peers - 1))
    q_to(0, 0).start()

    @pl.when(jnp.logical_not(inner))
    def _():
        for k in range(1, 4):
            q_to(0, k).start()
        signal(ready, other_planes)

    x_copy.start()
    for copy in part_copies:
        copy.start()
    hid_copy.start()
    w_copy(0, 0).start()
    own_copy.start()

    @pl.when(inner)
    def _():
        pl.semaphore_wait(ready, 2 * nb)
        for k in range(1, 4):
            q_to(0, k).start()

    x_copy.wait()
    tok_rows = x_v[...].astype(F32)
    for i in range(n_draft):
        tok_v[i] = jnp.broadcast_to(to_col(tok_rows[i:i + 1]), (seqs, 128)).astype(jnp.int32) - me * vocab
    hid_copy.wait()
    for copy in part_copies:
        copy.wait()

    @pl.loop(0, n_tiles)
    def _(tile):
        slot = lax.rem(tile, 2)
        w_copy(tile, slot).wait()

        @pl.when(tile + 1 < n_tiles)
        def _():
            w_copy(tile + 1, 1 - slot).start()

        @pl.loop(0, n_pos)
        def _(i):
            z_v[i, :, pl.ds(pl.multiple_of(tile * NT, NT), NT)] = INV_TEMP * jnp.dot(
                hid_v[i], w_v[slot], preferred_element_type=F32)

    @pl.loop(0, nb)
    def _(core):
        def plane_rows(plane, tile):
            def one(i, rows):
                z = z_v[i, rows_of(plane * nb + core), :]
                m = jnp.max(z, axis=1, keepdims=True)
                s = jnp.sum(jnp.exp(z - m), axis=1, keepdims=True)
                return rows[0] + spread(m, 128, i * n_loc), rows[1] + spread(s, 128, i * n_loc)

            zero = jnp.zeros((1, 128), F32)
            return put(tile, plane, *lax.fori_loop(0, n_pos, one, (zero, zero)))

        stat_out[core] = lax.fori_loop(0, na, plane_rows, jnp.zeros((8, 128), F32))

    stat_1[tb] = stat_out[tb]
    start(in_plane(stat_out, stat_1, a1_send, a1_recv, True))
    await_slots(stat_1, a1_recv, 3)
    stat_2[za] = jnp.concatenate(combine(stat_1), axis=0)
    start(across(stat_2, a2_send, a2_recv))
    for k in (4, 5):
        q_to(0, k).start()
    await_slots(stat_2, a2_recv, 3)
    top, total = combine(stat_2)
    used = lax.broadcasted_iota(jnp.int32, (4, 128), 1) < n_pos * n_loc
    norm_v[tb] = jnp.concatenate([top, 1.0 / jnp.where(used, total, 1.0)], axis=0)
    start(in_plane(norm_v, norm_v, a3_send, a3_recv, False))
    for k in range(6, 15):
        q_to(0, k).start()
    for k in range(10):
        q_to(1, k).start()

    @pl.when(jnp.logical_not(inner))
    def _():
        q_to(1, 10).start()

    await_slots(norm_v, a3_recv, 3)

    def probs(i, group):
        norm, plane = norm_v[lax.rem(group, nb)], group // nb
        m = gather(get_row(norm, plane), i * n_loc, n_loc)
        r = gather(get_row(norm, na + plane), i * n_loc, n_loc)
        return jnp.exp(z_v[i, rows_of(group), :] - m) * r

    @pl.loop(0, n_peers)
    def _(group):
        bonus_ref[rows_of(group), :] = probs(n_draft, group)

    def cell(i, group):
        rows = rows_of(group)
        p, q, tok = probs(i, group), ex_ref[i, rows, :], tok_v[i, rows, 0:1]
        hit = lax.broadcasted_iota(jnp.int32, (n_loc, vocab), 1) == tok
        p_pick = jnp.sum(jnp.where(hit, p, 0.0), axis=1, keepdims=True)
        q_pick = jnp.sum(jnp.where(hit, q, 0.0), axis=1, keepdims=True)
        excess = jnp.maximum(p - q, 0.0)
        ex_ref[i, rows, :] = excess
        owned = (tok >= 0) & (tok < vocab)
        accept = jnp.where(owned, jnp.minimum(1.0, p_pick / jnp.where(owned, q_pick, 1.0)), 0.0)
        return jnp.sum(excess, axis=1, keepdims=True), accept

    def absorb_early(group):
        def one(i, rows):
            z, a = cell(i, group)
            return rows[0] + spread(z, 128, i * n_loc), rows[1] + spread(a, 128, i * n_loc)

        zero = jnp.zeros((1, 128), F32)
        z_row, a_row = lax.fori_loop(0, n_early, one, (zero, zero))
        core = lax.rem(group, nb)
        sum_out[core] = put(sum_out[core], group // nb, z_row, a_row)

    sum_out[...] = jnp.zeros_like(sum_out)
    own_copy.wait()
    absorb_early(me)

    q_from_plane(za, nb - 1)
    for k in range(1, nb):
        absorb_early(za * nb + lax.rem(tb + k, nb))

    @pl.loop(0, na - 1)
    def _(step):
        plane = jnp.where(step == 0, pick(za, RECV[0]), jnp.where(step == 1, pick(za, RECV[1]), pick(za, RECV[2])))
        q_from_plane(plane, nb)

        @pl.loop(0, nb)
        def _(core):
            absorb_early(plane * nb + core)

    sum_1[tb] = sum_out[tb]
    start(in_plane(sum_out, sum_1, b1_send, b1_recv, True))
    await_slots(sum_1, b1_recv, 3)
    sum_2[za] = add(sum_1)
    start(across(sum_2, b2_send, b2_recv))

    head = pltpu.make_async_remote_copy(
        src_ref=q_ref.at[n_early, pl.ds(0, n_loc // 2), pl.ds(pl.multiple_of((partner * nb + tb) * vocab, 128), vocab)],
        dst_ref=part_head_ref, send_sem=h_send, recv_sem=h_recv, device_id=(dp, partner, tb), device_id_type=MESH)

    @pl.when(inner)
    def _():
        q_to(1, 10).start()
        head.start()

    @pl.loop(0, nb)
    def _(core):
        group = partner * nb + core
        part_p_ref[pl.ds(pl.multiple_of(core * n_loc, 8), n_loc), :] = probs(n_early, group)
        part_tok_ref[pl.ds(pl.multiple_of(core * n_loc, 8), n_loc), :] = tok_v[n_early, rows_of(group), :]

    def absorb_late(group):
        z, a = cell(n_early, group)
        late_ref[...] += jnp.concatenate([spread(z, seqs, group * n_loc), spread(a, seqs, group * n_loc)], axis=0)

    def arrived(k):
        plane, core = recv_peer(k)
        q_from(plane * nb + core).wait_recv()
        absorb_late(plane * nb + core)

    late_ref[...] = jnp.zeros_like(late_ref)
    absorb_late(me)
    pl.loop(0, 10)(arrived)

    plane, core = recv_peer(10)
    q_from(plane * nb + core).wait_recv()

    @pl.when(jnp.logical_not(inner))
    def _():
        for k in range(11, 15):
            q_to(1, k).start()

    absorb_late(plane * nb + core)
    await_slots(sum_2, b2_recv, 3)
    early_ref[tb] = add(sum_2)
    start(in_plane(early_ref, early_ref, b3_send, b3_recv, False))

    @pl.when(inner)
    def _():
        head.wait()

    @pl.when(jnp.logical_not(inner))
    def _():
        pl.loop(11, 15)(arrived)
        sent = q_ref.at[0:4, :, pl.ds(0, vocab)]
        pltpu.make_async_copy(sent, sent, r_send).wait()

    await_slots(early_ref, b3_recv, 3)
    slices = (n_peers - 1) * n_early + 11
    sent = q_ref.at[:, :, pl.ds(0, slices * vocab // n_draft)]
    pltpu.make_async_copy(sent, sent, q_send).wait()
    for ref, sem in ((stat_1, a1_send), (stat_2, a2_send), (norm_v, a3_send), (sum_1, b1_send), (sum_2, b2_send),
                     (early_ref, b3_send)):
        await_slots(ref, sem, 3)


def last_kernel(dims, q_ref, head_ref, p_ref, tok_ref, part_ref, order_ref, ex_ref, late_ref, own_v, ready, q_send, q_recv, l_send, l_recv):
    n_draft, seqs, vocab, n_loc, na, nb = dims
    n_peers = na * nb
    dp, za, tb = lax.axis_index("dp"), lax.axis_index("tpa"), lax.axis_index("tpb")
    me, partner = za * nb + tb, na - 1 - za
    inner = (za == 1) | (za == 2)
    same = [(za, lax.rem(tb + k, nb)) for k in range(1, nb)] + [(partner, lax.rem(tb + k, nb)) for k in range(nb)]
    other_planes = (jnp.where(inner, 0, 1), jnp.where(inner, 3, 2))
    other = [(plane, lax.rem(tb + k, nb)) for plane in other_planes for k in range(nb)]

    def signal(sem, peers):
        for plane, core in peers:
            pl.semaphore_signal(sem, inc=1, device_id=(dp, plane, core), device_id_type=MESH)

    barrier = pltpu.get_barrier_semaphore()
    signal(barrier, same)

    @pl.when(inner)
    def _():
        signal(barrier, other)

    pl.semaphore_wait(barrier, jnp.where(inner, 2 * nb - 1, n_peers - 1))

    @pl.when(jnp.logical_not(inner))
    def _():
        signal(ready, other)

    def q_copy(core, own_core, first):
        return pltpu.make_async_remote_copy(
            src_ref=q_ref.at[pl.ds(pl.multiple_of(core * n_loc + first, 8), n_loc - first), :],
            dst_ref=ex_ref.at[pl.ds(pl.multiple_of(own_core * n_loc + first, 8), n_loc - first), :],
            send_sem=q_send, recv_sem=q_recv.at[own_core], device_id=(dp, partner, core), device_id_type=MESH)

    def late_to(peer):
        plane, core = peer
        return pltpu.make_async_remote_copy(
            src_ref=late_ref.at[me], dst_ref=late_ref.at[me], send_sem=l_send, recv_sem=l_recv,
            device_id=(dp, plane, core), device_id_type=MESH)

    own_v[...] = part_ref[...]

    @pl.when(inner)
    def _():
        for k in CORE_OFFSETS:
            q_copy(lax.rem(tb + k, nb), tb, 0 if k else n_loc // 2).start()

        ex_ref[pl.ds(pl.multiple_of(tb * n_loc, 8), n_loc // 2), :] = head_ref[...]
        q_copy(tb, tb, n_loc // 2).wait_recv()

        @pl.loop(0, nb)
        def _(k):
            core = lax.rem(tb + nb - pick(k, CORE_OFFSETS), nb)
            rows = pl.ds(pl.multiple_of(core * n_loc, 8), n_loc)

            @pl.when(k > 0)
            def _():
                q_copy(core, core, 0).wait_recv()

            p, q, tok = p_ref[rows, :], ex_ref[rows, :], tok_ref[rows, 0:1]
            hit = lax.broadcasted_iota(jnp.int32, (n_loc, vocab), 1) == tok
            excess = jnp.maximum(p - q, 0.0)
            ex_ref[rows, :] = excess
            z = jnp.sum(excess, axis=1, keepdims=True)
            p_pick = jnp.sum(jnp.where(hit, p, 0.0), axis=1, keepdims=True)
            q_pick = jnp.sum(jnp.where(hit, q, 0.0), axis=1, keepdims=True)
            owned = (tok >= 0) & (tok < vocab)
            a = jnp.where(owned, jnp.minimum(1.0, p_pick / jnp.where(owned, q_pick, 1.0)), 0.0)
            first = (partner * nb + core) * n_loc
            own_v[...] += jnp.concatenate([spread(z, seqs, first), spread(a, seqs, first)], axis=0)

    late_ref[me] = own_v[...]

    @pl.when(inner)
    def _():
        sent = q_ref.at[pl.ds(0, nb * n_loc - n_loc // 2), :]
        pltpu.make_async_copy(sent, sent, q_send).wait()
        pl.semaphore_wait(ready, 2 * nb)

    for peer in other + same:
        late_to(peer).start()
    slots = late_ref.at[pl.ds(0, n_peers - 1)]
    pltpu.make_async_copy(slots, slots, l_recv).wait()
    pltpu.make_async_copy(slots, slots, l_send).wait()


SLOTS = 4


def by_position(na, nb, early_ref, which, n_early, seqs):
    n_peers = na * nb
    n_loc = seqs // n_peers
    lane = lax.broadcasted_iota(jnp.int32, (n_peers, 128), 1)
    mine = (lax.broadcasted_iota(jnp.int32, (n_peers, seqs), 1) // n_loc
            == lax.broadcasted_iota(jnp.int32, (n_peers, seqs), 0))
    table = jnp.concatenate(
        [early_ref[g % nb, na * which + g // nb:na * which + g // nb + 1, :] for g in range(n_peers)], axis=0)
    out = jnp.ones((8, seqs), F32)
    for i in range(n_early):
        x = pltpu.roll(table, (128 - n_loc * i) % 128, 1)
        x = jnp.where(lane < n_loc, x, 0.0)
        shift = n_loc
        while shift < 128:
            x = x + pltpu.roll(x, shift, 1)
            shift *= 2
        x = jnp.concatenate([x] * (seqs // 128), axis=1)
        row = jnp.sum(jnp.where(mine, x, 0.0), axis=0, keepdims=True)
        out = jnp.where(lax.broadcasted_iota(jnp.int32, (8, seqs), 0) == i, row, out)
    return out


def early_output_kernel(na, nb, ex_ref, bonus_ref, early_ref, res_ref, bonus_out, order_ref, stage, stage_sem, bonus_sem):
    n_draft, seqs, vocab = ex_ref.shape
    n_early, half = n_draft - 1, seqs // 2
    bonus_copy = pltpu.make_async_copy(bonus_ref, bonus_out, bonus_sem)
    bonus_copy.start()
    order_ref[...] = jnp.zeros_like(order_ref)
    inv = 1.0 / by_position(na, nb, early_ref, 0, n_early, seqs)

    def out_copy(k, slot):
        i, h = k // 2, lax.rem(k, 2)
        return pltpu.make_async_copy(
            stage.at[slot], res_ref.at[i, pl.ds(pl.multiple_of(h * half, half), half), :], stage_sem.at[slot])

    @pl.loop(0, 2 * n_early)
    def _(k):
        i, h, slot = k // 2, lax.rem(k, 2), lax.rem(k, SLOTS)
        row = get_row(inv, i)
        col = to_col(jnp.where(h == 0, row[:, :half], row[:, half:]))

        @pl.when(k >= SLOTS)
        def _():
            out_copy(k - SLOTS, slot).wait()

        @pl.loop(0, vocab // NT)
        def _(t):
            cols = pl.ds(pl.multiple_of(t * NT, NT), NT)
            stage[slot, :, cols] = ex_ref[i, pl.ds(pl.multiple_of(h * half, half), half), cols] * col

        out_copy(k, slot).start()

    for k in range(2 * n_early - SLOTS, 2 * n_early):
        out_copy(k, k % SLOTS).wait()
    bonus_copy.wait()


def late_output_kernel(na, nb, ex_ref, part_ref, early_ref, late_ref, res_in, res_ref, accept_ref, expected_ref,
                       stage, accept_v, expected_v, stage_sem, small_sem):
    n_draft, seqs, vocab = ex_ref.shape
    n_early, block = n_draft - 1, seqs // na
    za = lax.axis_index("tpa")
    inner, partner = (za == 1) | (za == 2), na - 1 - za
    late = late_ref[0]
    for k in range(1, na * nb):
        late += late_ref[k]
    col = to_col(1.0 / late[0:1])

    def out_copy(plane):
        rows = pl.ds(plane * block, block)
        return pltpu.make_async_copy(stage.at[rows], res_ref.at[n_early, rows, :], stage_sem.at[plane])

    for plane in range(na):
        rows, scale = pl.ds(plane * block, block), col[plane * block:(plane + 1) * block]
        from_part = inner & (partner == plane)

        @pl.when(from_part)
        def _():
            @pl.loop(0, vocab // NT)
            def _(t):
                cols = pl.ds(pl.multiple_of(t * NT, NT), NT)
                stage[rows, cols] = part_ref[:, cols] * scale

        @pl.when(jnp.logical_not(from_part))
        def _():
            @pl.loop(0, vocab // NT)
            def _(t):
                cols = pl.ds(pl.multiple_of(t * NT, NT), NT)
                stage[rows, cols] = ex_ref[n_early, rows, cols] * scale

        out_copy(plane).start()

    accept = by_position(na, nb, early_ref, 1, n_early, seqs)
    accept = jnp.where(lax.broadcasted_iota(jnp.int32, accept.shape, 0) == n_early, late[1:2], accept)[:n_draft]
    accept_v[...] = accept
    prod = accept[0:1]
    expected = prod
    for i in range(1, n_draft):
        prod = prod * accept[i:i + 1]
        expected += prod
    expected_v[...] = expected
    small_copies = (pltpu.make_async_copy(accept_v, accept_ref, small_sem.at[0]),
                    pltpu.make_async_copy(expected_v, expected_ref, small_sem.at[1]))
    for copy in small_copies:
        copy.start()
    for plane in range(na):
        out_copy(plane).wait()
    for copy in small_copies:
        copy.wait()


def solution(mesh):
    na, nb = mesh.shape["tpa"], mesh.shape["tpb"]
    n_peers = na * nb
    any_spec = pl.BlockSpec(memory_space=pl.ANY)
    vmem_spec = pl.BlockSpec(memory_space=pltpu.VMEM)

    def local_step(hidden, w_head, q_draft, x_draft):
        seqs, n_pos, depth = hidden.shape
        vocab = w_head.shape[1]
        n_loc, n_draft, _ = q_draft.shape
        dims = (n_pos, seqs, depth, vocab, n_loc, na, nb)
        dma = pltpu.SemaphoreType.DMA
        small = pltpu.VMEM((4, 8, 128), F32)
        q_rows = q_draft.transpose(1, 0, 2)
        block = seqs // na
        ex, bonus, early, late_part, part_p, part_q, part_head, part_tok = pl.pallas_call(
            functools.partial(exchange_kernel, dims),
            out_shape=(pltpu.VMEM((n_draft, seqs, vocab), F32), pltpu.VMEM((seqs, vocab), F32), small,
                       pltpu.VMEM((2, seqs), F32), pltpu.VMEM((block, vocab), F32), pltpu.VMEM((block, vocab), F32),
                       pltpu.VMEM((n_loc // 2, vocab), F32), pltpu.VMEM((block, 128), jnp.int32)),
            in_specs=[any_spec] * 4,
            out_specs=(vmem_spec,) * 8,
            scratch_shapes=[
                pltpu.VMEM((n_pos, seqs, depth), jnp.bfloat16),
                pltpu.VMEM((2, depth, NT), jnp.bfloat16),
                pltpu.VMEM((n_pos, seqs, vocab), F32),
                pltpu.VMEM((n_draft, seqs), jnp.int32),
                pltpu.VMEM((n_draft, seqs, 128), jnp.int32),
                small, small, small, small, small, small, small,
                dma, dma((2,)), dma, dma, dma((nb,)), pltpu.SemaphoreType.REGULAR, dma, dma((na,)), dma, dma((n_peers,)),
            ] + [dma] * 14,
            compiler_params=pltpu.CompilerParams(collective_id=0, has_side_effects=True, vmem_limit_bytes=38 * 2**20),
            name="exchange",
        )(hidden.transpose(1, 0, 2), w_head, q_rows, x_draft.T)
        res, bonus_out, order = pl.pallas_call(
            functools.partial(early_output_kernel, na, nb),
            out_shape=(jax.ShapeDtypeStruct((n_draft, seqs, vocab), F32), jax.ShapeDtypeStruct((seqs, vocab), F32),
                       pltpu.VMEM((8, 128), F32)),
            in_specs=[vmem_spec] * 3,
            out_specs=(any_spec, any_spec, vmem_spec),
            scratch_shapes=[pltpu.VMEM((SLOTS, seqs // 2, vocab), F32), dma((SLOTS,)), dma],
            compiler_params=pltpu.CompilerParams(vmem_limit_bytes=12 * 2**20),
            name="early_output",
        )(ex, bonus, early)
        part, late = pl.pallas_call(
            functools.partial(last_kernel, (n_draft, seqs, vocab, n_loc, na, nb)),
            out_shape=(pltpu.VMEM((block, vocab), F32), pltpu.VMEM((n_peers, 2, seqs), F32)),
            in_specs=[vmem_spec] * 6,
            out_specs=(vmem_spec, vmem_spec),
            scratch_shapes=[pltpu.VMEM((2, seqs), F32), pltpu.SemaphoreType.REGULAR, dma, dma((nb,)), dma, dma],
            compiler_params=pltpu.CompilerParams(collective_id=1, has_side_effects=True, vmem_limit_bytes=28 * 2**20),
            name="last",
        )(part_q, part_head, part_p, part_tok, late_part, order)
        res, accept, expected = pl.pallas_call(
            functools.partial(late_output_kernel, na, nb),
            out_shape=(jax.ShapeDtypeStruct((n_draft, seqs, vocab), F32), jax.ShapeDtypeStruct((n_draft, seqs), F32),
                       jax.ShapeDtypeStruct((1, seqs), F32)),
            in_specs=[vmem_spec] * 4 + [any_spec],
            out_specs=(any_spec,) * 3,
            scratch_shapes=[pltpu.VMEM((seqs, vocab), F32), pltpu.VMEM((n_draft, seqs), F32), pltpu.VMEM((1, seqs), F32),
                            dma((na,)), dma((2,))],
            input_output_aliases={4: 0},
            compiler_params=pltpu.CompilerParams(vmem_limit_bytes=12 * 2**20),
            name="late_output",
        )(ex, part, early, late, res)
        return accept.T, expected.reshape(seqs), res.transpose(1, 0, 2), bonus_out

    return jax.shard_map(
        local_step, mesh=mesh,
        in_specs=(P("dp", None, None), P(None, VOCAB_AXES), P(("dp",) + VOCAB_AXES, None, None), P("dp", None)),
        out_specs=(P("dp", None), P("dp"), P("dp", None, VOCAB_AXES), P("dp", VOCAB_AXES)),
        check_vma=False)
```

```python
import functools

import jax
import jax.numpy as jnp
from jax import lax
from jax.experimental import pallas as pl
from jax.experimental.pallas import tpu as pltpu
from jax.sharding import PartitionSpec as P

INV_TEMP = 1.25
VOCAB_AXES = ("tpa", "tpb")
MESH = pl.DeviceIdType.MESH
F32 = jnp.float32
SEND = ((3, 3, 0, 0), (1, 0, 3, 2), (2, 2, 1, 1))
RECV = ((3, 0, 3, 0), (2, 3, 0, 1), (1, 2, 1, 2))
LAST_RECV = ((1, 0, 3, 2), (2, 3, 0, 1))
CORE_OFFSETS = (0, 2, 1, 3)
NT = 512


def pick(index, values):
    out = jnp.int32(values[-1])
    for k in range(len(values) - 2, -1, -1):
        out = jnp.where(index == k, jnp.int32(values[k]), out)
    return out


def diag(n):
    return lax.broadcasted_iota(jnp.int32, (n, n), 0) == lax.broadcasted_iota(jnp.int32, (n, n), 1)


def to_col(row):
    return jnp.sum(jnp.where(diag(row.shape[1]), row, 0.0), axis=1, keepdims=True)


def get_row(rows, i):
    return jnp.sum(jnp.where(lax.broadcasted_iota(jnp.int32, rows.shape, 0) == i, rows, 0.0), axis=0, keepdims=True)


def lanes(n, first, rows):
    return (lax.broadcasted_iota(jnp.int32, (rows, n), 1)
            == lax.broadcasted_iota(jnp.int32, (rows, n), 0) + first)


def spread(col, n, first):
    return jnp.sum(jnp.where(lanes(n, first, col.shape[0]), col, 0.0), axis=0, keepdims=True)


def gather(row, first, rows):
    return jnp.sum(jnp.where(lanes(row.shape[1], first, rows), row, 0.0), axis=1, keepdims=True)


def exchange_kernel(dims, hid_ref, w_ref, q_ref, x_ref, ex_ref, bonus_ref, early_ref, late_ref, part_p_ref, part_q_ref, part_head_ref, part_tok_ref,
                    hid_v, w_v, z_v, x_v, tok_v, stat_out, stat_1, stat_2, norm_v, sum_out, sum_1, sum_2, hid_sem, w_sem, own_sem, x_sem, part_sem,
                    ready, q_send, q_recv, r_send, r_recv, h_send, h_recv,
                    a1_send, a1_recv, a2_send, a2_recv, a3_send, a3_recv, b1_send, b1_recv, b2_send, b2_recv, b3_send, b3_recv):
    n_pos, seqs, depth, vocab, n_loc, na, nb = dims
    n_draft = n_pos - 1
    n_early = n_draft - 1
    n_peers = na * nb
    n_tiles = vocab // NT
    others = range(n_peers - 1)
    dp, za, tb = lax.axis_index("dp"), lax.axis_index("tpa"), lax.axis_index("tpb")
    me = za * nb + tb

    inner = (za == 1) | (za == 2)

    def choose(end, mid):
        return [(jnp.where(inner, m[0], e[0]), lax.rem(tb + jnp.where(inner, m[1], e[1]), nb)) for e, m in zip(end, mid)]

    own = [(za, k) for k in range(1, nb)]
    steps = [[(pick(za, SEND[step]), CORE_OFFSETS[k]) for k in range(nb)] for step in range(3)]
    first_order = choose(steps[0] + steps[1] + steps[2] + own, steps[2][:1] + own + steps[0] + steps[1] + steps[2][1:])
    last_order = choose(steps[1] + own + steps[2] + steps[0], own + steps[1] + steps[0] + steps[2])

    def recv_peer(k):
        step, off = (k - 3) // nb, lax.rem(jnp.int32(k) + 1, nb)
        plane = jnp.where(k < 3, za, jnp.where(step == 0, pick(za, LAST_RECV[0]),
                          jnp.where(step == 1, pick(za, LAST_RECV[1]), na - 1 - za)))
        off = jnp.where(k < 3, k + 1, nb - pick(off, CORE_OFFSETS))
        return plane, lax.rem(tb + off, nb)

    def rows_of(group):
        return pl.ds(pl.multiple_of(group * n_loc, 8), n_loc)

    def q_copy(part, plane, core, own_group, column, send=q_send):
        i0, ni = (0, n_early) if part == 0 else (n_early, 1)
        recv = q_recv.at[own_group // nb] if part == 0 else r_recv.at[own_group]
        return pltpu.make_async_remote_copy(
            src_ref=q_ref.at[pl.ds(i0, ni), :, pl.ds(pl.multiple_of(column * vocab, 128), vocab)],
            dst_ref=ex_ref.at[pl.ds(i0, ni), rows_of(own_group), :],
            send_sem=send, recv_sem=recv,
            device_id=(dp, plane, core), device_id_type=MESH)

    def q_to(part, k):
        plane, core = (first_order, last_order)[part][k]
        return q_copy(part, plane, core, me, plane * nb + core, r_send if (part, k) >= (1, 11) else q_send)

    def q_from_plane(plane, count):
        rows = ex_ref.at[pl.ds(0, n_early), pl.ds(0, count * n_loc), :]
        pltpu.make_async_copy(rows, rows, q_recv.at[plane]).wait()

    def q_from(group):
        return q_copy(1, za, tb, group, 0)

    def small(src, dst, send, recv, src_slot, dst_slot, plane, core):
        return pltpu.make_async_remote_copy(
            src_ref=src.at[src_slot], dst_ref=dst.at[dst_slot], send_sem=send, recv_sem=recv,
            device_id=(dp, plane, core), device_id_type=MESH)

    def await_slots(ref, sem, count):
        part = ref.at[pl.ds(0, count)]
        pltpu.make_async_copy(part, part, sem).wait()

    def in_plane(src, dst, send, recv, scatter):
        cores = [lax.rem(tb + k, nb) for k in range(1, nb)]
        return [small(src, dst, send, recv, core if scatter else tb, tb, za, core) for core in cores]

    def across(ref, send, recv):
        planes = [lax.rem(za + k, na) for k in range(1, na)]
        return [small(ref, ref, send, recv, za, za, plane, tb) for plane in planes]

    def start(copies):
        for copy in copies:
            copy.start()

    def combine(ref):
        top = ref[0, 0:4]
        for k in range(1, 4):
            top = jnp.maximum(top, ref[k, 0:4])
        total = ref[0, 4:8] * jnp.exp(ref[0, 0:4] - top)
        for k in range(1, 4):
            total += ref[k, 4:8] * jnp.exp(ref[k, 0:4] - top)
        return top, total

    def add(ref):
        return (ref[0] + ref[1]) + (ref[2] + ref[3])

    def put(tile, plane, first, second):
        row = lax.broadcasted_iota(jnp.int32, tile.shape, 0)
        return jnp.where(row == plane, first, jnp.where(row == na + plane, second, tile))

    def w_copy(tile, slot):
        return pltpu.make_async_copy(w_ref.at[:, pl.ds(pl.multiple_of(tile * NT, NT), NT)], w_v.at[slot], w_sem.at[slot])

    hid_copy = pltpu.make_async_copy(hid_ref, hid_v, hid_sem)
    part_copies = [pltpu.make_async_copy(
        q_ref.at[n_early, :, pl.ds(pl.multiple_of(((na - 1 - za) * nb + core) * vocab, 128), vocab)],
        part_q_ref.at[pl.ds(core * n_loc, n_loc), :], part_sem.at[core]) for core in range(nb)]
    x_copy = pltpu.make_async_copy(x_ref, x_v, x_sem)
    own_copy = pltpu.make_async_copy(
        q_ref.at[:, :, pl.ds(pl.multiple_of(me * vocab, 128), vocab)], ex_ref.at[:, rows_of(me), :], own_sem)

    def signal(sem, peers):
        for plane, core in peers:
            pl.semaphore_signal(sem, inc=1, device_id=(dp, plane, core), device_id_type=MESH)

    partner = na - 1 - za
    own_plane = [(za, lax.rem(tb + k, nb)) for k in range(1, nb)]
    partner_plane = [(partner, lax.rem(tb + k, nb)) for k in range(nb)]
    other_planes = [(plane, lax.rem(tb + k, nb)) for plane in (jnp.where(inner, 0, 1), jnp.where(inner, 3, 2)) for k in range(nb)]

    barrier = pltpu.get_barrier_semaphore()

    @pl.when(inner)
    def _():
        signal(barrier, [(partner, tb)] + other_planes)

    @pl.when(jnp.logical_not(inner))
    def _():
        signal(barrier, partner_plane + own_plane)

    pl.semaphore_wait(barrier, jnp.where(inner, 1, n_peers - 1))
    q_to(0, 0).start()

    @pl.when(jnp.logical_not(inner))
    def _():
        for k in range(1, 4):
            q_to(0, k).start()
        signal(ready, other_planes)

    x_copy.start()
    for copy in part_copies:
        copy.start()
    hid_copy.start()
    w_copy(0, 0).start()
    own_copy.start()

    @pl.when(inner)
    def _():
        pl.semaphore_wait(ready, 2 * nb)
        for k in range(1, 4):
            q_to(0, k).start()

    hid_copy.wait()
    for copy in part_copies:
        copy.wait()

    @pl.loop(0, n_tiles)
    def _(tile):
        slot = lax.rem(tile, 2)
        w_copy(tile, slot).wait()

        @pl.when(tile + 1 < n_tiles)
        def _():
            w_copy(tile + 1, 1 - slot).start()

        @pl.loop(0, n_pos)
        def _(i):
            z_v[i, :, pl.ds(pl.multiple_of(tile * NT, NT), NT)] = INV_TEMP * jnp.dot(
                hid_v[i], w_v[slot], preferred_element_type=F32)

    @pl.loop(0, nb)
    def _(core):
        def plane_rows(plane, tile):
            def one(i, rows):
                z = z_v[i, rows_of(plane * nb + core), :]
                m = jnp.max(z, axis=1, keepdims=True)
                s = jnp.sum(jnp.exp(z - m), axis=1, keepdims=True)
                return rows[0] + spread(m, 128, i * n_loc), rows[1] + spread(s, 128, i * n_loc)

            zero = jnp.zeros((1, 128), F32)
            return put(tile, plane, *lax.fori_loop(0, n_pos, one, (zero, zero)))

        stat_out[core] = lax.fori_loop(0, na, plane_rows, jnp.zeros((8, 128), F32))

    stat_1[tb] = stat_out[tb]

    x_copy.wait()
    tok_rows = x_v[...].astype(F32)

    def token_columns(positions):
        for i in positions:
            tok_v[i] = jnp.broadcast_to(to_col(tok_rows[i:i + 1]), (seqs, 128)).astype(jnp.int32) - me * vocab

    token_columns(range(2))
    start(in_plane(stat_out, stat_1, a1_send, a1_recv, True))
    await_slots(stat_1, a1_recv, 3)
    stat_2[za] = jnp.concatenate(combine(stat_1), axis=0)
    token_columns(range(2, 4))
    start(across(stat_2, a2_send, a2_recv))
    for k in (4,):
        q_to(0, k).start()
    await_slots(stat_2, a2_recv, 3)
    top, total = combine(stat_2)
    used = lax.broadcasted_iota(jnp.int32, (4, 128), 1) < n_pos * n_loc
    norm_v[tb] = jnp.concatenate([top, 1.0 / jnp.where(used, total, 1.0)], axis=0)
    token_columns(range(4, n_draft))
    start(in_plane(norm_v, norm_v, a3_send, a3_recv, False))
    for k in range(5, 15):
        q_to(0, k).start()
    for k in range(10):
        q_to(1, k).start()

    @pl.when(jnp.logical_not(inner))
    def _():
        q_to(1, 10).start()

    await_slots(norm_v, a3_recv, 3)

    def probs(i, group):
        norm, plane = norm_v[lax.rem(group, nb)], group // nb
        m = gather(get_row(norm, plane), i * n_loc, n_loc)
        r = gather(get_row(norm, na + plane), i * n_loc, n_loc)
        return jnp.exp(z_v[i, rows_of(group), :] - m) * r

    @pl.loop(0, n_peers)
    def _(group):
        bonus_ref[rows_of(group), :] = probs(n_draft, group)

    def cell(i, group):
        rows = rows_of(group)
        p, q, tok = probs(i, group), ex_ref[i, rows, :], tok_v[i, rows, 0:1]
        hit = lax.broadcasted_iota(jnp.int32, (n_loc, vocab), 1) == tok
        p_pick = jnp.sum(jnp.where(hit, p, 0.0), axis=1, keepdims=True)
        q_pick = jnp.sum(jnp.where(hit, q, 0.0), axis=1, keepdims=True)
        excess = jnp.maximum(p - q, 0.0)
        ex_ref[i, rows, :] = excess
        owned = (tok >= 0) & (tok < vocab)
        accept = jnp.where(owned, jnp.minimum(1.0, p_pick / jnp.where(owned, q_pick, 1.0)), 0.0)
        return jnp.sum(excess, axis=1, keepdims=True), accept

    def absorb_early(group):
        def one(i, rows):
            z, a = cell(i, group)
            return rows[0] + spread(z, 128, i * n_loc), rows[1] + spread(a, 128, i * n_loc)

        zero = jnp.zeros((1, 128), F32)
        z_row, a_row = lax.fori_loop(0, n_early, one, (zero, zero))
        core = lax.rem(group, nb)
        sum_out[core] = put(sum_out[core], group // nb, z_row, a_row)

    sum_out[...] = jnp.zeros_like(sum_out)
    own_copy.wait()
    absorb_early(me)

    q_from_plane(za, nb - 1)
    for k in range(1, nb):
        absorb_early(za * nb + lax.rem(tb + k, nb))

    @pl.loop(0, na - 1)
    def _(step):
        plane = jnp.where(step == 0, pick(za, RECV[0]), jnp.where(step == 1, pick(za, RECV[1]), pick(za, RECV[2])))
        q_from_plane(plane, nb)

        @pl.loop(0, nb)
        def _(core):
            absorb_early(plane * nb + core)

    sum_1[tb] = sum_out[tb]
    start(in_plane(sum_out, sum_1, b1_send, b1_recv, True))
    await_slots(sum_1, b1_recv, 3)
    sum_2[za] = add(sum_1)
    start(across(sum_2, b2_send, b2_recv))

    head = pltpu.make_async_remote_copy(
        src_ref=q_ref.at[n_early, pl.ds(0, n_loc // 2), pl.ds(pl.multiple_of((partner * nb + tb) * vocab, 128), vocab)],
        dst_ref=part_head_ref, send_sem=h_send, recv_sem=h_recv, device_id=(dp, partner, tb), device_id_type=MESH)

    @pl.when(inner)
    def _():
        q_to(1, 10).start()
        head.start()

    @pl.loop(0, nb)
    def _(core):
        group = partner * nb + core
        part_p_ref[pl.ds(pl.multiple_of(core * n_loc, 8), n_loc), :] = probs(n_early, group)
        part_tok_ref[pl.ds(pl.multiple_of(core * n_loc, 8), n_loc), :] = tok_v[n_early, rows_of(group), :]

    def absorb_late(group):
        z, a = cell(n_early, group)
        late_ref[...] += jnp.concatenate([spread(z, seqs, group * n_loc), spread(a, seqs, group * n_loc)], axis=0)

    def arrived(k):
        plane, core = recv_peer(k)
        q_from(plane * nb + core).wait_recv()
        absorb_late(plane * nb + core)

    late_ref[...] = jnp.zeros_like(late_ref)
    absorb_late(me)
    pl.loop(0, 10)(arrived)

    plane, core = recv_peer(10)
    q_from(plane * nb + core).wait_recv()

    @pl.when(jnp.logical_not(inner))
    def _():
        for k in range(11, 15):
            q_to(1, k).start()

    absorb_late(plane * nb + core)
    await_slots(sum_2, b2_recv, 3)
    early_ref[tb] = add(sum_2)
    start(in_plane(early_ref, early_ref, b3_send, b3_recv, False))

    @pl.when(inner)
    def _():
        head.wait()

    @pl.when(jnp.logical_not(inner))
    def _():
        pl.loop(11, 15)(arrived)
        sent = q_ref.at[0:4, :, pl.ds(0, vocab)]
        pltpu.make_async_copy(sent, sent, r_send).wait()

    await_slots(early_ref, b3_recv, 3)
    slices = (n_peers - 1) * n_early + 11
    sent = q_ref.at[:, :, pl.ds(0, slices * vocab // n_draft)]
    pltpu.make_async_copy(sent, sent, q_send).wait()
    for ref, sem in ((stat_1, a1_send), (stat_2, a2_send), (norm_v, a3_send), (sum_1, b1_send), (sum_2, b2_send),
                     (early_ref, b3_send)):
        await_slots(ref, sem, 3)


def last_kernel(dims, q_ref, head_ref, p_ref, tok_ref, part_ref, order_ref, ex_ref, late_ref, own_v, ready, q_send, q_recv, l_send, l_recv):
    n_draft, seqs, vocab, n_loc, na, nb = dims
    n_peers = na * nb
    dp, za, tb = lax.axis_index("dp"), lax.axis_index("tpa"), lax.axis_index("tpb")
    me, partner = za * nb + tb, na - 1 - za
    inner = (za == 1) | (za == 2)
    same = [(za, lax.rem(tb + k, nb)) for k in range(1, nb)] + [(partner, lax.rem(tb + k, nb)) for k in range(nb)]
    other_planes = (jnp.where(inner, 0, 1), jnp.where(inner, 3, 2))
    other = [(plane, lax.rem(tb + k, nb)) for plane in other_planes for k in range(nb)]

    def signal(sem, peers):
        for plane, core in peers:
            pl.semaphore_signal(sem, inc=1, device_id=(dp, plane, core), device_id_type=MESH)

    barrier = pltpu.get_barrier_semaphore()
    signal(barrier, same)

    @pl.when(inner)
    def _():
        signal(barrier, other)

    pl.semaphore_wait(barrier, jnp.where(inner, 2 * nb - 1, n_peers - 1))

    @pl.when(jnp.logical_not(inner))
    def _():
        signal(ready, other)

    def q_copy(core, own_core, first):
        return pltpu.make_async_remote_copy(
            src_ref=q_ref.at[pl.ds(pl.multiple_of(core * n_loc + first, 8), n_loc - first), :],
            dst_ref=ex_ref.at[pl.ds(pl.multiple_of(own_core * n_loc + first, 8), n_loc - first), :],
            send_sem=q_send, recv_sem=q_recv.at[own_core], device_id=(dp, partner, core), device_id_type=MESH)

    def late_to(peer):
        plane, core = peer
        return pltpu.make_async_remote_copy(
            src_ref=late_ref.at[me], dst_ref=late_ref.at[me], send_sem=l_send, recv_sem=l_recv,
            device_id=(dp, plane, core), device_id_type=MESH)

    own_v[...] = part_ref[...]

    @pl.when(inner)
    def _():
        for k in CORE_OFFSETS:
            q_copy(lax.rem(tb + k, nb), tb, 0 if k else n_loc // 2).start()

        ex_ref[pl.ds(pl.multiple_of(tb * n_loc, 8), n_loc // 2), :] = head_ref[...]
        q_copy(tb, tb, n_loc // 2).wait_recv()

        @pl.loop(0, nb)
        def _(k):
            core = lax.rem(tb + nb - pick(k, CORE_OFFSETS), nb)
            rows = pl.ds(pl.multiple_of(core * n_loc, 8), n_loc)

            @pl.when(k > 0)
            def _():
                q_copy(core, core, 0).wait_recv()

            p, q, tok = p_ref[rows, :], ex_ref[rows, :], tok_ref[rows, 0:1]
            hit = lax.broadcasted_iota(jnp.int32, (n_loc, vocab), 1) == tok
            excess = jnp.maximum(p - q, 0.0)
            ex_ref[rows, :] = excess
            z = jnp.sum(excess, axis=1, keepdims=True)
            p_pick = jnp.sum(jnp.where(hit, p, 0.0), axis=1, keepdims=True)
            q_pick = jnp.sum(jnp.where(hit, q, 0.0), axis=1, keepdims=True)
            owned = (tok >= 0) & (tok < vocab)
            a = jnp.where(owned, jnp.minimum(1.0, p_pick / jnp.where(owned, q_pick, 1.0)), 0.0)
            first = (partner * nb + core) * n_loc
            own_v[...] += jnp.concatenate([spread(z, seqs, first), spread(a, seqs, first)], axis=0)

    late_ref[me] = own_v[...]

    @pl.when(inner)
    def _():
        sent = q_ref.at[pl.ds(0, nb * n_loc - n_loc // 2), :]
        pltpu.make_async_copy(sent, sent, q_send).wait()
        pl.semaphore_wait(ready, 2 * nb)

    for peer in other + same:
        late_to(peer).start()
    slots = late_ref.at[pl.ds(0, n_peers - 1)]
    pltpu.make_async_copy(slots, slots, l_recv).wait()
    pltpu.make_async_copy(slots, slots, l_send).wait()


SLOTS = 4


def by_position(na, nb, early_ref, which, n_early, seqs):
    n_peers = na * nb
    n_loc = seqs // n_peers
    lane = lax.broadcasted_iota(jnp.int32, (n_peers, 128), 1)
    mine = (lax.broadcasted_iota(jnp.int32, (n_peers, seqs), 1) // n_loc
            == lax.broadcasted_iota(jnp.int32, (n_peers, seqs), 0))
    table = jnp.concatenate(
        [early_ref[g % nb, na * which + g // nb:na * which + g // nb + 1, :] for g in range(n_peers)], axis=0)
    out = jnp.ones((8, seqs), F32)
    for i in range(n_early):
        x = pltpu.roll(table, (128 - n_loc * i) % 128, 1)
        x = jnp.where(lane < n_loc, x, 0.0)
        shift = n_loc
        while shift < 128:
            x = x + pltpu.roll(x, shift, 1)
            shift *= 2
        x = jnp.concatenate([x] * (seqs // 128), axis=1)
        row = jnp.sum(jnp.where(mine, x, 0.0), axis=0, keepdims=True)
        out = jnp.where(lax.broadcasted_iota(jnp.int32, (8, seqs), 0) == i, row, out)
    return out


def early_output_kernel(na, nb, ex_ref, bonus_ref, early_ref, res_ref, bonus_out, order_ref, stage, stage_sem, bonus_sem):
    n_draft, seqs, vocab = ex_ref.shape
    n_early, half = n_draft - 1, seqs // 2
    bonus_copy = pltpu.make_async_copy(bonus_ref, bonus_out, bonus_sem)
    bonus_copy.start()
    order_ref[...] = jnp.zeros_like(order_ref)
    inv = 1.0 / by_position(na, nb, early_ref, 0, n_early, seqs)

    def out_copy(k, slot):
        i, h = k // 2, lax.rem(k, 2)
        return pltpu.make_async_copy(
            stage.at[slot], res_ref.at[i, pl.ds(pl.multiple_of(h * half, half), half), :], stage_sem.at[slot])

    @pl.loop(0, 2 * n_early)
    def _(k):
        i, h, slot = k // 2, lax.rem(k, 2), lax.rem(k, SLOTS)
        row = get_row(inv, i)
        col = to_col(jnp.where(h == 0, row[:, :half], row[:, half:]))

        @pl.when(k >= SLOTS)
        def _():
            out_copy(k - SLOTS, slot).wait()

        @pl.loop(0, vocab // NT)
        def _(t):
            cols = pl.ds(pl.multiple_of(t * NT, NT), NT)
            stage[slot, :, cols] = ex_ref[i, pl.ds(pl.multiple_of(h * half, half), half), cols] * col

        out_copy(k, slot).start()

    for k in range(2 * n_early - SLOTS, 2 * n_early):
        out_copy(k, k % SLOTS).wait()
    bonus_copy.wait()


def late_output_kernel(na, nb, ex_ref, part_ref, early_ref, late_ref, res_in, res_ref, accept_ref, expected_ref,
                       stage, accept_v, expected_v, stage_sem, small_sem):
    n_draft, seqs, vocab = ex_ref.shape
    n_early, block = n_draft - 1, seqs // na
    za = lax.axis_index("tpa")
    inner, partner = (za == 1) | (za == 2), na - 1 - za
    late = late_ref[0]
    for k in range(1, na * nb):
        late += late_ref[k]
    col = to_col(1.0 / late[0:1])

    def out_copy(plane):
        rows = pl.ds(plane * block, block)
        return pltpu.make_async_copy(stage.at[rows], res_ref.at[n_early, rows, :], stage_sem.at[plane])

    for plane in range(na):
        rows, scale = pl.ds(plane * block, block), col[plane * block:(plane + 1) * block]
        from_part = inner & (partner == plane)

        @pl.when(from_part)
        def _():
            @pl.loop(0, vocab // NT)
            def _(t):
                cols = pl.ds(pl.multiple_of(t * NT, NT), NT)
                stage[rows, cols] = part_ref[:, cols] * scale

        @pl.when(jnp.logical_not(from_part))
        def _():
            @pl.loop(0, vocab // NT)
            def _(t):
                cols = pl.ds(pl.multiple_of(t * NT, NT), NT)
                stage[rows, cols] = ex_ref[n_early, rows, cols] * scale

        out_copy(plane).start()

    accept = by_position(na, nb, early_ref, 1, n_early, seqs)
    accept = jnp.where(lax.broadcasted_iota(jnp.int32, accept.shape, 0) == n_early, late[1:2], accept)[:n_draft]
    accept_v[...] = accept
    prod = accept[0:1]
    expected = prod
    for i in range(1, n_draft):
        prod = prod * accept[i:i + 1]
        expected += prod
    expected_v[...] = expected
    small_copies = (pltpu.make_async_copy(accept_v, accept_ref, small_sem.at[0]),
                    pltpu.make_async_copy(expected_v, expected_ref, small_sem.at[1]))
    for copy in small_copies:
        copy.start()
    for plane in range(na):
        out_copy(plane).wait()
    for copy in small_copies:
        copy.wait()


def solution(mesh):
    na, nb = mesh.shape["tpa"], mesh.shape["tpb"]
    n_peers = na * nb
    any_spec = pl.BlockSpec(memory_space=pl.ANY)
    vmem_spec = pl.BlockSpec(memory_space=pltpu.VMEM)

    def local_step(hidden, w_head, q_draft, x_draft):
        seqs, n_pos, depth = hidden.shape
        vocab = w_head.shape[1]
        n_loc, n_draft, _ = q_draft.shape
        dims = (n_pos, seqs, depth, vocab, n_loc, na, nb)
        dma = pltpu.SemaphoreType.DMA
        small = pltpu.VMEM((4, 8, 128), F32)
        q_rows = q_draft.transpose(1, 0, 2)
        block = seqs // na
        ex, bonus, early, late_part, part_p, part_q, part_head, part_tok = pl.pallas_call(
            functools.partial(exchange_kernel, dims),
            out_shape=(pltpu.VMEM((n_draft, seqs, vocab), F32), pltpu.VMEM((seqs, vocab), F32), small,
                       pltpu.VMEM((2, seqs), F32), pltpu.VMEM((block, vocab), F32), pltpu.VMEM((block, vocab), F32),
                       pltpu.VMEM((n_loc // 2, vocab), F32), pltpu.VMEM((block, 128), jnp.int32)),
            in_specs=[any_spec] * 4,
            out_specs=(vmem_spec,) * 8,
            scratch_shapes=[
                pltpu.VMEM((n_pos, seqs, depth), jnp.bfloat16),
                pltpu.VMEM((2, depth, NT), jnp.bfloat16),
                pltpu.VMEM((n_pos, seqs, vocab), F32),
                pltpu.VMEM((n_draft, seqs), jnp.int32),
                pltpu.VMEM((n_draft, seqs, 128), jnp.int32),
                small, small, small, small, small, small, small,
                dma, dma((2,)), dma, dma, dma((nb,)), pltpu.SemaphoreType.REGULAR, dma, dma((na,)), dma, dma((n_peers,)),
            ] + [dma] * 14,
            compiler_params=pltpu.CompilerParams(collective_id=0, has_side_effects=True, vmem_limit_bytes=38 * 2**20),
            name="exchange",
        )(hidden.transpose(1, 0, 2), w_head, q_rows, x_draft.T)
        res, bonus_out, order = pl.pallas_call(
            functools.partial(early_output_kernel, na, nb),
            out_shape=(jax.ShapeDtypeStruct((n_draft, seqs, vocab), F32), jax.ShapeDtypeStruct((seqs, vocab), F32),
                       pltpu.VMEM((8, 128), F32)),
            in_specs=[vmem_spec] * 3,
            out_specs=(any_spec, any_spec, vmem_spec),
            scratch_shapes=[pltpu.VMEM((SLOTS, seqs // 2, vocab), F32), dma((SLOTS,)), dma],
            compiler_params=pltpu.CompilerParams(vmem_limit_bytes=12 * 2**20),
            name="early_output",
        )(ex, bonus, early)
        part, late = pl.pallas_call(
            functools.partial(last_kernel, (n_draft, seqs, vocab, n_loc, na, nb)),
            out_shape=(pltpu.VMEM((block, vocab), F32), pltpu.VMEM((n_peers, 2, seqs), F32)),
            in_specs=[vmem_spec] * 6,
            out_specs=(vmem_spec, vmem_spec),
            scratch_shapes=[pltpu.VMEM((2, seqs), F32), pltpu.SemaphoreType.REGULAR, dma, dma((nb,)), dma, dma],
            compiler_params=pltpu.CompilerParams(collective_id=1, has_side_effects=True, vmem_limit_bytes=28 * 2**20),
            name="last",
        )(part_q, part_head, part_p, part_tok, late_part, order)
        res, accept, expected = pl.pallas_call(
            functools.partial(late_output_kernel, na, nb),
            out_shape=(jax.ShapeDtypeStruct((n_draft, seqs, vocab), F32), jax.ShapeDtypeStruct((n_draft, seqs), F32),
                       jax.ShapeDtypeStruct((1, seqs), F32)),
            in_specs=[vmem_spec] * 4 + [any_spec],
            out_specs=(any_spec,) * 3,
            scratch_shapes=[pltpu.VMEM((seqs, vocab), F32), pltpu.VMEM((n_draft, seqs), F32), pltpu.VMEM((1, seqs), F32),
                            dma((na,)), dma((2,))],
            input_output_aliases={4: 0},
            compiler_params=pltpu.CompilerParams(vmem_limit_bytes=12 * 2**20),
            name="late_output",
        )(ex, part, early, late, res)
        return accept.T, expected.reshape(seqs), res.transpose(1, 0, 2), bonus_out

    return jax.shard_map(
        local_step, mesh=mesh,
        in_specs=(P("dp", None, None), P(None, VOCAB_AXES), P(("dp",) + VOCAB_AXES, None, None), P("dp", None)),
        out_specs=(P("dp", None), P("dp"), P("dp", None, VOCAB_AXES), P("dp", VOCAB_AXES)),
        check_vma=False)
```

```python
import functools

import jax
import jax.numpy as jnp
from jax import lax
from jax.experimental import pallas as pl
from jax.experimental.pallas import tpu as pltpu
from jax.sharding import PartitionSpec as P

INV_TEMP = 1.25
VOCAB_AXES = ("tpa", "tpb")
MESH = pl.DeviceIdType.MESH
F32 = jnp.float32
SEND = ((3, 3, 0, 0), (1, 0, 3, 2), (2, 2, 1, 1))
RECV = ((3, 0, 3, 0), (2, 3, 0, 1), (1, 2, 1, 2))
LAST_RECV = ((1, 0, 3, 2), (2, 3, 0, 1))
CORE_OFFSETS = (0, 2, 1, 3)
NT = 512


def pick(index, values):
    out = jnp.int32(values[-1])
    for k in range(len(values) - 2, -1, -1):
        out = jnp.where(index == k, jnp.int32(values[k]), out)
    return out


def diag(n):
    return lax.broadcasted_iota(jnp.int32, (n, n), 0) == lax.broadcasted_iota(jnp.int32, (n, n), 1)


def to_col(row):
    return jnp.sum(jnp.where(diag(row.shape[1]), row, 0.0), axis=1, keepdims=True)


def get_row(rows, i):
    return jnp.sum(jnp.where(lax.broadcasted_iota(jnp.int32, rows.shape, 0) == i, rows, 0.0), axis=0, keepdims=True)


def lanes(n, first, rows):
    return (lax.broadcasted_iota(jnp.int32, (rows, n), 1)
            == lax.broadcasted_iota(jnp.int32, (rows, n), 0) + first)


def spread(col, n, first):
    return jnp.sum(jnp.where(lanes(n, first, col.shape[0]), col, 0.0), axis=0, keepdims=True)


def gather(row, first, rows):
    return jnp.sum(jnp.where(lanes(row.shape[1], first, rows), row, 0.0), axis=1, keepdims=True)


def exchange_kernel(dims, hid_ref, w_ref, q_ref, x_ref, ex_ref, bonus_ref, early_ref, late_ref, part_p_ref, part_q_ref, part_head_ref, part_tok_ref,
                    hid_v, w_v, z_v, x_v, tok_v, stat_out, stat_1, stat_2, norm_v, sum_out, sum_1, sum_2, hid_sem, w_sem, own_sem, x_sem, part_sem,
                    ready, q_send, q_recv, r_send, r_recv, h_send, h_recv,
                    a1_send, a1_recv, a2_send, a2_recv, a3_send, a3_recv, b1_send, b1_recv, b2_send, b2_recv, b3_send, b3_recv):
    n_pos, seqs, depth, vocab, n_loc, na, nb = dims
    n_draft = n_pos - 1
    n_early = n_draft - 1
    n_peers = na * nb
    n_tiles = vocab // NT
    others = range(n_peers - 1)
    dp, za, tb = lax.axis_index("dp"), lax.axis_index("tpa"), lax.axis_index("tpb")
    me = za * nb + tb

    inner = (za == 1) | (za == 2)

    def choose(end, mid):
        return [(jnp.where(inner, m[0], e[0]), lax.rem(tb + jnp.where(inner, m[1], e[1]), nb)) for e, m in zip(end, mid)]

    own = [(za, k) for k in range(1, nb)]
    steps = [[(pick(za, SEND[step]), CORE_OFFSETS[k]) for k in range(nb)] for step in range(3)]
    first_order = choose(steps[0] + steps[1] + steps[2] + own, steps[2][:1] + own + steps[0] + steps[1] + steps[2][1:])
    last_order = choose(steps[1] + own + steps[2] + steps[0], own + steps[1] + steps[0] + steps[2])

    def recv_peer(k):
        step, off = (k - 3) // nb, lax.rem(jnp.int32(k) + 1, nb)
        plane = jnp.where(k < 3, za, jnp.where(step == 0, pick(za, LAST_RECV[0]),
                          jnp.where(step == 1, pick(za, LAST_RECV[1]), na - 1 - za)))
        off = jnp.where(k < 3, k + 1, nb - pick(off, CORE_OFFSETS))
        return plane, lax.rem(tb + off, nb)

    def rows_of(group):
        return pl.ds(pl.multiple_of(group * n_loc, 8), n_loc)

    def q_copy(part, plane, core, own_group, column, send=q_send):
        i0, ni = (0, n_early) if part == 0 else (n_early, 1)
        recv = q_recv.at[own_group // nb] if part == 0 else r_recv.at[own_group]
        return pltpu.make_async_remote_copy(
            src_ref=q_ref.at[pl.ds(i0, ni), :, pl.ds(pl.multiple_of(column * vocab, 128), vocab)],
            dst_ref=ex_ref.at[pl.ds(i0, ni), rows_of(own_group), :],
            send_sem=send, recv_sem=recv,
            device_id=(dp, plane, core), device_id_type=MESH)

    def q_to(part, k):
        plane, core = (first_order, last_order)[part][k]
        return q_copy(part, plane, core, me, plane * nb + core, r_send if (part, k) >= (1, 11) else q_send)

    def q_from_plane(plane, count):
        rows = ex_ref.at[pl.ds(0, n_early), pl.ds(0, count * n_loc), :]
        pltpu.make_async_copy(rows, rows, q_recv.at[plane]).wait()

    def q_from(group):
        return q_copy(1, za, tb, group, 0)

    def small(src, dst, send, recv, src_slot, dst_slot, plane, core):
        return pltpu.make_async_remote_copy(
            src_ref=src.at[src_slot], dst_ref=dst.at[dst_slot], send_sem=send, recv_sem=recv,
            device_id=(dp, plane, core), device_id_type=MESH)

    def await_slots(ref, sem, count):
        part = ref.at[pl.ds(0, count)]
        pltpu.make_async_copy(part, part, sem).wait()

    def in_plane(src, dst, send, recv, scatter):
        cores = [lax.rem(tb + k, nb) for k in range(1, nb)]
        return [small(src, dst, send, recv, core if scatter else tb, tb, za, core) for core in cores]

    def across(ref, send, recv):
        planes = [lax.rem(za + k, na) for k in range(1, na)]
        return [small(ref, ref, send, recv, za, za, plane, tb) for plane in planes]

    def start(copies):
        for copy in copies:
            copy.start()

    def combine(ref):
        top = ref[0, 0:4]
        for k in range(1, 4):
            top = jnp.maximum(top, ref[k, 0:4])
        total = ref[0, 4:8] * jnp.exp(ref[0, 0:4] - top)
        for k in range(1, 4):
            total += ref[k, 4:8] * jnp.exp(ref[k, 0:4] - top)
        return top, total

    def add(ref):
        return (ref[0] + ref[1]) + (ref[2] + ref[3])

    def put(tile, plane, first, second):
        row = lax.broadcasted_iota(jnp.int32, tile.shape, 0)
        return jnp.where(row == plane, first, jnp.where(row == na + plane, second, tile))

    def w_copy(tile, slot):
        return pltpu.make_async_copy(w_ref.at[:, pl.ds(pl.multiple_of(tile * NT, NT), NT)], w_v.at[slot], w_sem.at[slot])

    hid_copy = pltpu.make_async_copy(hid_ref, hid_v, hid_sem)
    part_copies = [pltpu.make_async_copy(
        q_ref.at[n_early, :, pl.ds(pl.multiple_of(((na - 1 - za) * nb + core) * vocab, 128), vocab)],
        part_q_ref.at[pl.ds(core * n_loc, n_loc), :], part_sem.at[core]) for core in range(nb)]
    x_copy = pltpu.make_async_copy(x_ref, x_v, x_sem)
    own_copy = pltpu.make_async_copy(
        q_ref.at[:, :, pl.ds(pl.multiple_of(me * vocab, 128), vocab)], ex_ref.at[:, rows_of(me), :], own_sem)

    def signal(sem, peers):
        for plane, core in peers:
            pl.semaphore_signal(sem, inc=1, device_id=(dp, plane, core), device_id_type=MESH)

    partner = na - 1 - za
    own_plane = [(za, lax.rem(tb + k, nb)) for k in range(1, nb)]
    partner_plane = [(partner, lax.rem(tb + k, nb)) for k in range(nb)]
    other_planes = [(plane, lax.rem(tb + k, nb)) for plane in (jnp.where(inner, 0, 1), jnp.where(inner, 3, 2)) for k in range(nb)]

    barrier = pltpu.get_barrier_semaphore()

    @pl.when(inner)
    def _():
        signal(barrier, [(partner, tb)] + other_planes)

    @pl.when(jnp.logical_not(inner))
    def _():
        signal(barrier, partner_plane + own_plane)

    pl.semaphore_wait(barrier, jnp.where(inner, 1, n_peers - 1))
    q_to(0, 0).start()

    @pl.when(jnp.logical_not(inner))
    def _():
        for k in range(1, 4):
            q_to(0, k).start()
        signal(ready, other_planes)

    x_copy.start()
    for copy in part_copies:
        copy.start()
    hid_copy.start()
    w_copy(0, 0).start()
    own_copy.start()

    @pl.when(inner)
    def _():
        pl.semaphore_wait(ready, 2 * nb)
        for k in range(1, 4):
            q_to(0, k).start()

    hid_copy.wait()
    for copy in part_copies:
        copy.wait()

    @pl.loop(0, n_tiles)
    def _(tile):
        slot = lax.rem(tile, 2)
        w_copy(tile, slot).wait()

        @pl.when(tile + 1 < n_tiles)
        def _():
            w_copy(tile + 1, 1 - slot).start()

        @pl.loop(0, n_pos)
        def _(i):
            z_v[i, :, pl.ds(pl.multiple_of(tile * NT, NT), NT)] = INV_TEMP * jnp.dot(
                hid_v[i], w_v[slot], preferred_element_type=F32)

    @pl.loop(0, nb)
    def _(core):
        def plane_rows(plane, tile):
            def one(i, rows):
                z = z_v[i, rows_of(plane * nb + core), :]
                m = jnp.max(z, axis=1, keepdims=True)
                s = jnp.sum(jnp.exp(z - m), axis=1, keepdims=True)
                return rows[0] + spread(m, 128, i * n_loc), rows[1] + spread(s, 128, i * n_loc)

            zero = jnp.zeros((1, 128), F32)
            return put(tile, plane, *lax.fori_loop(0, n_pos, one, (zero, zero)))

        stat_out[core] = lax.fori_loop(0, na, plane_rows, jnp.zeros((8, 128), F32))

    stat_1[tb] = stat_out[tb]

    x_copy.wait()
    tok_rows = x_v[...].astype(F32)

    def token_columns(positions):
        for i in positions:
            tok_v[i] = jnp.broadcast_to(to_col(tok_rows[i:i + 1]), (seqs, 128)).astype(jnp.int32) - me * vocab

    token_columns(range(2))
    start(in_plane(stat_out, stat_1, a1_send, a1_recv, True))
    await_slots(stat_1, a1_recv, 3)
    stat_2[za] = jnp.concatenate(combine(stat_1), axis=0)
    token_columns(range(2, 4))
    start(across(stat_2, a2_send, a2_recv))
    for k in (4,):
        q_to(0, k).start()
    await_slots(stat_2, a2_recv, 3)
    top, total = combine(stat_2)
    used = lax.broadcasted_iota(jnp.int32, (4, 128), 1) < n_pos * n_loc
    norm_v[tb] = jnp.concatenate([top, 1.0 / jnp.where(used, total, 1.0)], axis=0)
    token_columns(range(4, n_draft))
    start(in_plane(norm_v, norm_v, a3_send, a3_recv, False))
    for k in range(5, 15):
        q_to(0, k).start()
    for k in range(10):
        q_to(1, k).start()

    @pl.when(jnp.logical_not(inner))
    def _():
        q_to(1, 10).start()

    await_slots(norm_v, a3_recv, 3)

    def probs(i, group):
        norm, plane = norm_v[lax.rem(group, nb)], group // nb
        m = gather(get_row(norm, plane), i * n_loc, n_loc)
        r = gather(get_row(norm, na + plane), i * n_loc, n_loc)
        return jnp.exp(z_v[i, rows_of(group), :] - m) * r

    @pl.loop(0, n_peers)
    def _(group):
        bonus_ref[rows_of(group), :] = probs(n_draft, group)

    def cell(i, group):
        rows = rows_of(group)
        p, q, tok = probs(i, group), ex_ref[i, rows, :], tok_v[i, rows, 0:1]
        hit = lax.broadcasted_iota(jnp.int32, (n_loc, vocab), 1) == tok
        p_pick = jnp.sum(jnp.where(hit, p, 0.0), axis=1, keepdims=True)
        q_pick = jnp.sum(jnp.where(hit, q, 0.0), axis=1, keepdims=True)
        excess = jnp.maximum(p - q, 0.0)
        ex_ref[i, rows, :] = excess
        owned = (tok >= 0) & (tok < vocab)
        accept = jnp.where(owned, jnp.minimum(1.0, p_pick / jnp.where(owned, q_pick, 1.0)), 0.0)
        return jnp.sum(excess, axis=1, keepdims=True), accept

    def absorb_early(group):
        def one(i, rows):
            z, a = cell(i, group)
            return rows[0] + spread(z, 128, i * n_loc), rows[1] + spread(a, 128, i * n_loc)

        zero = jnp.zeros((1, 128), F32)
        z_row, a_row = lax.fori_loop(0, n_early, one, (zero, zero))
        core = lax.rem(group, nb)
        sum_out[core] = put(sum_out[core], group // nb, z_row, a_row)

    sum_out[...] = jnp.zeros_like(sum_out)
    own_copy.wait()
    absorb_early(me)

    q_from_plane(za, nb - 1)
    for k in range(1, nb):
        absorb_early(za * nb + lax.rem(tb + k, nb))

    @pl.loop(0, na - 1)
    def _(step):
        plane = jnp.where(step == 0, pick(za, RECV[0]), jnp.where(step == 1, pick(za, RECV[1]), pick(za, RECV[2])))
        q_from_plane(plane, nb)

        @pl.loop(0, nb)
        def _(core):
            absorb_early(plane * nb + core)

    sum_1[tb] = sum_out[tb]
    start(in_plane(sum_out, sum_1, b1_send, b1_recv, True))
    await_slots(sum_1, b1_recv, 3)
    sum_2[za] = add(sum_1)
    start(across(sum_2, b2_send, b2_recv))

    head = pltpu.make_async_remote_copy(
        src_ref=q_ref.at[n_early, pl.ds(0, n_loc // 2), pl.ds(pl.multiple_of((partner * nb + tb) * vocab, 128), vocab)],
        dst_ref=part_head_ref, send_sem=h_send, recv_sem=h_recv, device_id=(dp, partner, tb), device_id_type=MESH)

    @pl.when(inner)
    def _():
        q_to(1, 10).start()
        head.start()

    @pl.loop(0, nb)
    def _(core):
        group = partner * nb + core
        part_p_ref[pl.ds(pl.multiple_of(core * n_loc, 8), n_loc), :] = probs(n_early, group)
        part_tok_ref[pl.ds(pl.multiple_of(core * n_loc, 8), n_loc), :] = tok_v[n_early, rows_of(group), :]

    def absorb_late(group):
        z, a = cell(n_early, group)
        late_ref[...] += jnp.concatenate([spread(z, seqs, group * n_loc), spread(a, seqs, group * n_loc)], axis=0)

    def arrived(k):
        plane, core = recv_peer(k)
        q_from(plane * nb + core).wait_recv()
        absorb_late(plane * nb + core)

    late_ref[...] = jnp.zeros_like(late_ref)
    absorb_late(me)
    pl.loop(0, 10)(arrived)

    plane, core = recv_peer(10)
    q_from(plane * nb + core).wait_recv()

    @pl.when(jnp.logical_not(inner))
    def _():
        for k in range(11, 15):
            q_to(1, k).start()

    absorb_late(plane * nb + core)
    await_slots(sum_2, b2_recv, 3)
    early_ref[tb] = add(sum_2)
    start(in_plane(early_ref, early_ref, b3_send, b3_recv, False))

    @pl.when(inner)
    def _():
        head.wait()

    @pl.when(jnp.logical_not(inner))
    def _():
        pl.loop(11, 15)(arrived)
        sent = q_ref.at[0:4, :, pl.ds(0, vocab)]
        pltpu.make_async_copy(sent, sent, r_send).wait()

    await_slots(early_ref, b3_recv, 3)
    slices = (n_peers - 1) * n_early + 11
    sent = q_ref.at[:, :, pl.ds(0, slices * vocab // n_draft)]
    pltpu.make_async_copy(sent, sent, q_send).wait()
    for ref, sem in ((stat_1, a1_send), (stat_2, a2_send), (norm_v, a3_send), (sum_1, b1_send), (sum_2, b2_send),
                     (early_ref, b3_send)):
        await_slots(ref, sem, 3)


def last_kernel(dims, q_ref, head_ref, p_ref, tok_ref, part_ref, order_ref, ex_ref, late_ref, own_v, ready, q_send, q_recv, l_send, l_recv):
    n_draft, seqs, vocab, n_loc, na, nb = dims
    n_peers = na * nb
    dp, za, tb = lax.axis_index("dp"), lax.axis_index("tpa"), lax.axis_index("tpb")
    me, partner = za * nb + tb, na - 1 - za
    inner = (za == 1) | (za == 2)
    same = [(za, lax.rem(tb + k, nb)) for k in range(1, nb)] + [(partner, lax.rem(tb + k, nb)) for k in range(nb)]
    other_planes = (jnp.where(inner, 0, 1), jnp.where(inner, 3, 2))
    other = [(plane, lax.rem(tb + k, nb)) for plane in other_planes for k in range(nb)]

    def signal(sem, peers):
        for plane, core in peers:
            pl.semaphore_signal(sem, inc=1, device_id=(dp, plane, core), device_id_type=MESH)

    barrier = pltpu.get_barrier_semaphore()
    signal(barrier, same)

    @pl.when(inner)
    def _():
        signal(barrier, other)

    pl.semaphore_wait(barrier, jnp.where(inner, 2 * nb - 1, n_peers - 1))

    @pl.when(jnp.logical_not(inner))
    def _():
        signal(ready, other)

    def q_copy(core, own_core, first):
        return pltpu.make_async_remote_copy(
            src_ref=q_ref.at[pl.ds(pl.multiple_of(core * n_loc + first, 8), n_loc - first), :],
            dst_ref=ex_ref.at[pl.ds(pl.multiple_of(own_core * n_loc + first, 8), n_loc - first), :],
            send_sem=q_send, recv_sem=q_recv.at[own_core], device_id=(dp, partner, core), device_id_type=MESH)

    def late_to(peer):
        plane, core = peer
        return pltpu.make_async_remote_copy(
            src_ref=late_ref.at[me], dst_ref=late_ref.at[me], send_sem=l_send, recv_sem=l_recv,
            device_id=(dp, plane, core), device_id_type=MESH)

    own_v[...] = part_ref[...]

    @pl.when(inner)
    def _():
        for k in CORE_OFFSETS:
            q_copy(lax.rem(tb + k, nb), tb, 0 if k else n_loc // 2).start()

        ex_ref[pl.ds(pl.multiple_of(tb * n_loc, 8), n_loc // 2), :] = head_ref[...]
        q_copy(tb, tb, n_loc // 2).wait_recv()

        @pl.loop(0, nb)
        def _(k):
            core = lax.rem(tb + nb - pick(k, CORE_OFFSETS), nb)
            rows = pl.ds(pl.multiple_of(core * n_loc, 8), n_loc)

            @pl.when(k > 0)
            def _():
                q_copy(core, core, 0).wait_recv()

            p, q, tok = p_ref[rows, :], ex_ref[rows, :], tok_ref[rows, 0:1]
            hit = lax.broadcasted_iota(jnp.int32, (n_loc, vocab), 1) == tok
            excess = jnp.maximum(p - q, 0.0)
            ex_ref[rows, :] = excess
            z = jnp.sum(excess, axis=1, keepdims=True)
            p_pick = jnp.sum(jnp.where(hit, p, 0.0), axis=1, keepdims=True)
            q_pick = jnp.sum(jnp.where(hit, q, 0.0), axis=1, keepdims=True)
            owned = (tok >= 0) & (tok < vocab)
            a = jnp.where(owned, jnp.minimum(1.0, p_pick / jnp.where(owned, q_pick, 1.0)), 0.0)
            first = (partner * nb + core) * n_loc
            own_v[...] += jnp.concatenate([spread(z, seqs, first), spread(a, seqs, first)], axis=0)

    late_ref[me] = own_v[...]

    @pl.when(inner)
    def _():
        pl.semaphore_wait(ready, 2 * nb)

    for peer in other + same:
        late_to(peer).start()

    @pl.when(inner)
    def _():
        sent = q_ref.at[pl.ds(0, nb * n_loc - n_loc // 2), :]
        pltpu.make_async_copy(sent, sent, q_send).wait()

    slots = late_ref.at[pl.ds(0, n_peers - 1)]
    pltpu.make_async_copy(slots, slots, l_recv).wait()
    pltpu.make_async_copy(slots, slots, l_send).wait()


SLOTS = 4


def by_position(na, nb, early_ref, which, n_early, seqs):
    n_peers = na * nb
    n_loc = seqs // n_peers
    lane = lax.broadcasted_iota(jnp.int32, (n_peers, 128), 1)
    mine = (lax.broadcasted_iota(jnp.int32, (n_peers, seqs), 1) // n_loc
            == lax.broadcasted_iota(jnp.int32, (n_peers, seqs), 0))
    table = jnp.concatenate(
        [early_ref[g % nb, na * which + g // nb:na * which + g // nb + 1, :] for g in range(n_peers)], axis=0)
    out = jnp.ones((8, seqs), F32)
    for i in range(n_early):
        x = pltpu.roll(table, (128 - n_loc * i) % 128, 1)
        x = jnp.where(lane < n_loc, x, 0.0)
        shift = n_loc
        while shift < 128:
            x = x + pltpu.roll(x, shift, 1)
            shift *= 2
        x = jnp.concatenate([x] * (seqs // 128), axis=1)
        row = jnp.sum(jnp.where(mine, x, 0.0), axis=0, keepdims=True)
        out = jnp.where(lax.broadcasted_iota(jnp.int32, (8, seqs), 0) == i, row, out)
    return out


def early_output_kernel(na, nb, ex_ref, bonus_ref, early_ref, res_ref, bonus_out, order_ref, stage, stage_sem, bonus_sem):
    n_draft, seqs, vocab = ex_ref.shape
    n_early, half = n_draft - 1, seqs // 2
    bonus_copy = pltpu.make_async_copy(bonus_ref, bonus_out, bonus_sem)
    bonus_copy.start()
    order_ref[...] = jnp.zeros_like(order_ref)
    inv = 1.0 / by_position(na, nb, early_ref, 0, n_early, seqs)

    def out_copy(k, slot):
        i, h = k // 2, lax.rem(k, 2)
        return pltpu.make_async_copy(
            stage.at[slot], res_ref.at[i, pl.ds(pl.multiple_of(h * half, half), half), :], stage_sem.at[slot])

    @pl.loop(0, 2 * n_early)
    def _(k):
        i, h, slot = k // 2, lax.rem(k, 2), lax.rem(k, SLOTS)
        row = get_row(inv, i)
        col = to_col(jnp.where(h == 0, row[:, :half], row[:, half:]))

        @pl.when(k >= SLOTS)
        def _():
            out_copy(k - SLOTS, slot).wait()

        @pl.loop(0, vocab // NT)
        def _(t):
            cols = pl.ds(pl.multiple_of(t * NT, NT), NT)
            stage[slot, :, cols] = ex_ref[i, pl.ds(pl.multiple_of(h * half, half), half), cols] * col

        out_copy(k, slot).start()

    for k in range(2 * n_early - SLOTS, 2 * n_early):
        out_copy(k, k % SLOTS).wait()
    bonus_copy.wait()


def late_output_kernel(na, nb, ex_ref, part_ref, early_ref, late_ref, res_in, res_ref, accept_ref, expected_ref,
                       stage, accept_v, expected_v, stage_sem, small_sem):
    n_draft, seqs, vocab = ex_ref.shape
    n_early, block = n_draft - 1, seqs // na
    za = lax.axis_index("tpa")
    inner, partner = (za == 1) | (za == 2), na - 1 - za
    late = late_ref[0]
    for k in range(1, na * nb):
        late += late_ref[k]
    col = to_col(1.0 / late[0:1])

    pieces = 2 * na
    rows_each = seqs // pieces

    def out_copy(piece):
        rows = pl.ds(piece * rows_each, rows_each)
        return pltpu.make_async_copy(stage.at[rows], res_ref.at[n_early, rows, :], stage_sem.at[piece])

    for piece in range(pieces):
        first = piece * rows_each
        rows, scale = pl.ds(first, rows_each), col[first:first + rows_each]
        from_part = inner & (partner == first // block)

        @pl.when(from_part)
        def _():
            stage[rows, :] = part_ref[pl.ds(first % block, rows_each), :] * scale

        @pl.when(jnp.logical_not(from_part))
        def _():
            stage[rows, :] = ex_ref[n_early, rows, :] * scale

        out_copy(piece).start()

    accept = by_position(na, nb, early_ref, 1, n_early, seqs)
    accept = jnp.where(lax.broadcasted_iota(jnp.int32, accept.shape, 0) == n_early, late[1:2], accept)[:n_draft]
    accept_v[...] = accept
    prod = accept[0:1]
    expected = prod
    for i in range(1, n_draft):
        prod = prod * accept[i:i + 1]
        expected += prod
    expected_v[...] = expected
    small_copies = (pltpu.make_async_copy(accept_v, accept_ref, small_sem.at[0]),
                    pltpu.make_async_copy(expected_v, expected_ref, small_sem.at[1]))
    for copy in small_copies:
        copy.start()
    for piece in range(pieces):
        out_copy(piece).wait()
    for copy in small_copies:
        copy.wait()


def solution(mesh):
    na, nb = mesh.shape["tpa"], mesh.shape["tpb"]
    n_peers = na * nb
    any_spec = pl.BlockSpec(memory_space=pl.ANY)
    vmem_spec = pl.BlockSpec(memory_space=pltpu.VMEM)

    def local_step(hidden, w_head, q_draft, x_draft):
        seqs, n_pos, depth = hidden.shape
        vocab = w_head.shape[1]
        n_loc, n_draft, _ = q_draft.shape
        dims = (n_pos, seqs, depth, vocab, n_loc, na, nb)
        dma = pltpu.SemaphoreType.DMA
        small = pltpu.VMEM((4, 8, 128), F32)
        q_rows = q_draft.transpose(1, 0, 2)
        block = seqs // na
        ex, bonus, early, late_part, part_p, part_q, part_head, part_tok = pl.pallas_call(
            functools.partial(exchange_kernel, dims),
            out_shape=(pltpu.VMEM((n_draft, seqs, vocab), F32), pltpu.VMEM((seqs, vocab), F32), small,
                       pltpu.VMEM((2, seqs), F32), pltpu.VMEM((block, vocab), F32), pltpu.VMEM((block, vocab), F32),
                       pltpu.VMEM((n_loc // 2, vocab), F32), pltpu.VMEM((block, 128), jnp.int32)),
            in_specs=[any_spec] * 4,
            out_specs=(vmem_spec,) * 8,
            scratch_shapes=[
                pltpu.VMEM((n_pos, seqs, depth), jnp.bfloat16),
                pltpu.VMEM((2, depth, NT), jnp.bfloat16),
                pltpu.VMEM((n_pos, seqs, vocab), F32),
                pltpu.VMEM((n_draft, seqs), jnp.int32),
                pltpu.VMEM((n_draft, seqs, 128), jnp.int32),
                small, small, small, small, small, small, small,
                dma, dma((2,)), dma, dma, dma((nb,)), pltpu.SemaphoreType.REGULAR, dma, dma((na,)), dma, dma((n_peers,)),
            ] + [dma] * 14,
            compiler_params=pltpu.CompilerParams(collective_id=0, has_side_effects=True, vmem_limit_bytes=38 * 2**20),
            name="exchange",
        )(hidden.transpose(1, 0, 2), w_head, q_rows, x_draft.T)
        res, bonus_out, order = pl.pallas_call(
            functools.partial(early_output_kernel, na, nb),
            out_shape=(jax.ShapeDtypeStruct((n_draft, seqs, vocab), F32), jax.ShapeDtypeStruct((seqs, vocab), F32),
                       pltpu.VMEM((8, 128), F32)),
            in_specs=[vmem_spec] * 3,
            out_specs=(any_spec, any_spec, vmem_spec),
            scratch_shapes=[pltpu.VMEM((SLOTS, seqs // 2, vocab), F32), dma((SLOTS,)), dma],
            compiler_params=pltpu.CompilerParams(vmem_limit_bytes=12 * 2**20),
            name="early_output",
        )(ex, bonus, early)
        part, late = pl.pallas_call(
            functools.partial(last_kernel, (n_draft, seqs, vocab, n_loc, na, nb)),
            out_shape=(pltpu.VMEM((block, vocab), F32), pltpu.VMEM((n_peers, 2, seqs), F32)),
            in_specs=[vmem_spec] * 6,
            out_specs=(vmem_spec, vmem_spec),
            scratch_shapes=[pltpu.VMEM((2, seqs), F32), pltpu.SemaphoreType.REGULAR, dma, dma((nb,)), dma, dma],
            compiler_params=pltpu.CompilerParams(collective_id=1, has_side_effects=True, vmem_limit_bytes=28 * 2**20),
            name="last",
        )(part_q, part_head, part_p, part_tok, late_part, order)
        res, accept, expected = pl.pallas_call(
            functools.partial(late_output_kernel, na, nb),
            out_shape=(jax.ShapeDtypeStruct((n_draft, seqs, vocab), F32), jax.ShapeDtypeStruct((n_draft, seqs), F32),
                       jax.ShapeDtypeStruct((1, seqs), F32)),
            in_specs=[vmem_spec] * 4 + [any_spec],
            out_specs=(any_spec,) * 3,
            scratch_shapes=[pltpu.VMEM((seqs, vocab), F32), pltpu.VMEM((n_draft, seqs), F32), pltpu.VMEM((1, seqs), F32),
                            dma((2 * na,)), dma((2,))],
            input_output_aliases={4: 0},
            compiler_params=pltpu.CompilerParams(vmem_limit_bytes=12 * 2**20),
            name="late_output",
        )(ex, part, early, late, res)
        return accept.T, expected.reshape(seqs), res.transpose(1, 0, 2), bonus_out

    return jax.shard_map(
        local_step, mesh=mesh,
        in_specs=(P("dp", None, None), P(None, VOCAB_AXES), P(("dp",) + VOCAB_AXES, None, None), P("dp", None)),
        out_specs=(P("dp", None), P("dp"), P("dp", None, VOCAB_AXES), P("dp", VOCAB_AXES)),
        check_vma=False)
```
